8 devices in a mesh: dp: 1 (over z), tp: 8 (over y, x, core).
Axes of the slice: x: 2, y: 2, z: 1, core: 2. Of those that a mesh axis runs over, the one named last changes fastest.
Arguments:
- x_in: bfloat16 [256, 2048], P('dp')
- seq_lens: int32 [256], P('dp')
- g_attn: bfloat16 [2, 2048], replicated
- g_mlp: bfloat16 [2, 2048], replicated
- w_q: bfloat16 [2, 2048, 2048], P(None, None, 'tp')
- b_q: bfloat16 [2, 2048], P(None, 'tp')
- w_k: bfloat16 [2, 2048, 1024], P(None, None, 'tp')
- b_k: bfloat16 [2, 1024], P(None, 'tp')
- w_v: bfloat16 [2, 2048, 1024], P(None, None, 'tp')
- b_v: bfloat16 [2, 1024], P(None, 'tp')
- w_o: bfloat16 [2, 2048, 2048], P(None, 'tp')
- w_gate: bfloat16 [2, 2048, 6144], P(None, None, 'tp')
- w_up: bfloat16 [2, 2048, 6144], P(None, None, 'tp')
- w_down: bfloat16 [2, 6144, 2048], P(None, 'tp')
- k_cache: bfloat16 [2, 256, 256, 8, 128], P(None, 'dp', None, 'tp')
- v_cache: bfloat16 [2, 256, 256, 8, 128], P(None, 'dp', None, 'tp')
Outputs:
- output 1: bfloat16 [256, 2048], P('dp')
- output 2: bfloat16 [2, 256, 256, 8, 128], P(None, 'dp', None, 'tp')
- output 3: bfloat16 [2, 256, 256, 8, 128], P(None, 'dp', None, 'tp')
All inputs are finite; a program needn't handle non-finite values.
Results may differ from the reference program's by a relative error of at most 0.0194395.
Values are sent between devices in bfloat16 or wider.
A program may use at most 1 GiB of HBM per device.

```python
import math
import jax
import jax.numpy as jnp
from jax import lax

D = 2048
HEADS = 16
KV_HEADS = 8
HEAD = 128
FF = 6144
BATCH = 256
CACHE = 256
LAYERS = 2
ROPE_THETA = 1000000.0
EPS = 1e-6


def setup_inputs(seed: int = 0, part: int = 0) -> dict:
    root_key = jax.random.key(seed)
    weight_keys = jax.random.split(root_key, 12)
    part_keys = jax.random.split(jax.random.fold_in(root_key, part), 5)
    group_size = HEADS // KV_HEADS
    q_width = HEADS * HEAD
    kv_width = KV_HEADS * HEAD
    couple = 0.6 * math.log(CACHE) / math.sqrt(HEAD)

    def normal(sub_key, arr_shape, arr_scale):
        return jax.random.normal(sub_key, arr_shape, jnp.float32) * arr_scale

    seq_lens = jax.random.randint(part_keys[1], (BATCH,), CACHE // 16, CACHE, dtype=jnp.int32)
    seq_lens = seq_lens.at[0].set(CACHE - 1).at[1].set(CACHE // 16)
    k_bias = normal(weight_keys[5], (LAYERS, KV_HEADS, 1, HEAD), 1.0)
    q_bias = couple * k_bias + normal(weight_keys[3], (LAYERS, KV_HEADS, group_size, HEAD), 1.0)
    cache_shape = (LAYERS, BATCH, CACHE, KV_HEADS, HEAD)
    v_mean = normal(part_keys[3], (LAYERS, BATCH, 1, KV_HEADS, HEAD), 1.0)
    return {
        "x_in": normal(part_keys[0], (BATCH, D), 1.0).astype(jnp.bfloat16),
        "seq_lens": seq_lens,
        "g_attn": (1.0 + normal(weight_keys[0], (LAYERS, D), 0.25)).astype(jnp.bfloat16),
        "g_mlp": (1.0 + normal(weight_keys[1], (LAYERS, D), 0.25)).astype(jnp.bfloat16),
        "w_q": normal(weight_keys[2], (LAYERS, D, q_width), D ** -0.5).astype(jnp.bfloat16),
        "b_q": q_bias.reshape(LAYERS, q_width).astype(jnp.bfloat16),
        "w_k": normal(weight_keys[4], (LAYERS, D, kv_width), D ** -0.5).astype(jnp.bfloat16),
        "b_k": k_bias.reshape(LAYERS, kv_width).astype(jnp.bfloat16),
        "w_v": normal(weight_keys[6], (LAYERS, D, kv_width), D ** -0.5).astype(jnp.bfloat16),
        "b_v": normal(weight_keys[7], (LAYERS, kv_width), 1.0).astype(jnp.bfloat16),
        "w_o": normal(weight_keys[8], (LAYERS, q_width, D), q_width ** -0.5).astype(jnp.bfloat16),
        "w_gate": normal(weight_keys[9], (LAYERS, D, FF), D ** -0.5).astype(jnp.bfloat16),
        "w_up": normal(weight_keys[10], (LAYERS, D, FF), D ** -0.5).astype(jnp.bfloat16),
        "w_down": normal(weight_keys[11], (LAYERS, FF, D), FF ** -0.5).astype(jnp.bfloat16),
        "k_cache": normal(part_keys[2], cache_shape, 1.0).astype(jnp.bfloat16),
        "v_cache": (v_mean + normal(part_keys[4], cache_shape, 1.0)).astype(jnp.bfloat16),
    }


def rms_norm(vec_in, gain_vec):
    vec_f32 = vec_in.astype(jnp.float32)
    mean_sq = jnp.mean(vec_f32 * vec_f32, axis=-1, keepdims=True)
    return (vec_f32 * lax.rsqrt(mean_sq + EPS) * gain_vec.astype(jnp.float32)).astype(jnp.bfloat16)


def rope_tables(seq_lens, head_dim):
    half_dim = head_dim // 2
    inv_freq = ROPE_THETA ** (-2.0 * jnp.arange(half_dim, dtype=jnp.float32) / head_dim)
    angles = seq_lens.astype(jnp.float32)[:, None] * inv_freq[None, :]
    angles = jnp.concatenate([angles, angles], axis=-1)[:, None, :]
    return jnp.cos(angles), jnp.sin(angles)


def apply_rope(vec_in, cos_tab, sin_tab):
    half_dim = vec_in.shape[-1] // 2
    rotated = jnp.concatenate([-vec_in[..., half_dim:], vec_in[..., :half_dim]], axis=-1)
    return vec_in * cos_tab + rotated * sin_tab


def decoder_layer(x_in, seq_lens, cos_tab, sin_tab, params):
    g_attn, g_mlp, w_q, b_q, w_k, b_k, w_v, b_v, w_o, w_gate, w_up, w_down, k_cache, v_cache = params
    num_rows = x_in.shape[0]
    group_size = HEADS // KV_HEADS
    normed = rms_norm(x_in, g_attn)
    q_full = jnp.dot(normed, w_q, preferred_element_type=jnp.float32) + b_q.astype(jnp.float32)
    q_rot = apply_rope(q_full.reshape(num_rows, HEADS, HEAD), cos_tab, sin_tab).astype(jnp.bfloat16)
    k_full = jnp.dot(normed, w_k, preferred_element_type=jnp.float32) + b_k.astype(jnp.float32)
    k_rot = apply_rope(k_full.reshape(num_rows, KV_HEADS, HEAD), cos_tab, sin_tab).astype(jnp.bfloat16)
    v_full = jnp.dot(normed, w_v, preferred_element_type=jnp.float32) + b_v.astype(jnp.float32)
    v_new = v_full.astype(jnp.bfloat16).reshape(num_rows, KV_HEADS, HEAD)
    slot_ids = jnp.arange(CACHE, dtype=jnp.int32)
    is_new = (slot_ids[None, :] == seq_lens[:, None])[:, :, None, None]
    k_next = jnp.where(is_new, k_rot[:, None], k_cache)
    v_next = jnp.where(is_new, v_new[:, None], v_cache)
    q_grouped = q_rot.reshape(num_rows, KV_HEADS, group_size, HEAD)

    def attend_row(row_args):
        q_row, k_row, v_row, row_len = row_args
        scores = jnp.einsum("kgd,skd->kgs", q_row.astype(jnp.float32), k_row.astype(jnp.float32)) * (HEAD ** -0.5)
        visible = slot_ids <= row_len
        scores = jnp.where(visible[None, None, :], scores, -1e30)
        attn_probs = jax.nn.softmax(scores, axis=-1).astype(jnp.bfloat16)
        out_row = jnp.einsum("kgs,skd->kgd", attn_probs.astype(jnp.float32), v_row.astype(jnp.float32))
        return out_row.astype(jnp.bfloat16)

    attn_out = lax.map(attend_row, (q_grouped, k_next, v_next, seq_lens)).reshape(num_rows, HEADS * HEAD)
    x_mid = (x_in.astype(jnp.float32) + jnp.dot(attn_out, w_o, preferred_element_type=jnp.float32)).astype(jnp.bfloat16)
    normed_mlp = rms_norm(x_mid, g_mlp)
    gate_proj = jnp.dot(normed_mlp, w_gate, preferred_element_type=jnp.float32)
    up_proj = jnp.dot(normed_mlp, w_up, preferred_element_type=jnp.float32)
    hidden_act = (jax.nn.silu(gate_proj) * up_proj).astype(jnp.bfloat16)
    x_next = (x_mid.astype(jnp.float32) + jnp.dot(hidden_act, w_down, preferred_element_type=jnp.float32)).astype(jnp.bfloat16)
    return x_next, k_next, v_next


def reference(x_in, seq_lens, g_attn, g_mlp, w_q, b_q, w_k, b_k, w_v, b_v, w_o, w_gate, w_up, w_down, k_cache, v_cache):
    cos_tab, sin_tab = rope_tables(seq_lens, HEAD)

    def layer_step(x_carry, params):
        x_next, k_next, v_next = decoder_layer(x_carry, seq_lens, cos_tab, sin_tab, params)
        return x_next, (k_next, v_next)

    layer_params = (g_attn, g_mlp, w_q, b_q, w_k, b_k, w_v, b_v, w_o, w_gate, w_up, w_down, k_cache, v_cache)
    x_out, cache_pair = lax.scan(layer_step, x_in, layer_params)
    return x_out, cache_pair[0], cache_pair[1]
```

```python
import functools
import math

import jax
import jax.numpy as jnp
import numpy as np
from jax import lax
from jax.experimental import pallas as pl
from jax.experimental.pallas import tpu as pltpu
from jax.sharding import PartitionSpec as P

ROPE_THETA = 1000000.0
EPS = 1e-6
F32 = jnp.float32
BF16 = jnp.bfloat16
NT = (((1,), (1,)), ((), ()))
SEQ_CHUNK = 16
ROW_CHUNKS = 2


def norm_rows(vec_f32, gain_row):
    mean_sq = jnp.mean(vec_f32 * vec_f32, axis=-1, keepdims=True)
    return (vec_f32 * lax.rsqrt(mean_sq + EPS) * gain_row).astype(BF16)


def attn_kernel(layer, do_norm, aliased, *refs):
    (lens_smem, lens_row, freq, x_hbm, g_ref, bq_ref, bk_ref, bv_ref, wq_hbm, wk_hbm, wv_hbm, kc_hbm, vc_hbm) = refs[:13]
    refs = refs[13 + (2 if aliased else 0):]
    attn_ref, ko_hbm, vo_hbm = refs[:3]
    (x_buf, w_buf, k_buf, v_buf, q_f32, k_f32, v_f32, lens_col, out_f32, x_sem, w_sem, k_sem, v_sem, ko_sem, vo_sem) = refs[3:]
    batch, slots, head = k_buf.shape
    q_width = wq_hbm.shape[2]
    n_chunks = batch // SEQ_CHUNK

    x_copy = pltpu.make_async_copy(x_hbm, x_buf, x_sem)
    x_copy.start()
    w_copies = [
        pltpu.make_async_copy(wq_hbm.at[layer], w_buf.at[:, :q_width], w_sem.at[0]),
        pltpu.make_async_copy(wk_hbm.at[layer], w_buf.at[:, q_width:q_width + head], w_sem.at[1]),
        pltpu.make_async_copy(wv_hbm.at[layer], w_buf.at[:, q_width + head:], w_sem.at[2]),
    ]
    for copy in w_copies:
        copy.start()

    def chunk_copies(idx):
        rows = pl.ds(pl.multiple_of(idx * SEQ_CHUNK, SEQ_CHUNK), SEQ_CHUNK)
        return (
            pltpu.make_async_copy(kc_hbm.at[layer, rows], k_buf.at[rows], k_sem.at[idx]),
            pltpu.make_async_copy(vc_hbm.at[layer, rows], v_buf.at[rows], v_sem.at[idx]),
            pltpu.make_async_copy(k_buf.at[rows], ko_hbm.at[layer, rows], ko_sem.at[idx]),
            pltpu.make_async_copy(v_buf.at[rows], vo_hbm.at[layer, rows], vo_sem.at[idx]),
        )

    @pl.loop(0, n_chunks)
    def _(idx):
        k_in, v_in, _, _ = chunk_copies(idx)
        k_in.start()
        v_in.start()

    lens_f = lens_row[...].astype(F32)
    same = lax.broadcasted_iota(jnp.int32, (batch, batch), 0) == lax.broadcasted_iota(jnp.int32, (batch, batch), 1)
    pos_col = jnp.sum(jnp.where(same, jnp.broadcast_to(lens_f, (batch, batch)), 0.0), axis=1, keepdims=True)
    lens_col[...] = jnp.broadcast_to(pos_col, (batch, head)).astype(jnp.int32)
    angles = pos_col * freq[...]
    cos_tab = jnp.cos(angles)
    lane = lax.broadcasted_iota(jnp.int32, (1, head), 1)
    sin_tab = jnp.sin(angles) * jnp.where(lane < head // 2, -1.0, 1.0)

    def rope(vec):
        return vec * cos_tab + pltpu.roll(vec, head // 2, 1) * sin_tab

    x_copy.wait()
    for copy in w_copies:
        copy.wait()
    if do_norm:
        normed = norm_rows(x_buf[...].astype(F32), g_ref[layer:layer + 1, :].astype(F32))
    else:
        normed = x_buf[...]
    for col in range(q_width // head):
        cols = slice(col * head, (col + 1) * head)
        part = jnp.dot(normed, w_buf[:, cols], preferred_element_type=F32) + bq_ref[layer:layer + 1, cols].astype(F32)
        q_f32[:, cols] = rope(part).astype(BF16).astype(F32)
    part = jnp.dot(normed, w_buf[:, q_width:], preferred_element_type=F32)
    k_f32[...] = rope(part[:, :head] + bk_ref[layer:layer + 1, :].astype(F32)).astype(BF16).astype(F32)
    v_f32[...] = (part[:, head:] + bv_ref[layer:layer + 1, :].astype(F32)).astype(BF16).astype(F32)

    half = 8
    scale = head ** -0.5
    row_in_group = lax.broadcasted_iota(jnp.int32, (2 * half, head), 0) % half
    slot_id = lax.broadcasted_iota(jnp.int32, (2 * half, slots), 1)
    tile_row = lax.broadcasted_iota(jnp.int32, (16, head), 0)

    @pl.loop(0, n_chunks)
    def _(idx):
        k_in, v_in, k_out, v_out = chunk_copies(idx)
        k_in.wait()
        v_in.wait()
        for sub in range(SEQ_CHUNK):
            seq = idx * SEQ_CHUNK + sub
            pos = lens_smem[seq]
            base = pl.multiple_of((pos // 16) * 16, 16)
            hit = tile_row == pos - base
            for buf, new in ((k_buf, k_f32), (v_buf, v_f32)):
                row = jnp.broadcast_to(new[pl.ds(seq, 1), :], (16, head))
                old = buf[seq, pl.ds(base, 16), :]
                buf[seq, pl.ds(base, 16), :] = jnp.where(hit, row, old.astype(F32)).astype(BF16)
        k_out.start()
        v_out.start()
        for group in range(SEQ_CHUNK // half):
            first = pl.multiple_of(idx * SEQ_CHUNK + group * half, half)
            q_rows = q_f32[pl.ds(first, half), :]
            q_all = jnp.concatenate([q_rows[:, :head], q_rows[:, head:]], axis=0)
            scores = jnp.zeros((2 * half, slots), F32)
            for pair in range(half // 2):
                lhs = jnp.concatenate([jnp.where(row_in_group == 2 * pair + e, q_all, 0.0) for e in range(2)], axis=1).astype(BF16)
                rhs = jnp.concatenate([k_buf[first + 2 * pair + e] for e in range(2)], axis=1)
                scores += lax.dot_general(lhs, rhs, NT, preferred_element_type=F32)
            pos_rows = lens_col[pl.ds(first, half), 0:1]
            pos_all = jnp.concatenate([pos_rows, pos_rows], axis=0)
            scores = jnp.where(slot_id <= pos_all, scores * scale, -1e30)
            top = jnp.max(scores, axis=-1, keepdims=True)
            expo = jnp.exp(scores - top)
            probs = (expo / jnp.sum(expo, axis=-1, keepdims=True)).astype(BF16)
            out = jnp.zeros((2 * half, head), F32)
            for pair in range(half // 2):
                rhs = jnp.concatenate([v_buf[first + 2 * pair + e] for e in range(2)], axis=1)
                both = jnp.dot(probs, rhs, preferred_element_type=F32)
                for e in range(2):
                    out = jnp.where(row_in_group == 2 * pair + e, both[:, e * head:(e + 1) * head], out)
            out_f32[pl.ds(first, half), :] = jnp.concatenate([out[:half], out[half:]], axis=1)

    attn_ref[...] = out_f32[...].astype(BF16)

    @pl.loop(0, n_chunks)
    def _(idx):
        _, _, k_out, v_out = chunk_copies(idx)
        k_out.wait()
        v_out.wait()


def attn_call(layer, do_norm, lens, freq, x_in, gain, b_q, b_k, b_v, w_q, w_k, w_v, k_cache, v_cache, prev):
    batch, slots, head = k_cache.shape[1:]
    width = x_in.shape[1]
    q_width = w_q.shape[2]
    any_spec = pl.BlockSpec(memory_space=pl.ANY)
    vmem = pl.BlockSpec(memory_space=pltpu.VMEM)
    aliased = prev is not None
    args = [lens, lens.reshape(1, batch), freq, x_in, gain, b_q, b_k, b_v, w_q, w_k, w_v, k_cache, v_cache]
    in_specs = [pl.BlockSpec(memory_space=pltpu.SMEM), vmem, vmem, any_spec, vmem, vmem, vmem, vmem] + [any_spec] * 5
    aliases = {}
    if aliased:
        aliases = {len(args): 1, len(args) + 1: 2}
        args += list(prev)
        in_specs += [any_spec] * 2
    n_chunks = batch // SEQ_CHUNK
    macs = batch * width * (q_width + 2 * head) + 2 * batch * slots * q_width
    return pl.pallas_call(
        functools.partial(attn_kernel, layer, do_norm, aliased),
        out_shape=(
            jax.ShapeDtypeStruct((batch, q_width), BF16),
            jax.ShapeDtypeStruct(k_cache.shape, BF16),
            jax.ShapeDtypeStruct(v_cache.shape, BF16),
        ),
        in_specs=in_specs,
        out_specs=(vmem, any_spec, any_spec),
        scratch_shapes=[
            pltpu.VMEM((batch, width), BF16),
            pltpu.VMEM((width, q_width + 2 * head), BF16),
            pltpu.VMEM((batch, slots, head), BF16),
            pltpu.VMEM((batch, slots, head), BF16),
            pltpu.VMEM((batch, q_width), F32),
            pltpu.VMEM((batch, head), F32),
            pltpu.VMEM((batch, head), F32),
            pltpu.VMEM((batch, head), jnp.int32),
            pltpu.VMEM((batch, q_width), F32),
            pltpu.SemaphoreType.DMA,
            pltpu.SemaphoreType.DMA((3,)),
            pltpu.SemaphoreType.DMA((n_chunks,)),
            pltpu.SemaphoreType.DMA((n_chunks,)),
            pltpu.SemaphoreType.DMA((n_chunks,)),
            pltpu.SemaphoreType.DMA((n_chunks,)),
        ],
        input_output_aliases=aliases,
        compiler_params=pltpu.CompilerParams(vmem_limit_bytes=60 * 1024 * 1024),
        cost_estimate=pl.CostEstimate(flops=2 * macs, bytes_accessed=4 * batch * slots * head * 2, transcendentals=batch * slots * 2),
        name=f"attn{layer}",
    )(*args)


def mix_kernel(layer, last, attn_ref, x_hbm, gm_ref, gn_ref, wo_hbm, wg_hbm, wu_hbm, wd_hbm, *refs):
    if last:
        out_hbm = refs[0]
        refs = refs[1:]
    else:
        out_hbm, xs_ref = refs[:2]
        refs = refs[2:]
    (wo, wg, wu, wd, x_own, act, d_send, d_recv, own, r_send, r_recv, gathered,
     w_sem, x_sem, ds_sem, dr_sem, rs_sem, rr_sem, as_sem, ar_sem, fs_sem, fr_sem, o_sem) = refs
    width = wo.shape[1]
    hidden = wg.shape[1]
    rows = attn_ref.shape[0] // ROW_CHUNKS
    core_rows = rows // 2
    blk = core_rows // 4
    me = lax.axis_index("tp")
    core = me % 2
    chip = me // 2
    partner = me + 1 - 2 * core
    peer_y = (chip + 2) % 4
    peers = [chip, 3 - peer_y, peer_y, 3 - chip]

    def dev(idx):
        return {"tp": idx}

    w_copies = [pltpu.make_async_copy(src.at[layer], dst, w_sem.at[i])
                for i, (src, dst) in enumerate(((wo_hbm, wo), (wg_hbm, wg), (wu_hbm, wu), (wd_hbm, wd)))]
    for copy in w_copies:
        copy.start()

    def own_row(j):
        return pl.multiple_of(j * rows + core * core_rows + chip * blk, blk)

    x_copies = []
    for j in range(ROW_CHUNKS):
        src = x_hbm.at[j] if x_hbm.shape[0] == ROW_CHUNKS else x_hbm.at[pl.ds(own_row(j), blk)]
        x_copies.append(pltpu.make_async_copy(src, x_own.at[j], x_sem.at[j]))
        x_copies[-1].start()

    barrier = pltpu.get_barrier_semaphore()
    others = [partner] + [2 * peers[r] + core for r in range(1, 4)]
    for other in others:
        pl.semaphore_signal(barrier, inc=1, device_id=dev(other), device_id_type=pl.DeviceIdType.MESH)

    def remote(src, dst, send, recv, target):
        return pltpu.make_async_remote_copy(src_ref=src, dst_ref=dst, send_sem=send, recv_sem=recv,
                                            device_id=dev(target), device_id_type=pl.DeviceIdType.MESH)

    def share(s, j, lhs, weight):
        step = 512

        @pl.loop(0, width // step)
        def _(n):
            cols = pl.ds(pl.multiple_of(n * step, step), step)
            part = jnp.dot(lhs, weight[:, cols], preferred_element_type=F32)
            act_dst = own.at[s, j]
            act_dst[:, cols] = part
        other_half = pl.multiple_of((1 - core) * core_rows, core_rows)
        d_send[s, j] = own[s, j, pl.ds(other_half, core_rows), :].astype(BF16)

    def d_copy(s, j):
        return remote(d_send.at[s, j], d_recv.at[s, j], ds_sem.at[s, j], dr_sem.at[s, j], partner)

    def r_copy(s, j, r):
        return remote(r_send.at[s, j, r], r_recv.at[s, j, r], rs_sem.at[s, j, r], rr_sem.at[s, j, r], 2 * peers[r] + core)

    def scatter(s, j):
        d_copy(s, j).wait()
        for r in (3, 1, 2):
            off = pl.multiple_of(peers[r] * blk, blk)
            mine = own[s, j, pl.ds(core * core_rows + off, blk), :]
            r_send[s, j, r] = (mine + d_recv[s, j, pl.ds(off, blk), :].astype(F32)).astype(BF16)
            r_copy(s, j, r).start()

    def reduce(s, j):
        off = pl.multiple_of(chip * blk, blk)
        total = own[s, j, pl.ds(core * core_rows + off, blk), :] + d_recv[s, j, pl.ds(off, blk), :].astype(F32)
        for r in (1, 2, 3):
            r_copy(s, j, r).wait()
            total += r_recv[s, j, r].astype(F32)
        new = (x_own[j].astype(F32) + total).astype(BF16)
        x_own[j] = new
        return new

    def block_row(j, cc, k):
        return pl.ds(pl.multiple_of(j * rows + cc * core_rows + k * blk, blk), blk)

    def a_copy(s, j, r):
        here = block_row(j, core, chip)
        target = partner if r == 0 else 2 * peers[r] + core
        return remote(gathered.at[s, here], gathered.at[s, here], as_sem.at[s, j, r], ar_sem.at[s, j, r], target)

    def f_copy(s, j, r):
        here = block_row(j, core, peers[r])
        return remote(gathered.at[s, here], gathered.at[s, here], fs_sem.at[s, j, r], fr_sem.at[s, j, r], partner)

    def gather_start(s, j, value):
        gathered[s, block_row(j, core, chip), :] = value
        for r in (3, 1, 2, 0):
            a_copy(s, j, r).start()

    def gather_finish(s, j):
        for r in (1, 2, 3):
            a_copy(s, j, r).wait_recv()
            f_copy(s, j, r).start()
        a_copy(s, j, 0).wait_recv()
        for r in (1, 2, 3):
            f_copy(s, j, r).wait_recv()

    w_copies[0].wait()
    for j in range(ROW_CHUNKS):
        share(0, j, attn_ref[j * rows:(j + 1) * rows, :], wo)
        if j == 0:
            pl.semaphore_wait(barrier, len(others))
        d_copy(0, j).start()
    for copy in x_copies:
        copy.wait()
    for j in range(ROW_CHUNKS):
        scatter(0, j)
    for j in range(ROW_CHUNKS):
        new = reduce(0, j)
        gather_start(0, j, norm_rows(new.astype(F32), gm_ref[layer:layer + 1, :].astype(F32)))
    for copy in w_copies[1:]:
        copy.wait()
    for j in range(ROW_CHUNKS):
        gather_finish(0, j)
        step = 256

        @pl.loop(0, hidden // step)
        def _(n):
            cols = pl.ds(pl.multiple_of(n * step, step), step)
            lhs = gathered[0, j * rows:(j + 1) * rows, :]
            gate = jnp.dot(lhs, wg[:, cols], preferred_element_type=F32)
            up = jnp.dot(lhs, wu[:, cols], preferred_element_type=F32)
            act[j, :, cols] = (gate * jax.nn.sigmoid(gate) * up).astype(BF16)
        share(1, j, act[j], wd)
        d_copy(1, j).start()
    for j in range(ROW_CHUNKS):
        scatter(1, j)
    outs = []
    for j in range(ROW_CHUNKS):
        new = reduce(1, j)
        if last:
            gather_start(1, j, new)
        else:
            xs_ref[j] = new
            gather_start(1, j, norm_rows(new.astype(F32), gn_ref[layer + 1:layer + 2, :].astype(F32)))
    for j in range(ROW_CHUNKS):
        gather_finish(1, j)
        here = pl.ds(j * rows, rows)
        outs.append(pltpu.make_async_copy(gathered.at[1, here], out_hbm.at[here], o_sem.at[j]))
        outs[-1].start()
    for s in range(2):
        for j in range(ROW_CHUNKS):
            for r in range(4):
                a_copy(s, j, r).wait_send()
            for r in range(1, 4):
                f_copy(s, j, r).wait_send()
    for copy in outs:
        copy.wait()


def mix_call(layer, last, attn, x_own, g_mlp, g_attn, w_o, w_gate, w_up, w_down):
    batch = attn.shape[0]
    depth, width = w_o.shape[1:]
    hidden = w_gate.shape[2]
    rows = batch // ROW_CHUNKS
    blk = rows // 8
    any_spec = pl.BlockSpec(memory_space=pl.ANY)
    vmem = pl.BlockSpec(memory_space=pltpu.VMEM)
    out_shape = [jax.ShapeDtypeStruct((batch, width), BF16)]
    out_specs = [any_spec]
    if not last:
        out_shape.append(jax.ShapeDtypeStruct((ROW_CHUNKS, blk, width), BF16))
        out_specs.append(vmem)
    sem = pltpu.SemaphoreType.DMA
    nc = ROW_CHUNKS
    return pl.pallas_call(
        functools.partial(mix_kernel, layer, last),
        out_shape=out_shape,
        in_specs=[vmem, any_spec, vmem, vmem, any_spec, any_spec, any_spec, any_spec],
        out_specs=out_specs,
        scratch_shapes=[
            pltpu.VMEM((depth, width), BF16),
            pltpu.VMEM((width, hidden), BF16),
            pltpu.VMEM((width, hidden), BF16),
            pltpu.VMEM((hidden, width), BF16),
            pltpu.VMEM((nc, blk, width), BF16),
            pltpu.VMEM((nc, rows, hidden), BF16),
            pltpu.VMEM((2, nc, rows // 2, width), BF16),
            pltpu.VMEM((2, nc, rows // 2, width), BF16),
            pltpu.VMEM((2, nc, rows, width), F32),
            pltpu.VMEM((2, nc, 4, blk, width), BF16),
            pltpu.VMEM((2, nc, 4, blk, width), BF16),
            pltpu.VMEM((2, batch, width), BF16),
            sem((4,)), sem((nc,)),
            sem((2, nc)), sem((2, nc)),
            sem((2, nc, 4)), sem((2, nc, 4)),
            sem((2, nc, 4)), sem((2, nc, 4)),
            sem((2, nc, 4)), sem((2, nc, 4)),
            sem((nc,)),
        ],
        compiler_params=pltpu.CompilerParams(collective_id=layer, has_side_effects=True, vmem_limit_bytes=48 * 1024 * 1024),
        cost_estimate=pl.CostEstimate(flops=2 * batch * width * (depth + 3 * hidden), bytes_accessed=2 * width * (depth + 3 * hidden), transcendentals=batch * hidden),
        name=f"mix{layer}",
    )(attn, x_own, g_mlp, g_attn, w_o, w_gate, w_up, w_down)


def solution(mesh):
    weight_col = P(None, None, "tp")
    weight_row = P(None, "tp", None)
    bias_col = P(None, "tp")
    cache_spec = P(None, "dp", None, "tp", None)
    in_specs = (P("dp", None), P("dp"), P(None, None), P(None, None), weight_col, bias_col, weight_col, bias_col, weight_col, bias_col, weight_row, weight_col, weight_col, weight_row, cache_spec, cache_spec)
    out_specs = (P("dp", None), cache_spec, cache_spec)

    def local_step(x_in, seq_lens, g_attn, g_mlp, w_q, b_q, w_k, b_k, w_v, b_v, w_o, w_gate, w_up, w_down, k_cache, v_cache):
        layers, batch, slots, _, head = k_cache.shape
        inv_freq = ROPE_THETA ** (-2.0 * np.arange(head // 2) / head)
        freq = jnp.asarray(np.concatenate([inv_freq, inv_freq])[None, :].astype(np.float32))
        k_flat = k_cache.reshape(layers, batch, slots, head)
        v_flat = v_cache.reshape(layers, batch, slots, head)
        normed, x_own, prev = x_in, x_in, None
        for layer in range(layers):
            last = layer == layers - 1
            attn, k_out, v_out = attn_call(layer, layer == 0, seq_lens, freq, normed, g_attn, b_q, b_k, b_v, w_q, w_k, w_v, k_flat, v_flat, prev)
            prev = (k_out, v_out)
            outs = mix_call(layer, last, attn, x_own, g_mlp, g_attn, w_o, w_gate, w_up, w_down)
            if last:
                x_out = outs[0]
            else:
                normed, x_own = outs
        return x_out, prev[0].reshape(k_cache.shape), prev[1].reshape(v_cache.shape)

    return jax.shard_map(local_step, mesh=mesh, in_specs=in_specs, out_specs=out_specs, check_vma=False)
```

```python
import functools
import math

import jax
import jax.numpy as jnp
import numpy as np
from jax import lax
from jax.experimental import pallas as pl
from jax.experimental.pallas import tpu as pltpu
from jax.sharding import PartitionSpec as P

ROPE_THETA = 1000000.0
EPS = 1e-6
F32 = jnp.float32
BF16 = jnp.bfloat16
NT = (((1,), (1,)), ((), ()))
SEQ_CHUNK = 16
ROW_CHUNKS = 2
ATTN_VMEM = 24 * 1024 * 1024
MIX_VMEM = 22 * 1024 * 1024


def norm_rows(vec_f32, gain_row):
    mean_sq = jnp.mean(vec_f32 * vec_f32, axis=-1, keepdims=True)
    return (vec_f32 * lax.rsqrt(mean_sq + EPS) * gain_row).astype(BF16)


def attn_kernel(layer, do_norm, aliased, *refs):
    (lens_smem, lens_row, freq, x_hbm, g_ref, bq_ref, bk_ref, bv_ref, wq_hbm, wk_hbm, wv_hbm) = refs[:11]
    kc_hbm, vc_hbm = (None, None) if aliased else refs[11:13]
    refs = refs[14 if aliased else 13:]
    attn_ref, ko_hbm, vo_hbm = refs[:3]
    refs = refs[3:]
    kv_buf = refs[0] if aliased else refs[-1]
    k_buf, v_buf = kv_buf.at[0], kv_buf.at[1]
    refs = refs[1:] if aliased else refs[:-1]
    (x_buf, w_buf, q_f32, k_f32, v_f32, lens_col, out_f32, x_sem, w_sem, k_sem, v_sem, ko_sem, vo_sem) = refs
    batch, slots, head = k_buf.shape
    q_width = wq_hbm.shape[2]
    n_chunks = batch // SEQ_CHUNK

    if do_norm:
        x_copy = pltpu.make_async_copy(x_hbm, x_buf, x_sem)
        x_copy.start()
    w_copies = [
        pltpu.make_async_copy(wq_hbm.at[layer], w_buf.at[:, :q_width], w_sem.at[0]),
        pltpu.make_async_copy(wk_hbm.at[layer], w_buf.at[:, q_width:q_width + head], w_sem.at[1]),
        pltpu.make_async_copy(wv_hbm.at[layer], w_buf.at[:, q_width + head:], w_sem.at[2]),
    ]
    for copy in w_copies:
        copy.start()

    def chunk_copies(idx):
        rows = pl.ds(pl.multiple_of(idx * SEQ_CHUNK, SEQ_CHUNK), SEQ_CHUNK)
        return (
            None if aliased else pltpu.make_async_copy(kc_hbm.at[layer, rows], k_buf.at[rows], k_sem.at[idx]),
            None if aliased else pltpu.make_async_copy(vc_hbm.at[layer, rows], v_buf.at[rows], v_sem.at[idx]),
            pltpu.make_async_copy(k_buf.at[rows], ko_hbm.at[layer, rows], ko_sem.at[idx]),
            pltpu.make_async_copy(v_buf.at[rows], vo_hbm.at[layer, rows], vo_sem.at[idx]),
        )

    if not aliased:
        @pl.loop(0, n_chunks)
        def _(idx):
            k_in, v_in, _, _ = chunk_copies(idx)
            k_in.start()
            v_in.start()

    lens_f = lens_row[...].astype(F32)
    same = lax.broadcasted_iota(jnp.int32, (batch, batch), 0) == lax.broadcasted_iota(jnp.int32, (batch, batch), 1)
    pos_col = jnp.sum(jnp.where(same, jnp.broadcast_to(lens_f, (batch, batch)), 0.0), axis=1, keepdims=True)
    lens_col[...] = jnp.broadcast_to(pos_col, (batch, head)).astype(jnp.int32)
    angles = pos_col * freq[...]
    cos_tab = jnp.cos(angles)
    lane = lax.broadcasted_iota(jnp.int32, (1, head), 1)
    sin_tab = jnp.sin(angles) * jnp.where(lane < head // 2, -1.0, 1.0)

    def rope(vec):
        return vec * cos_tab + pltpu.roll(vec, head // 2, 1) * sin_tab

    for copy in w_copies:
        copy.wait()
    if do_norm:
        x_copy.wait()
        normed = norm_rows(x_buf[...].astype(F32), g_ref[layer:layer + 1, :].astype(F32))
    else:
        normed = x_hbm[...]
    for col in range(q_width // head):
        cols = slice(col * head, (col + 1) * head)
        part = jnp.dot(normed, w_buf[:, cols], preferred_element_type=F32) + bq_ref[layer:layer + 1, cols].astype(F32)
        q_f32[:, cols] = rope(part).astype(BF16).astype(F32)
    part = jnp.dot(normed, w_buf[:, q_width:], preferred_element_type=F32)
    k_f32[...] = rope(part[:, :head] + bk_ref[layer:layer + 1, :].astype(F32)).astype(BF16).astype(F32)
    v_f32[...] = (part[:, head:] + bv_ref[layer:layer + 1, :].astype(F32)).astype(BF16).astype(F32)

    half = 8
    scale = head ** -0.5
    row_in_group = lax.broadcasted_iota(jnp.int32, (2 * half, head), 0) % half
    slot_id = lax.broadcasted_iota(jnp.int32, (2 * half, slots), 1)
    tile_row = lax.broadcasted_iota(jnp.int32, (16, head), 0)

    @pl.loop(0, n_chunks)
    def _(idx):
        k_in, v_in, k_out, v_out = chunk_copies(idx)
        if not aliased:
            k_in.wait()
            v_in.wait()
        for sub in range(SEQ_CHUNK):
            seq = idx * SEQ_CHUNK + sub
            pos = lens_smem[seq]
            base = pl.multiple_of((pos // 16) * 16, 16)
            hit = tile_row == pos - base
            for buf, new in ((k_buf, k_f32), (v_buf, v_f32)):
                row = jnp.broadcast_to(new[pl.ds(seq, 1), :], (16, head))
                old = buf[seq, pl.ds(base, 16), :]
                buf[seq, pl.ds(base, 16), :] = jnp.where(hit, row, old.astype(F32)).astype(BF16)
        k_out.start()
        v_out.start()
        for group in range(SEQ_CHUNK // half):
            first = pl.multiple_of(idx * SEQ_CHUNK + group * half, half)
            q_rows = q_f32[pl.ds(first, half), :]
            q_all = jnp.concatenate([q_rows[:, :head], q_rows[:, head:]], axis=0)
            scores = jnp.zeros((2 * half, slots), F32)
            for pair in range(half // 2):
                lhs = jnp.concatenate([jnp.where(row_in_group == 2 * pair + e, q_all, 0.0) for e in range(2)], axis=1).astype(BF16)
                rhs = jnp.concatenate([k_buf[first + 2 * pair + e] for e in range(2)], axis=1)
                scores += lax.dot_general(lhs, rhs, NT, preferred_element_type=F32)
            pos_rows = lens_col[pl.ds(first, half), 0:1]
            pos_all = jnp.concatenate([pos_rows, pos_rows], axis=0)
            scores = jnp.where(slot_id <= pos_all, scores * scale, -1e30)
            top = jnp.max(scores, axis=-1, keepdims=True)
            expo = jnp.exp(scores - top)
            probs = (expo / jnp.sum(expo, axis=-1, keepdims=True)).astype(BF16)
            out = jnp.zeros((2 * half, head), F32)
            for pair in range(half // 2):
                rhs = jnp.concatenate([v_buf[first + 2 * pair + e] for e in range(2)], axis=1)
                both = jnp.dot(probs, rhs, preferred_element_type=F32)
                for e in range(2):
                    out = jnp.where(row_in_group == 2 * pair + e, both[:, e * head:(e + 1) * head], out)
            out_f32[pl.ds(first, half), :] = jnp.concatenate([out[:half], out[half:]], axis=1)

    attn_ref[...] = out_f32[...].astype(BF16)

    @pl.loop(0, n_chunks)
    def _(idx):
        _, _, k_out, v_out = chunk_copies(idx)
        k_out.wait()
        v_out.wait()


def in_hbm(*arrays):
    return [pltpu.with_memory_space_constraint(a, pltpu.HBM) for a in arrays]


def in_vmem(*arrays):
    return [pltpu.with_memory_space_constraint(a, pltpu.VMEM) for a in arrays]


def attn_call(layer, do_norm, lens, freq, x_in, gain, b_q, b_k, b_v, w_q, w_k, w_v, caches, prev):
    batch, slots, head = caches[0].shape[-3:]
    width = x_in.shape[1]
    q_width = w_q.shape[2]
    any_spec = pl.BlockSpec(memory_space=pltpu.HBM)
    vmem = pl.BlockSpec(memory_space=pltpu.VMEM)
    aliased = prev is not None
    place = in_hbm if do_norm else in_vmem
    args = [lens, lens.reshape(1, batch), freq, *place(x_in), gain, b_q, b_k, b_v, *in_hbm(w_q, w_k, w_v), *place(*caches)]
    in_specs = [pl.BlockSpec(memory_space=pltpu.SMEM), vmem, vmem, any_spec if do_norm else vmem, vmem, vmem, vmem, vmem] + [any_spec] * 5
    aliases = {}
    if aliased:
        aliases = {len(args): 1, len(args) + 1: 2, len(args) - 1: 3}
        args += in_hbm(*prev)
        in_specs = in_specs[:-2] + [vmem] + [any_spec] * 2
    cache_buf = pltpu.VMEM((2, batch, slots, head), BF16)
    out_cache = jax.ShapeDtypeStruct((w_q.shape[0], batch, slots, head), BF16)
    n_chunks = batch // SEQ_CHUNK
    macs = batch * width * (q_width + 2 * head) + 2 * batch * slots * q_width
    return pl.pallas_call(
        functools.partial(attn_kernel, layer, do_norm, aliased),
        out_shape=(
            pltpu.VMEM((batch, q_width), BF16),
            out_cache,
            out_cache,
        ) + ((cache_buf,) if aliased else ()),
        in_specs=in_specs,
        out_specs=(vmem, any_spec, any_spec) + ((vmem,) if aliased else ()),
        scratch_shapes=[
            pltpu.VMEM((batch, width), BF16),
            pltpu.VMEM((width, q_width + 2 * head), BF16),
            pltpu.VMEM((batch, q_width), F32),
            pltpu.VMEM((batch, head), F32),
            pltpu.VMEM((batch, head), F32),
            pltpu.VMEM((batch, head), jnp.int32),
            pltpu.VMEM((batch, q_width), F32),
            pltpu.SemaphoreType.DMA,
            pltpu.SemaphoreType.DMA((3,)),
            pltpu.SemaphoreType.DMA((n_chunks,)),
            pltpu.SemaphoreType.DMA((n_chunks,)),
            pltpu.SemaphoreType.DMA((n_chunks,)),
            pltpu.SemaphoreType.DMA((n_chunks,)),
        ] + ([] if aliased else [cache_buf]),
        input_output_aliases=aliases,
        compiler_params=pltpu.CompilerParams(vmem_limit_bytes=ATTN_VMEM + (0 if aliased else 4 * batch * slots * head)),
        cost_estimate=pl.CostEstimate(flops=2 * macs, bytes_accessed=4 * batch * slots * head * 2, transcendentals=batch * slots * 2),
        name=f"attn{layer}",
    )(*args)[:3]


def mix_kernel(layer, last, attn_ref, x_hbm, gm_ref, gn_ref, wo_hbm, wg_hbm, wu_hbm, wd_hbm, kc_hbm, vc_hbm, *refs):
    if last:
        out_hbm = refs[0]
        refs = refs[1:]
    else:
        out_hbm, xs_ref, kv_next = refs[:3]
        refs = refs[3:]
    (wo, wg, wu, wd, x_own, act, d_send, d_recv, own, r_send, r_recv, gathered,
     w_sem, x_sem, ds_sem, dr_sem, rs_sem, rr_sem, as_sem, ar_sem, fs_sem, fr_sem, o_sem, c_sem) = refs
    width = wo.shape[1]
    hidden = wg.shape[1]
    rows = attn_ref.shape[0] // ROW_CHUNKS
    core_rows = rows // 2
    blk = core_rows // 4
    me = lax.axis_index("tp")
    core = me % 2
    chip = me // 2
    partner = me + 1 - 2 * core
    peer_y = (chip + 2) % 4
    peers = [chip, 3 - peer_y, peer_y, 3 - chip]

    def dev(idx):
        return {"tp": idx}

    w_copies = [pltpu.make_async_copy(src.at[layer], dst, w_sem.at[i])
                for i, (src, dst) in enumerate(((wo_hbm, wo), (wg_hbm, wg), (wu_hbm, wu), (wd_hbm, wd)))]
    for copy in w_copies:
        copy.start()

    def own_row(j):
        return pl.multiple_of(j * rows + core * core_rows + chip * blk, blk)

    x_copies = []
    for j in range(ROW_CHUNKS):
        if layer:
            x_own[j] = x_hbm[j]
        else:
            x_copies.append(pltpu.make_async_copy(x_hbm.at[pl.ds(own_row(j), blk)], x_own.at[j], x_sem.at[j]))
            x_copies[-1].start()

    c_copies = []
    if not last:
        parts = c_sem.shape[1]
        size = kv_next.shape[1] // parts
        for i, src in enumerate((kc_hbm, vc_hbm)):
            for n in range(parts):
                part = pl.ds(n * size, size)
                c_copies.append(pltpu.make_async_copy(src.at[layer + 1, part], kv_next.at[i, part], c_sem.at[i, n]))
                c_copies[-1].start()

    barrier = pltpu.get_barrier_semaphore()
    others = [partner] + [2 * peers[r] + core for r in range(1, 4)]
    for other in others:
        pl.semaphore_signal(barrier, inc=1, device_id=dev(other), device_id_type=pl.DeviceIdType.MESH)

    def remote(src, dst, send, recv, target):
        return pltpu.make_async_remote_copy(src_ref=src, dst_ref=dst, send_sem=send, recv_sem=recv,
                                            device_id=dev(target), device_id_type=pl.DeviceIdType.MESH)

    def share(s, j, lhs, weight):
        step = 512

        @pl.loop(0, width // step)
        def _(n):
            cols = pl.ds(pl.multiple_of(n * step, step), step)
            part = jnp.dot(lhs, weight[:, cols], preferred_element_type=F32)
            act_dst = own.at[s, j]
            act_dst[:, cols] = part
        other_half = pl.multiple_of((1 - core) * core_rows, core_rows)
        d_send[s, j] = own[s, j, pl.ds(other_half, core_rows), :].astype(BF16)

    def d_copy(s, j):
        return remote(d_send.at[s, j], d_recv.at[s, j], ds_sem.at[s, j], dr_sem.at[s, j], partner)

    def r_copy(s, j, r):
        return remote(r_send.at[s, j, r], r_recv.at[s, j, r], rs_sem.at[s, j, r], rr_sem.at[s, j, r], 2 * peers[r] + core)

    def scatter(s, j):
        d_copy(s, j).wait()
        for r in (3, 1, 2):
            off = pl.multiple_of(peers[r] * blk, blk)
            mine = own[s, j, pl.ds(core * core_rows + off, blk), :]
            r_send[s, j, r] = (mine + d_recv[s, j, pl.ds(off, blk), :].astype(F32)).astype(BF16)
            r_copy(s, j, r).start()

    def reduce(s, j):
        off = pl.multiple_of(chip * blk, blk)
        total = own[s, j, pl.ds(core * core_rows + off, blk), :] + d_recv[s, j, pl.ds(off, blk), :].astype(F32)
        for r in (1, 2, 3):
            r_copy(s, j, r).wait()
            total += r_recv[s, j, r].astype(F32)
        new = (x_own[j].astype(F32) + total).astype(BF16)
        x_own[j] = new
        return new

    def block_row(j, cc, k):
        return pl.ds(pl.multiple_of(j * rows + cc * core_rows + k * blk, blk), blk)

    def a_copy(s, j, r):
        here = block_row(j, core, chip)
        target = partner if r == 0 else 2 * peers[r] + core
        return remote(gathered.at[s, here], gathered.at[s, here], as_sem.at[s, j, r], ar_sem.at[s, j, r], target)

    def f_copy(s, j, r):
        here = block_row(j, core, peers[r])
        return remote(gathered.at[s, here], gathered.at[s, here], fs_sem.at[s, j, r], fr_sem.at[s, j, r], partner)

    def gather_start(s, j, value):
        gathered[s, block_row(j, core, chip), :] = value
        for r in (3, 1, 2, 0):
            a_copy(s, j, r).start()

    def gather_finish(s, j):
        for r in (1, 2, 3):
            a_copy(s, j, r).wait_recv()
            f_copy(s, j, r).start()
        a_copy(s, j, 0).wait_recv()
        for r in (1, 2, 3):
            f_copy(s, j, r).wait_recv()

    w_copies[0].wait()
    for j in range(ROW_CHUNKS):
        share(0, j, attn_ref[j * rows:(j + 1) * rows, :], wo)
        if j == 0:
            pl.semaphore_wait(barrier, len(others))
        d_copy(0, j).start()
    for copy in x_copies:
        copy.wait()
    for j in range(ROW_CHUNKS):
        scatter(0, j)
    for j in range(ROW_CHUNKS):
        new = reduce(0, j)
        gather_start(0, j, norm_rows(new.astype(F32), gm_ref[layer:layer + 1, :].astype(F32)))
    for copy in w_copies[1:]:
        copy.wait()
    for j in range(ROW_CHUNKS):
        gather_finish(0, j)
        step = 256

        @pl.loop(0, hidden // step)
        def _(n):
            cols = pl.ds(pl.multiple_of(n * step, step), step)
            lhs = gathered[0, j * rows:(j + 1) * rows, :]
            gate = jnp.dot(lhs, wg[:, cols], preferred_element_type=F32)
            up = jnp.dot(lhs, wu[:, cols], preferred_element_type=F32)
            act[j, :, cols] = (gate * jax.nn.sigmoid(gate) * up).astype(BF16)
        share(1, j, act[j], wd)
        d_copy(1, j).start()
    for j in range(ROW_CHUNKS):
        scatter(1, j)
    outs = []
    for j in range(ROW_CHUNKS):
        new = reduce(1, j)
        if last:
            gather_start(1, j, new)
        else:
            xs_ref[j] = new
            gather_start(1, j, norm_rows(new.astype(F32), gn_ref[layer + 1:layer + 2, :].astype(F32)))
    for j in range(ROW_CHUNKS):
        gather_finish(1, j)
        here = pl.ds(j * rows, rows)
        if last:
            outs.append(pltpu.make_async_copy(gathered.at[1, here], out_hbm.at[here], o_sem.at[j]))
            outs[-1].start()
        else:
            out_hbm[here, :] = gathered[1, here, :]
    for s in range(2):
        for j in range(ROW_CHUNKS):
            for r in range(4):
                a_copy(s, j, r).wait_send()
            for r in range(1, 4):
                f_copy(s, j, r).wait_send()
    for copy in outs + c_copies:
        copy.wait()


def mix_call(layer, last, attn, x_own, g_mlp, g_attn, w_o, w_gate, w_up, w_down, k_cache, v_cache):
    batch = attn.shape[0]
    depth, width = w_o.shape[1:]
    hidden = w_gate.shape[2]
    rows = batch // ROW_CHUNKS
    blk = rows // 8
    any_spec = pl.BlockSpec(memory_space=pltpu.HBM)
    vmem = pl.BlockSpec(memory_space=pltpu.VMEM)
    if last:
        out_shape = [jax.ShapeDtypeStruct((batch, width), BF16)]
        out_specs = [any_spec]
    else:
        out_shape = [pltpu.VMEM((batch, width), BF16), pltpu.VMEM((ROW_CHUNKS, blk, width), BF16)]
        out_shape.append(pltpu.VMEM((2,) + k_cache.shape[1:], BF16))
        out_specs = [vmem] * 3
    sem = pltpu.SemaphoreType.DMA
    nc = ROW_CHUNKS
    return pl.pallas_call(
        functools.partial(mix_kernel, layer, last),
        out_shape=out_shape,
        in_specs=[vmem, any_spec if layer == 0 else vmem, vmem, vmem] + [any_spec] * 6,
        out_specs=out_specs,
        scratch_shapes=[
            pltpu.VMEM((depth, width), BF16),
            pltpu.VMEM((width, hidden), BF16),
            pltpu.VMEM((width, hidden), BF16),
            pltpu.VMEM((hidden, width), BF16),
            pltpu.VMEM((nc, blk, width), BF16),
            pltpu.VMEM((nc, rows, hidden), BF16),
            pltpu.VMEM((2, nc, rows // 2, width), BF16),
            pltpu.VMEM((2, nc, rows // 2, width), BF16),
            pltpu.VMEM((2, nc, rows, width), F32),
            pltpu.VMEM((2, nc, 4, blk, width), BF16),
            pltpu.VMEM((2, nc, 4, blk, width), BF16),
            pltpu.VMEM((2, batch, width), BF16),
            sem((4,)), sem((nc,)),
            sem((2, nc)), sem((2, nc)),
            sem((2, nc, 4)), sem((2, nc, 4)),
            sem((2, nc, 4)), sem((2, nc, 4)),
            sem((2, nc, 4)), sem((2, nc, 4)),
            sem((nc,)), sem((2, 8)),
        ],
        compiler_params=pltpu.CompilerParams(collective_id=layer, has_side_effects=True, vmem_limit_bytes=MIX_VMEM),
        cost_estimate=pl.CostEstimate(flops=2 * batch * width * (depth + 3 * hidden), bytes_accessed=2 * width * (depth + 3 * hidden), transcendentals=batch * hidden),
        name=f"mix{layer}",
    )(*in_vmem(attn), *(in_hbm if layer == 0 else in_vmem)(x_own), g_mlp, g_attn, *in_hbm(w_o, w_gate, w_up, w_down, k_cache, v_cache))


def solution(mesh):
    weight_col = P(None, None, "tp")
    weight_row = P(None, "tp", None)
    bias_col = P(None, "tp")
    cache_spec = P(None, "dp", None, "tp", None)
    in_specs = (P("dp", None), P("dp"), P(None, None), P(None, None), weight_col, bias_col, weight_col, bias_col, weight_col, bias_col, weight_row, weight_col, weight_col, weight_row, cache_spec, cache_spec)
    out_specs = (P("dp", None), cache_spec, cache_spec)

    def local_step(x_in, seq_lens, g_attn, g_mlp, w_q, b_q, w_k, b_k, w_v, b_v, w_o, w_gate, w_up, w_down, k_cache, v_cache):
        layers, batch, slots, _, head = k_cache.shape
        inv_freq = ROPE_THETA ** (-2.0 * np.arange(head // 2) / head)
        freq = jnp.asarray(np.concatenate([inv_freq, inv_freq])[None, :].astype(np.float32))
        k_flat = k_cache.reshape(layers, batch, slots, head)
        v_flat = v_cache.reshape(layers, batch, slots, head)
        normed, x_own, prev = x_in, x_in, None
        caches = (k_flat, v_flat)
        for layer in range(layers):
            last = layer == layers - 1
            attn, k_out, v_out = attn_call(layer, layer == 0, seq_lens, freq, normed, g_attn, b_q, b_k, b_v, w_q, w_k, w_v, caches, prev)
            prev = (k_out, v_out)
            outs = mix_call(layer, last, attn, x_own, g_mlp, g_attn, w_o, w_gate, w_up, w_down, k_flat, v_flat)
            if last:
                x_out = outs[0]
            else:
                normed, x_own, caches = outs[0], outs[1], outs[2:]
        return x_out, prev[0].reshape(k_cache.shape), prev[1].reshape(v_cache.shape)

    return jax.shard_map(local_step, mesh=mesh, in_specs=in_specs, out_specs=out_specs, check_vma=False)
```

```python
import functools
import math

import jax
import jax.numpy as jnp
import numpy as np
from jax import lax
from jax.experimental import pallas as pl
from jax.experimental.pallas import tpu as pltpu
from jax.sharding import PartitionSpec as P

ROPE_THETA = 1000000.0
EPS = 1e-6
F32 = jnp.float32
BF16 = jnp.bfloat16
NT = (((1,), (1,)), ((), ()))
SEQ_CHUNK = 16
ROW_CHUNKS = 2
ATTN_VMEM = 24 * 1024 * 1024
MIX_VMEM = 22 * 1024 * 1024


def norm_rows(vec_f32, gain_row):
    mean_sq = jnp.mean(vec_f32 * vec_f32, axis=-1, keepdims=True)
    return (vec_f32 * lax.rsqrt(mean_sq + EPS) * gain_row).astype(BF16)


def attn_kernel(layer, do_norm, aliased, *refs):
    (lens_smem, lens_row, freq, x_hbm, g_ref, bq_ref, bk_ref, bv_ref, wq_hbm, wk_hbm, wv_hbm) = refs[:11]
    kc_hbm, vc_hbm = (None, None) if aliased else refs[11:13]
    refs = refs[14 if aliased else 13:]
    attn_ref, ko_hbm, vo_hbm = refs[:3]
    refs = refs[3:]
    kv_buf = refs[0] if aliased else refs[-1]
    k_buf, v_buf = kv_buf.at[0], kv_buf.at[1]
    refs = refs[1:] if aliased else refs[:-1]
    (x_buf, w_buf, q_f32, k_f32, v_f32, lens_col, out_f32, s_buf, x_sem, w_sem, k_sem, v_sem, ko_sem, vo_sem) = refs
    batch, slots, head = k_buf.shape
    q_width = wq_hbm.shape[2]
    n_chunks = batch // SEQ_CHUNK

    if do_norm:
        x_copy = pltpu.make_async_copy(x_hbm, x_buf, x_sem)
        x_copy.start()
    w_copies = [
        pltpu.make_async_copy(wq_hbm.at[layer], w_buf.at[:, :q_width], w_sem.at[0]),
        pltpu.make_async_copy(wk_hbm.at[layer], w_buf.at[:, q_width:q_width + head], w_sem.at[1]),
        pltpu.make_async_copy(wv_hbm.at[layer], w_buf.at[:, q_width + head:], w_sem.at[2]),
    ]
    for copy in w_copies:
        copy.start()

    def chunk_copies(idx):
        rows = pl.ds(pl.multiple_of(idx * SEQ_CHUNK, SEQ_CHUNK), SEQ_CHUNK)
        return (
            None if aliased else pltpu.make_async_copy(kc_hbm.at[layer, rows], k_buf.at[rows], k_sem.at[idx]),
            None if aliased else pltpu.make_async_copy(vc_hbm.at[layer, rows], v_buf.at[rows], v_sem.at[idx]),
            pltpu.make_async_copy(k_buf.at[rows], ko_hbm.at[layer, rows], ko_sem.at[idx]),
            pltpu.make_async_copy(v_buf.at[rows], vo_hbm.at[layer, rows], vo_sem.at[idx]),
        )

    if not aliased:
        @pl.loop(0, n_chunks)
        def _(idx):
            k_in, v_in, _, _ = chunk_copies(idx)
            k_in.start()
            v_in.start()

    lens_f = lens_row[...].astype(F32)
    same = lax.broadcasted_iota(jnp.int32, (batch, batch), 0) == lax.broadcasted_iota(jnp.int32, (batch, batch), 1)
    pos_col = jnp.sum(jnp.where(same, jnp.broadcast_to(lens_f, (batch, batch)), 0.0), axis=1, keepdims=True)
    lens_col[...] = jnp.broadcast_to(pos_col, (batch, head)).astype(jnp.int32)
    angles = pos_col * freq[...]
    cos_tab = jnp.cos(angles)
    lane = lax.broadcasted_iota(jnp.int32, (1, head), 1)
    sin_tab = jnp.sin(angles) * jnp.where(lane < head // 2, -1.0, 1.0)

    def rope(vec):
        return vec * cos_tab + pltpu.roll(vec, head // 2, 1) * sin_tab

    for copy in w_copies:
        copy.wait()
    if do_norm:
        x_copy.wait()
        normed = norm_rows(x_buf[...].astype(F32), g_ref[layer:layer + 1, :].astype(F32))
    else:
        normed = x_hbm[...]
    for col in range(q_width // head):
        cols = slice(col * head, (col + 1) * head)
        part = jnp.dot(normed, w_buf[:, cols], preferred_element_type=F32) + bq_ref[layer:layer + 1, cols].astype(F32)
        q_f32[:, cols] = rope(part).astype(BF16).astype(F32)
    part = jnp.dot(normed, w_buf[:, q_width:], preferred_element_type=F32)
    k_f32[...] = rope(part[:, :head] + bk_ref[layer:layer + 1, :].astype(F32)).astype(BF16).astype(F32)
    v_f32[...] = (part[:, head:] + bv_ref[layer:layer + 1, :].astype(F32)).astype(BF16).astype(F32)

    half = 8
    scale = head ** -0.5
    row_in_group = lax.broadcasted_iota(jnp.int32, (2 * half, head), 0) % half
    slot_id = lax.broadcasted_iota(jnp.int32, (2 * half, slots), 1)
    tile_row = lax.broadcasted_iota(jnp.int32, (16, head), 0)

    def patch(idx):
        for sub in range(SEQ_CHUNK):
            seq = idx * SEQ_CHUNK + sub
            pos = lens_smem[seq]
            base = pl.multiple_of((pos >> 4) << 4, 16)
            hit = tile_row == pos - base
            for buf, new in ((k_buf, k_f32), (v_buf, v_f32)):
                row = jnp.broadcast_to(new[pl.ds(seq, 1), :], (16, head))
                old = buf[seq, pl.ds(base, 16), :]
                buf[seq, pl.ds(base, 16), :] = jnp.where(hit, row, old.astype(F32)).astype(BF16)

    groups = SEQ_CHUNK // half

    def first_row(idx, group):
        return pl.multiple_of(idx * SEQ_CHUNK + group * half, half)

    def scores_of(idx, group):
        first = first_row(idx, group)
        q_rows = q_f32[pl.ds(first, half), :]
        q_all = jnp.concatenate([q_rows[:, :head], q_rows[:, head:]], axis=0)
        scores = jnp.zeros((2 * half, slots), F32)
        for pair in range(half // 2):
            lhs = jnp.concatenate([jnp.where(row_in_group == 2 * pair + e, q_all, 0.0) for e in range(2)], axis=1).astype(BF16)
            rhs = jnp.concatenate([k_buf[first + 2 * pair + e] for e in range(2)], axis=1)
            scores += lax.dot_general(lhs, rhs, NT, preferred_element_type=F32)
        return scores

    def probs_of(idx, group):
        pos_rows = lens_col[pl.ds(first_row(idx, group), half), 0:1]
        pos_all = jnp.concatenate([pos_rows, pos_rows], axis=0)
        scores = jnp.where(slot_id <= pos_all, s_buf[group] * scale, -1e30)
        expo = jnp.exp(scores - jnp.max(scores, axis=-1, keepdims=True))
        return (expo / jnp.sum(expo, axis=-1, keepdims=True)).astype(BF16)

    def values_of(idx, group, probs):
        first = first_row(idx, group)
        out = jnp.zeros((2 * half, head), F32)
        for pair in range(half // 2):
            rhs = jnp.concatenate([v_buf[first + 2 * pair + e] for e in range(2)], axis=1)
            both = jnp.dot(probs, rhs, preferred_element_type=F32)
            for e in range(2):
                out = jnp.where(row_in_group == 2 * pair + e, both[:, e * head:(e + 1) * head], out)
        return jnp.concatenate([out[:half], out[half:]], axis=1)

    s_buf[...] = jnp.zeros_like(s_buf)

    @pl.loop(0, n_chunks + 1)
    def _(idx):
        @pl.when(idx < n_chunks)
        def _():
            k_in, v_in, k_out, v_out = chunk_copies(idx)
            if not aliased:
                k_in.wait()
                v_in.wait()
            patch(idx)
            k_out.start()
            v_out.start()

        now = jnp.maximum(idx - 1, 0)
        later = jnp.minimum(idx, n_chunks - 1)
        new_scores = [scores_of(later, group) for group in range(groups)]
        probs = [probs_of(now, group) for group in range(groups)]
        outs = [values_of(now, group, probs[group]) for group in range(groups)]
        for group in range(groups):
            s_buf[group] = new_scores[group]
            out_f32[pl.ds(first_row(now, group), half), :] = outs[group]

    attn_ref[...] = out_f32[...].astype(BF16)

    @pl.loop(0, n_chunks)
    def _(idx):
        _, _, k_out, v_out = chunk_copies(idx)
        k_out.wait()
        v_out.wait()


def in_hbm(*arrays):
    return [pltpu.with_memory_space_constraint(a, pltpu.HBM) for a in arrays]


def in_vmem(*arrays):
    return [pltpu.with_memory_space_constraint(a, pltpu.VMEM) for a in arrays]


def attn_call(layer, do_norm, lens, freq, x_in, gain, b_q, b_k, b_v, w_q, w_k, w_v, caches, prev):
    batch, slots, head = caches[0].shape[-3:]
    width = x_in.shape[1]
    q_width = w_q.shape[2]
    any_spec = pl.BlockSpec(memory_space=pltpu.HBM)
    vmem = pl.BlockSpec(memory_space=pltpu.VMEM)
    aliased = prev is not None
    place = in_hbm if do_norm else in_vmem
    args = [lens, lens.reshape(1, batch), freq, *place(x_in), gain, b_q, b_k, b_v, *in_hbm(w_q, w_k, w_v), *place(*caches)]
    in_specs = [pl.BlockSpec(memory_space=pltpu.SMEM), vmem, vmem, any_spec if do_norm else vmem, vmem, vmem, vmem, vmem] + [any_spec] * 5
    aliases = {}
    if aliased:
        aliases = {len(args): 1, len(args) + 1: 2, len(args) - 1: 3}
        args += in_hbm(*prev)
        in_specs = in_specs[:-2] + [vmem] + [any_spec] * 2
    cache_buf = pltpu.VMEM((2, batch, slots, head), BF16)
    out_cache = jax.ShapeDtypeStruct((w_q.shape[0], batch, slots, head), BF16)
    n_chunks = batch // SEQ_CHUNK
    macs = batch * width * (q_width + 2 * head) + 2 * batch * slots * q_width
    return pl.pallas_call(
        functools.partial(attn_kernel, layer, do_norm, aliased),
        out_shape=(
            pltpu.VMEM((batch, q_width), BF16),
            out_cache,
            out_cache,
        ) + ((cache_buf,) if aliased else ()),
        in_specs=in_specs,
        out_specs=(vmem, any_spec, any_spec) + ((vmem,) if aliased else ()),
        scratch_shapes=[
            pltpu.VMEM((batch, width), BF16),
            pltpu.VMEM((width, q_width + 2 * head), BF16),
            pltpu.VMEM((batch, q_width), F32),
            pltpu.VMEM((batch, head), F32),
            pltpu.VMEM((batch, head), F32),
            pltpu.VMEM((batch, head), jnp.int32),
            pltpu.VMEM((batch, q_width), F32),
            pltpu.VMEM((SEQ_CHUNK // 8, 16, slots), F32),
            pltpu.SemaphoreType.DMA,
            pltpu.SemaphoreType.DMA((3,)),
            pltpu.SemaphoreType.DMA((n_chunks,)),
            pltpu.SemaphoreType.DMA((n_chunks,)),
            pltpu.SemaphoreType.DMA((n_chunks,)),
            pltpu.SemaphoreType.DMA((n_chunks,)),
        ] + ([] if aliased else [cache_buf]),
        input_output_aliases=aliases,
        compiler_params=pltpu.CompilerParams(vmem_limit_bytes=ATTN_VMEM + (0 if aliased else 4 * batch * slots * head)),
        cost_estimate=pl.CostEstimate(flops=2 * macs, bytes_accessed=4 * batch * slots * head * 2, transcendentals=batch * slots * 2),
        name=f"attn{layer}",
    )(*args)[:3]


def mix_kernel(layer, last, attn_ref, x_hbm, gm_ref, gn_ref, wo_hbm, wg_hbm, wu_hbm, wd_hbm, kc_hbm, vc_hbm, *refs):
    if last:
        out_hbm = refs[0]
        refs = refs[1:]
    else:
        out_hbm, xs_ref, kv_next = refs[:3]
        refs = refs[3:]
    (wo, wg, wu, wd, x_own, act, d_send, d_recv, own, r_send, r_recv, gathered,
     w_sem, x_sem, ds_sem, dr_sem, rs_sem, rr_sem, as_sem, ar_sem, fs_sem, fr_sem, o_sem, c_sem) = refs
    width = wo.shape[1]
    hidden = wg.shape[1]
    rows = attn_ref.shape[0] // ROW_CHUNKS
    core_rows = rows // 2
    blk = core_rows // 4
    me = lax.axis_index("tp")
    core = me % 2
    chip = me // 2
    partner = me + 1 - 2 * core
    peer_y = (chip + 2) % 4
    peers = [chip, 3 - peer_y, peer_y, 3 - chip]

    def dev(idx):
        return {"tp": idx}

    w_copies = [pltpu.make_async_copy(src.at[layer], dst, w_sem.at[i])
                for i, (src, dst) in enumerate(((wo_hbm, wo), (wg_hbm, wg), (wu_hbm, wu), (wd_hbm, wd)))]
    w_copies[0].start()

    def own_row(j):
        return pl.multiple_of(j * rows + core * core_rows + chip * blk, blk)

    x_copies = []
    for j in range(ROW_CHUNKS):
        if layer:
            x_own[j] = x_hbm[j]
        else:
            x_copies.append(pltpu.make_async_copy(x_hbm.at[pl.ds(own_row(j), blk)], x_own.at[j], x_sem.at[j]))
            x_copies[-1].start()

    c_copies = []
    if not last:
        parts = c_sem.shape[1]
        size = kv_next.shape[1] // parts
        for i, src in enumerate((kc_hbm, vc_hbm)):
            for n in range(parts):
                part = pl.ds(n * size, size)
                c_copies.append(pltpu.make_async_copy(src.at[layer + 1, part], kv_next.at[i, part], c_sem.at[i, n]))

    def prefetch(count):
        for _ in range(min(count, len(waiting))):
            waiting.pop(0).start()

    waiting = list(c_copies)
    barrier = pltpu.get_barrier_semaphore()
    others = [partner] + [2 * peers[r] + core for r in range(1, 4)]
    for other in others:
        pl.semaphore_signal(barrier, inc=1, device_id=dev(other), device_id_type=pl.DeviceIdType.MESH)

    def remote(src, dst, send, recv, target):
        return pltpu.make_async_remote_copy(src_ref=src, dst_ref=dst, send_sem=send, recv_sem=recv,
                                            device_id=dev(target), device_id_type=pl.DeviceIdType.MESH)

    def share(s, j, lhs, weight):
        step = 512

        @pl.loop(0, width // step)
        def _(n):
            cols = pl.ds(pl.multiple_of(n * step, step), step)
            part = jnp.dot(lhs, weight[:, cols], preferred_element_type=F32)
            act_dst = own.at[s, j]
            act_dst[:, cols] = part
        other_half = pl.multiple_of((1 - core) * core_rows, core_rows)
        d_send[s, j] = own[s, j, pl.ds(other_half, core_rows), :].astype(BF16)

    def d_copy(s, j):
        return remote(d_send.at[s, j], d_recv.at[s, j], ds_sem.at[s, j], dr_sem.at[s, j], partner)

    def r_copy(s, j, r):
        return remote(r_send.at[s, j, r], r_recv.at[s, j, r], rs_sem.at[s, j, r], rr_sem.at[s, j, r], 2 * peers[r] + core)

    def scatter(s, j):
        d_copy(s, j).wait()
        for r in (3, 1, 2):
            off = pl.multiple_of(peers[r] * blk, blk)
            mine = own[s, j, pl.ds(core * core_rows + off, blk), :]
            r_send[s, j, r] = (mine + d_recv[s, j, pl.ds(off, blk), :].astype(F32)).astype(BF16)
            r_copy(s, j, r).start()

    def reduce(s, j):
        off = pl.multiple_of(chip * blk, blk)
        total = own[s, j, pl.ds(core * core_rows + off, blk), :] + d_recv[s, j, pl.ds(off, blk), :].astype(F32)
        for r in (1, 2, 3):
            r_copy(s, j, r).wait()
            total += r_recv[s, j, r].astype(F32)
        new = (x_own[j].astype(F32) + total).astype(BF16)
        x_own[j] = new
        return new

    def block_row(j, cc, k):
        return pl.ds(pl.multiple_of(j * rows + cc * core_rows + k * blk, blk), blk)

    def a_copy(s, j, r):
        here = block_row(j, core, chip)
        target = partner if r == 0 else 2 * peers[r] + core
        return remote(gathered.at[s, here], gathered.at[s, here], as_sem.at[s, j, r], ar_sem.at[s, j, r], target)

    def f_copy(s, j, r):
        here = block_row(j, core, peers[r])
        return remote(gathered.at[s, here], gathered.at[s, here], fs_sem.at[s, j, r], fr_sem.at[s, j, r], partner)

    def gather_start(s, j, value):
        gathered[s, block_row(j, core, chip), :] = value
        for r in (3, 1, 2, 0):
            a_copy(s, j, r).start()

    def gather_finish(s, j):
        for r in (1, 2, 3):
            a_copy(s, j, r).wait_recv()
            f_copy(s, j, r).start()
        a_copy(s, j, 0).wait_recv()
        for r in (1, 2, 3):
            f_copy(s, j, r).wait_recv()

    w_copies[0].wait()
    for j in range(ROW_CHUNKS):
        share(0, j, attn_ref[j * rows:(j + 1) * rows, :], wo)
        if j == 0:
            pl.semaphore_wait(barrier, len(others))
        d_copy(0, j).start()
    for copy in x_copies:
        copy.wait()
    for j in range(ROW_CHUNKS):
        scatter(0, j)
    for copy in w_copies[1:]:
        copy.start()
    for j in range(ROW_CHUNKS):
        new = reduce(0, j)
        gather_start(0, j, norm_rows(new.astype(F32), gm_ref[layer:layer + 1, :].astype(F32)))
    prefetch(4)
    for copy in w_copies[1:]:
        copy.wait()
    for j in range(ROW_CHUNKS):
        gather_finish(0, j)
        prefetch(2)
        step = 256

        @pl.loop(0, hidden // step)
        def _(n):
            cols = pl.ds(pl.multiple_of(n * step, step), step)
            lhs = gathered[0, j * rows:(j + 1) * rows, :]
            gate = jnp.dot(lhs, wg[:, cols], preferred_element_type=F32)
            up = jnp.dot(lhs, wu[:, cols], preferred_element_type=F32)
            act[j, :, cols] = (gate * jax.nn.sigmoid(gate) * up).astype(BF16)
        share(1, j, act[j], wd)
        d_copy(1, j).start()
    for j in range(ROW_CHUNKS):
        scatter(1, j)
    prefetch(4)
    outs = []
    for j in range(ROW_CHUNKS):
        new = reduce(1, j)
        if last:
            gather_start(1, j, new)
        else:
            xs_ref[j] = new
            gather_start(1, j, norm_rows(new.astype(F32), gn_ref[layer + 1:layer + 2, :].astype(F32)))
    prefetch(len(waiting))
    for j in range(ROW_CHUNKS):
        gather_finish(1, j)
        here = pl.ds(j * rows, rows)
        if last:
            outs.append(pltpu.make_async_copy(gathered.at[1, here], out_hbm.at[here], o_sem.at[j]))
            outs[-1].start()
        else:
            out_hbm[here, :] = gathered[1, here, :]
    for s in range(2):
        for j in range(ROW_CHUNKS):
            for r in range(4):
                a_copy(s, j, r).wait_send()
            for r in range(1, 4):
                f_copy(s, j, r).wait_send()
    for copy in outs + c_copies:
        copy.wait()


def mix_call(layer, last, attn, x_own, g_mlp, g_attn, w_o, w_gate, w_up, w_down, k_cache, v_cache):
    batch = attn.shape[0]
    depth, width = w_o.shape[1:]
    hidden = w_gate.shape[2]
    rows = batch // ROW_CHUNKS
    blk = rows // 8
    any_spec = pl.BlockSpec(memory_space=pltpu.HBM)
    vmem = pl.BlockSpec(memory_space=pltpu.VMEM)
    if last:
        out_shape = [jax.ShapeDtypeStruct((batch, width), BF16)]
        out_specs = [any_spec]
    else:
        out_shape = [pltpu.VMEM((batch, width), BF16), pltpu.VMEM((ROW_CHUNKS, blk, width), BF16)]
        out_shape.append(pltpu.VMEM((2,) + k_cache.shape[1:], BF16))
        out_specs = [vmem] * 3
    sem = pltpu.SemaphoreType.DMA
    nc = ROW_CHUNKS
    return pl.pallas_call(
        functools.partial(mix_kernel, layer, last),
        out_shape=out_shape,
        in_specs=[vmem, any_spec if layer == 0 else vmem, vmem, vmem] + [any_spec] * 6,
        out_specs=out_specs,
        scratch_shapes=[
            pltpu.VMEM((depth, width), BF16),
            pltpu.VMEM((width, hidden), BF16),
            pltpu.VMEM((width, hidden), BF16),
            pltpu.VMEM((hidden, width), BF16),
            pltpu.VMEM((nc, blk, width), BF16),
            pltpu.VMEM((nc, rows, hidden), BF16),
            pltpu.VMEM((2, nc, rows // 2, width), BF16),
            pltpu.VMEM((2, nc, rows // 2, width), BF16),
            pltpu.VMEM((2, nc, rows, width), F32),
            pltpu.VMEM((2, nc, 4, blk, width), BF16),
            pltpu.VMEM((2, nc, 4, blk, width), BF16),
            pltpu.VMEM((2, batch, width), BF16),
            sem((4,)), sem((nc,)),
            sem((2, nc)), sem((2, nc)),
            sem((2, nc, 4)), sem((2, nc, 4)),
            sem((2, nc, 4)), sem((2, nc, 4)),
            sem((2, nc, 4)), sem((2, nc, 4)),
            sem((nc,)), sem((2, 8)),
        ],
        compiler_params=pltpu.CompilerParams(collective_id=layer, has_side_effects=True, vmem_limit_bytes=MIX_VMEM),
        cost_estimate=pl.CostEstimate(flops=2 * batch * width * (depth + 3 * hidden), bytes_accessed=2 * width * (depth + 3 * hidden), transcendentals=batch * hidden),
        name=f"mix{layer}",
    )(*in_vmem(attn), *(in_hbm if layer == 0 else in_vmem)(x_own), g_mlp, g_attn, *in_hbm(w_o, w_gate, w_up, w_down, k_cache, v_cache))


def solution(mesh):
    weight_col = P(None, None, "tp")
    weight_row = P(None, "tp", None)
    bias_col = P(None, "tp")
    cache_spec = P(None, "dp", None, "tp", None)
    in_specs = (P("dp", None), P("dp"), P(None, None), P(None, None), weight_col, bias_col, weight_col, bias_col, weight_col, bias_col, weight_row, weight_col, weight_col, weight_row, cache_spec, cache_spec)
    out_specs = (P("dp", None), cache_spec, cache_spec)

    def local_step(x_in, seq_lens, g_attn, g_mlp, w_q, b_q, w_k, b_k, w_v, b_v, w_o, w_gate, w_up, w_down, k_cache, v_cache):
        layers, batch, slots, _, head = k_cache.shape
        inv_freq = ROPE_THETA ** (-2.0 * np.arange(head // 2) / head)
        freq = jnp.asarray(np.concatenate([inv_freq, inv_freq])[None, :].astype(np.float32))
        k_flat = k_cache.reshape(layers, batch, slots, head)
        v_flat = v_cache.reshape(layers, batch, slots, head)
        normed, x_own, prev = x_in, x_in, None
        caches = (k_flat, v_flat)
        for layer in range(layers):
            last = layer == layers - 1
            attn, k_out, v_out = attn_call(layer, layer == 0, seq_lens, freq, normed, g_attn, b_q, b_k, b_v, w_q, w_k, w_v, caches, prev)
            prev = (k_out, v_out)
            outs = mix_call(layer, last, attn, x_own, g_mlp, g_attn, w_o, w_gate, w_up, w_down, k_flat, v_flat)
            if last:
                x_out = outs[0]
            else:
                normed, x_own, caches = outs[0], outs[1], outs[2:]
        return x_out, prev[0].reshape(k_cache.shape), prev[1].reshape(v_cache.shape)

    return jax.shard_map(local_step, mesh=mesh, in_specs=in_specs, out_specs=out_specs, check_vma=False)
```

```python
import functools
import math

import jax
import jax.numpy as jnp
import numpy as np
from jax import lax
from jax.experimental import pallas as pl
from jax.experimental.pallas import tpu as pltpu
from jax.sharding import PartitionSpec as P

ROPE_THETA = 1000000.0
EPS = 1e-6
F32 = jnp.float32
BF16 = jnp.bfloat16
NT = (((1,), (1,)), ((), ()))
SEQ_CHUNK = 16
ROW_CHUNKS = 4
MLP_CHUNKS = 2
ATTN_VMEM = 24 * 1024 * 1024
MIX_VMEM = 22 * 1024 * 1024


def norm_rows(vec_f32, gain_row):
    mean_sq = jnp.mean(vec_f32 * vec_f32, axis=-1, keepdims=True)
    return (vec_f32 * lax.rsqrt(mean_sq + EPS) * gain_row).astype(BF16)


def attn_kernel(layer, do_norm, aliased, *refs):
    (lens_smem, lens_row, freq, x_hbm, g_ref, bq_ref, bk_ref, bv_ref, wq_hbm, wk_hbm, wv_hbm) = refs[:11]
    kc_hbm, vc_hbm = (None, None) if aliased else refs[11:13]
    refs = refs[14 if aliased else 13:]
    attn_ref, ko_hbm, vo_hbm = refs[:3]
    refs = refs[3:]
    kv_buf = refs[0] if aliased else refs[-1]
    k_buf, v_buf = kv_buf.at[0], kv_buf.at[1]
    refs = refs[1:] if aliased else refs[:-1]
    (x_buf, w_buf, q_f32, k_f32, v_f32, lens_col, out_f32, s_buf, x_sem, w_sem, k_sem, v_sem, ko_sem, vo_sem) = refs
    batch, slots, head = k_buf.shape
    q_width = wq_hbm.shape[2]
    n_chunks = batch // SEQ_CHUNK

    if do_norm:
        x_copy = pltpu.make_async_copy(x_hbm, x_buf, x_sem)
        x_copy.start()
    w_copies = [
        pltpu.make_async_copy(wq_hbm.at[layer], w_buf.at[:, :q_width], w_sem.at[0]),
        pltpu.make_async_copy(wk_hbm.at[layer], w_buf.at[:, q_width:q_width + head], w_sem.at[1]),
        pltpu.make_async_copy(wv_hbm.at[layer], w_buf.at[:, q_width + head:], w_sem.at[2]),
    ]
    for copy in w_copies:
        copy.start()

    def chunk_copies(idx):
        rows = pl.ds(pl.multiple_of(idx * SEQ_CHUNK, SEQ_CHUNK), SEQ_CHUNK)
        return (
            None if aliased else pltpu.make_async_copy(kc_hbm.at[layer, rows], k_buf.at[rows], k_sem.at[idx]),
            None if aliased else pltpu.make_async_copy(vc_hbm.at[layer, rows], v_buf.at[rows], v_sem.at[idx]),
            pltpu.make_async_copy(k_buf.at[rows], ko_hbm.at[layer, rows], ko_sem.at[idx]),
            pltpu.make_async_copy(v_buf.at[rows], vo_hbm.at[layer, rows], vo_sem.at[idx]),
        )

    if not aliased:
        @pl.loop(0, n_chunks)
        def _(idx):
            k_in, v_in, _, _ = chunk_copies(idx)
            k_in.start()
            v_in.start()

    lens_f = lens_row[...].astype(F32)
    same = lax.broadcasted_iota(jnp.int32, (batch, batch), 0) == lax.broadcasted_iota(jnp.int32, (batch, batch), 1)
    pos_col = jnp.sum(jnp.where(same, jnp.broadcast_to(lens_f, (batch, batch)), 0.0), axis=1, keepdims=True)
    lens_col[...] = jnp.broadcast_to(pos_col, (batch, head)).astype(jnp.int32)
    angles = pos_col * freq[...]
    cos_tab = jnp.cos(angles)
    lane = lax.broadcasted_iota(jnp.int32, (1, head), 1)
    sin_tab = jnp.sin(angles) * jnp.where(lane < head // 2, -1.0, 1.0)

    def rope(vec):
        return vec * cos_tab + pltpu.roll(vec, head // 2, 1) * sin_tab

    for copy in w_copies:
        copy.wait()
    if do_norm:
        x_copy.wait()
        normed = norm_rows(x_buf[...].astype(F32), g_ref[layer:layer + 1, :].astype(F32))
    else:
        normed = x_hbm[...]
    for col in range(q_width // head):
        cols = slice(col * head, (col + 1) * head)
        part = jnp.dot(normed, w_buf[:, cols], preferred_element_type=F32) + bq_ref[layer:layer + 1, cols].astype(F32)
        q_f32[:, cols] = rope(part).astype(BF16).astype(F32)
    part = jnp.dot(normed, w_buf[:, q_width:], preferred_element_type=F32)
    k_f32[...] = rope(part[:, :head] + bk_ref[layer:layer + 1, :].astype(F32)).astype(BF16).astype(F32)
    v_f32[...] = (part[:, head:] + bv_ref[layer:layer + 1, :].astype(F32)).astype(BF16).astype(F32)

    half = 8
    scale = head ** -0.5
    row_in_group = lax.broadcasted_iota(jnp.int32, (2 * half, head), 0) % half
    slot_id = lax.broadcasted_iota(jnp.int32, (2 * half, slots), 1)
    tile_row = lax.broadcasted_iota(jnp.int32, (16, head), 0)

    def patch(idx):
        for sub in range(SEQ_CHUNK):
            seq = idx * SEQ_CHUNK + sub
            pos = lens_smem[seq]
            base = pl.multiple_of((pos >> 4) << 4, 16)
            hit = tile_row == pos - base
            for buf, new in ((k_buf, k_f32), (v_buf, v_f32)):
                row = jnp.broadcast_to(new[pl.ds(seq, 1), :], (16, head))
                old = buf[seq, pl.ds(base, 16), :]
                buf[seq, pl.ds(base, 16), :] = jnp.where(hit, row, old.astype(F32)).astype(BF16)

    groups = SEQ_CHUNK // half

    def first_row(idx, group):
        return pl.multiple_of(idx * SEQ_CHUNK + group * half, half)

    def scores_of(idx, group):
        first = first_row(idx, group)
        q_rows = q_f32[pl.ds(first, half), :]
        q_all = jnp.concatenate([q_rows[:, :head], q_rows[:, head:]], axis=0)
        scores = jnp.zeros((2 * half, slots), F32)
        for pair in range(half // 2):
            lhs = jnp.concatenate([jnp.where(row_in_group == 2 * pair + e, q_all, 0.0) for e in range(2)], axis=1).astype(BF16)
            rhs = jnp.concatenate([k_buf[first + 2 * pair + e] for e in range(2)], axis=1)
            scores += lax.dot_general(lhs, rhs, NT, preferred_element_type=F32)
        return scores

    def probs_of(idx, group):
        pos_rows = lens_col[pl.ds(first_row(idx, group), half), 0:1]
        pos_all = jnp.concatenate([pos_rows, pos_rows], axis=0)
        scores = jnp.where(slot_id <= pos_all, s_buf[group] * scale, -1e30)
        expo = jnp.exp(scores - jnp.max(scores, axis=-1, keepdims=True))
        return (expo / jnp.sum(expo, axis=-1, keepdims=True)).astype(BF16)

    def values_of(idx, group, probs):
        first = first_row(idx, group)
        out = jnp.zeros((2 * half, head), F32)
        for pair in range(half // 2):
            rhs = jnp.concatenate([v_buf[first + 2 * pair + e] for e in range(2)], axis=1)
            both = jnp.dot(probs, rhs, preferred_element_type=F32)
            for e in range(2):
                out = jnp.where(row_in_group == 2 * pair + e, both[:, e * head:(e + 1) * head], out)
        return jnp.concatenate([out[:half], out[half:]], axis=1)

    s_buf[...] = jnp.zeros_like(s_buf)

    @pl.loop(0, n_chunks + 1)
    def _(idx):
        @pl.when(idx < n_chunks)
        def _():
            k_in, v_in, k_out, v_out = chunk_copies(idx)
            if not aliased:
                k_in.wait()
                v_in.wait()
            patch(idx)
            k_out.start()
            v_out.start()

        now = jnp.maximum(idx - 1, 0)
        later = jnp.minimum(idx, n_chunks - 1)
        new_scores = [scores_of(later, group) for group in range(groups)]
        probs = [probs_of(now, group) for group in range(groups)]
        outs = [values_of(now, group, probs[group]) for group in range(groups)]
        for group in range(groups):
            s_buf[group] = new_scores[group]
            out_f32[pl.ds(first_row(now, group), half), :] = outs[group]

    attn_ref[...] = out_f32[...].astype(BF16)

    @pl.loop(0, n_chunks)
    def _(idx):
        _, _, k_out, v_out = chunk_copies(idx)
        k_out.wait()
        v_out.wait()


def in_hbm(*arrays):
    return [pltpu.with_memory_space_constraint(a, pltpu.HBM) for a in arrays]


def in_vmem(*arrays):
    return [pltpu.with_memory_space_constraint(a, pltpu.VMEM) for a in arrays]


def attn_call(layer, do_norm, lens, freq, x_in, gain, b_q, b_k, b_v, w_q, w_k, w_v, caches, prev):
    batch, slots, head = caches[0].shape[-3:]
    width = x_in.shape[1]
    q_width = w_q.shape[2]
    any_spec = pl.BlockSpec(memory_space=pltpu.HBM)
    vmem = pl.BlockSpec(memory_space=pltpu.VMEM)
    aliased = prev is not None
    place = in_hbm if do_norm else in_vmem
    args = [lens, lens.reshape(1, batch), freq, *place(x_in), gain, b_q, b_k, b_v, *in_hbm(w_q, w_k, w_v), *place(*caches)]
    in_specs = [pl.BlockSpec(memory_space=pltpu.SMEM), vmem, vmem, any_spec if do_norm else vmem, vmem, vmem, vmem, vmem] + [any_spec] * 5
    aliases = {}
    if aliased:
        aliases = {len(args): 1, len(args) + 1: 2, len(args) - 1: 3}
        args += in_hbm(*prev)
        in_specs = in_specs[:-2] + [vmem] + [any_spec] * 2
    cache_buf = pltpu.VMEM((2, batch, slots, head), BF16)
    out_cache = jax.ShapeDtypeStruct((w_q.shape[0], batch, slots, head), BF16)
    n_chunks = batch // SEQ_CHUNK
    macs = batch * width * (q_width + 2 * head) + 2 * batch * slots * q_width
    return pl.pallas_call(
        functools.partial(attn_kernel, layer, do_norm, aliased),
        out_shape=(
            pltpu.VMEM((batch, q_width), BF16),
            out_cache,
            out_cache,
        ) + ((cache_buf,) if aliased else ()),
        in_specs=in_specs,
        out_specs=(vmem, any_spec, any_spec) + ((vmem,) if aliased else ()),
        scratch_shapes=[
            pltpu.VMEM((batch, width), BF16),
            pltpu.VMEM((width, q_width + 2 * head), BF16),
            pltpu.VMEM((batch, q_width), F32),
            pltpu.VMEM((batch, head), F32),
            pltpu.VMEM((batch, head), F32),
            pltpu.VMEM((batch, head), jnp.int32),
            pltpu.VMEM((batch, q_width), F32),
            pltpu.VMEM((SEQ_CHUNK // 8, 16, slots), F32),
            pltpu.SemaphoreType.DMA,
            pltpu.SemaphoreType.DMA((3,)),
            pltpu.SemaphoreType.DMA((n_chunks,)),
            pltpu.SemaphoreType.DMA((n_chunks,)),
            pltpu.SemaphoreType.DMA((n_chunks,)),
            pltpu.SemaphoreType.DMA((n_chunks,)),
        ] + ([] if aliased else [cache_buf]),
        input_output_aliases=aliases,
        compiler_params=pltpu.CompilerParams(vmem_limit_bytes=ATTN_VMEM + (0 if aliased else 4 * batch * slots * head)),
        cost_estimate=pl.CostEstimate(flops=2 * macs, bytes_accessed=4 * batch * slots * head * 2, transcendentals=batch * slots * 2),
        name=f"attn{layer}",
    )(*args)[:3]


def mix_kernel(layer, last, attn_ref, x_hbm, gm_ref, gn_ref, wo_hbm, wg_hbm, wu_hbm, wd_hbm, kc_hbm, vc_hbm, *refs):
    if last:
        out_hbm = refs[0]
        refs = refs[1:]
    else:
        out_hbm, xs_ref, kv_next = refs[:3]
        refs = refs[3:]
    (wo, wg, wu, wd, x_own, act, d_send, d_recv, own, r_send, r_recv, gathered,
     w_sem, x_sem, ds_sem, dr_sem, rs_sem, rr_sem, as_sem, ar_sem, fs_sem, fr_sem, o_sem, c_sem) = refs
    width = wo.shape[1]
    hidden = wg.shape[1]
    rows = attn_ref.shape[0] // ROW_CHUNKS
    core_rows = rows // 2
    blk = core_rows // 4
    me = lax.axis_index("tp")
    core = me % 2
    chip = me // 2
    partner = me + 1 - 2 * core
    peer_y = (chip + 2) % 4
    peers = [chip, 3 - peer_y, peer_y, 3 - chip]

    def dev(idx):
        return {"tp": idx}

    w_copies = [pltpu.make_async_copy(src.at[layer], dst, w_sem.at[i])
                for i, (src, dst) in enumerate(((wo_hbm, wo), (wg_hbm, wg), (wu_hbm, wu), (wd_hbm, wd)))]
    w_copies[0].start()

    def own_rows(j):
        return pl.ds(pl.multiple_of(j * rows + core * core_rows + chip * blk, blk), blk)

    x_copies = []
    for j in range(ROW_CHUNKS):
        if layer:
            x_own[j] = x_hbm[j]
        else:
            x_copies.append(pltpu.make_async_copy(x_hbm.at[own_rows(j)], x_own.at[j], x_sem.at[j]))
            x_copies[-1].start()

    c_copies = []
    if not last:
        parts = c_sem.shape[1]
        size = kv_next.shape[1] // parts
        for i, src in enumerate((kc_hbm, vc_hbm)):
            for n in range(parts):
                part = pl.ds(n * size, size)
                c_copies.append(pltpu.make_async_copy(src.at[layer + 1, part], kv_next.at[i, part], c_sem.at[i, n]))

    def prefetch(count):
        for _ in range(min(count, len(waiting))):
            waiting.pop(0).start()

    waiting = list(c_copies)
    prefetch(2)
    barrier = pltpu.get_barrier_semaphore()
    others = [partner] + [2 * peers[r] + core for r in range(1, 4)]
    for other in others:
        pl.semaphore_signal(barrier, inc=1, device_id=dev(other), device_id_type=pl.DeviceIdType.MESH)

    def remote(src, dst, send, recv, target):
        return pltpu.make_async_remote_copy(src_ref=src, dst_ref=dst, send_sem=send, recv_sem=recv,
                                            device_id=dev(target), device_id_type=pl.DeviceIdType.MESH)

    def share(s, first, count, lhs, weight):
        step = 512
        here = pl.ds(first * rows, count * rows)

        @pl.loop(0, width // step)
        def _(n):
            cols = pl.ds(pl.multiple_of(n * step, step), step)
            own[s, here, cols] = jnp.dot(lhs, weight[:, cols], preferred_element_type=F32)

        for j in range(first, first + count):
            d_send[s, j] = own[s, pl.ds(pl.multiple_of(j * rows + (1 - core) * core_rows, core_rows), core_rows), :].astype(BF16)

    def d_copy(s, j):
        return remote(d_send.at[s, j], d_recv.at[s, j], ds_sem.at[s, j], dr_sem.at[s, j], partner)

    def r_copy(s, j, r):
        return remote(r_send.at[s, j, r], r_recv.at[s, j, r], rs_sem.at[s, j, r], rr_sem.at[s, j, r], 2 * peers[r] + core)

    def scatter(s, j):
        d_copy(s, j).wait()
        for r in (3, 1, 2):
            off = pl.multiple_of(peers[r] * blk, blk)
            mine = own[s, pl.ds(pl.multiple_of(j * rows + core * core_rows + off, blk), blk), :]
            r_send[s, j, r] = (mine + d_recv[s, j, pl.ds(off, blk), :].astype(F32)).astype(BF16)
            r_copy(s, j, r).start()

    def reduce(s, j):
        off = pl.multiple_of(chip * blk, blk)
        total = own[s, own_rows(j), :] + d_recv[s, j, pl.ds(off, blk), :].astype(F32)
        for r in (1, 2, 3):
            r_copy(s, j, r).wait()
            total += r_recv[s, j, r].astype(F32)
        new = (x_own[j].astype(F32) + total).astype(BF16)
        x_own[j] = new
        return new

    def block_row(j, cc, k):
        return pl.ds(pl.multiple_of(j * rows + cc * core_rows + k * blk, blk), blk)

    def a_copy(s, j, r):
        here = block_row(j, core, chip)
        target = partner if r == 0 else 2 * peers[r] + core
        return remote(gathered.at[s, here], gathered.at[s, here], as_sem.at[s, j, r], ar_sem.at[s, j, r], target)

    def f_copy(s, j, r):
        here = block_row(j, core, peers[r])
        return remote(gathered.at[s, here], gathered.at[s, here], fs_sem.at[s, j, r], fr_sem.at[s, j, r], partner)

    def gather_start(s, j, value):
        gathered[s, block_row(j, core, chip), :] = value
        for r in (3, 1, 2, 0):
            a_copy(s, j, r).start()

    def gather_forward(s, j):
        for r in (1, 2, 3):
            a_copy(s, j, r).wait_recv()
            f_copy(s, j, r).start()

    def gather_finish(s, j):
        a_copy(s, j, 0).wait_recv()
        for r in (1, 2, 3):
            f_copy(s, j, r).wait_recv()

    chunks = range(ROW_CHUNKS)
    per = MLP_CHUNKS
    w_copies[0].wait()
    for first in range(0, ROW_CHUNKS, per):
        share(0, first, per, attn_ref[first * rows:(first + per) * rows, :], wo)
        if first == 0:
            pl.semaphore_wait(barrier, len(others))
        for j in range(first, first + per):
            d_copy(0, j).start()
    for copy in x_copies:
        copy.wait()
    for j in chunks:
        scatter(0, j)
    for copy in w_copies[1:]:
        copy.start()
    for j in chunks:
        new = reduce(0, j)
        gather_start(0, j, norm_rows(new.astype(F32), gm_ref[layer:layer + 1, :].astype(F32)))
    prefetch(3)

    def mlp(first):
        here = slice(first * rows, (first + per) * rows)
        step = 256

        @pl.loop(0, hidden // step)
        def _(n):
            cols = pl.ds(pl.multiple_of(n * step, step), step)
            lhs = gathered[0, here, :]
            gate = jnp.dot(lhs, wg[:, cols], preferred_element_type=F32)
            up = jnp.dot(lhs, wu[:, cols], preferred_element_type=F32)
            act[here, cols] = (gate * jax.nn.sigmoid(gate) * up).astype(BF16)
        share(1, first, per, act[here, :], wd)
        for j in range(first, first + per):
            d_copy(1, j).start()

    for j in range(per):
        gather_forward(0, j)
    for copy in w_copies[1:]:
        copy.wait()
    for first in range(0, ROW_CHUNKS, per):
        for j in range(first, first + per):
            gather_finish(0, j)
        prefetch(3)
        mlp(first)
        for j in range(first + per, min(first + 2 * per, ROW_CHUNKS)):
            gather_forward(0, j)
        for j in range(first, first + per):
            scatter(1, j)

    def second(j):
        new = reduce(1, j)
        if last:
            gather_start(1, j, new)
        else:
            xs_ref[j] = new
            gather_start(1, j, norm_rows(new.astype(F32), gn_ref[layer + 1:layer + 2, :].astype(F32)))

    prefetch(1)
    for j in chunks:
        second(j)
    prefetch(4)
    for j in chunks:
        gather_forward(1, j)
    prefetch(len(waiting))
    outs = []
    for j in chunks:
        gather_finish(1, j)
        here = pl.ds(j * rows, rows)
        if last:
            outs.append(pltpu.make_async_copy(gathered.at[1, here], out_hbm.at[here], o_sem.at[j]))
            outs[-1].start()
        else:
            out_hbm[here, :] = gathered[1, here, :]
    for s in range(2):
        for j in range(ROW_CHUNKS):
            for r in range(4):
                a_copy(s, j, r).wait_send()
            for r in range(1, 4):
                f_copy(s, j, r).wait_send()
    for copy in outs + c_copies:
        copy.wait()


def mix_call(layer, last, attn, x_own, g_mlp, g_attn, w_o, w_gate, w_up, w_down, k_cache, v_cache):
    batch = attn.shape[0]
    depth, width = w_o.shape[1:]
    hidden = w_gate.shape[2]
    rows = batch // ROW_CHUNKS
    blk = rows // 8
    any_spec = pl.BlockSpec(memory_space=pltpu.HBM)
    vmem = pl.BlockSpec(memory_space=pltpu.VMEM)
    if last:
        out_shape = [jax.ShapeDtypeStruct((batch, width), BF16)]
        out_specs = [any_spec]
    else:
        out_shape = [pltpu.VMEM((batch, width), BF16), pltpu.VMEM((ROW_CHUNKS, blk, width), BF16)]
        out_shape.append(pltpu.VMEM((2,) + k_cache.shape[1:], BF16))
        out_specs = [vmem] * 3
    sem = pltpu.SemaphoreType.DMA
    nc = ROW_CHUNKS
    return pl.pallas_call(
        functools.partial(mix_kernel, layer, last),
        out_shape=out_shape,
        in_specs=[vmem, any_spec if layer == 0 else vmem, vmem, vmem] + [any_spec] * 6,
        out_specs=out_specs,
        scratch_shapes=[
            pltpu.VMEM((depth, width), BF16),
            pltpu.VMEM((width, hidden), BF16),
            pltpu.VMEM((width, hidden), BF16),
            pltpu.VMEM((hidden, width), BF16),
            pltpu.VMEM((nc, blk, width), BF16),
            pltpu.VMEM((batch, hidden), BF16),
            pltpu.VMEM((2, nc, rows // 2, width), BF16),
            pltpu.VMEM((2, nc, rows // 2, width), BF16),
            pltpu.VMEM((2, batch, width), F32),
            pltpu.VMEM((2, nc, 4, blk, width), BF16),
            pltpu.VMEM((2, nc, 4, blk, width), BF16),
            pltpu.VMEM((2, batch, width), BF16),
            sem((4,)), sem((nc,)),
            sem((2, nc)), sem((2, nc)),
            sem((2, nc, 4)), sem((2, nc, 4)),
            sem((2, nc, 4)), sem((2, nc, 4)),
            sem((2, nc, 4)), sem((2, nc, 4)),
            sem((nc,)), sem((2, 8)),
        ],
        compiler_params=pltpu.CompilerParams(collective_id=layer, has_side_effects=True, vmem_limit_bytes=MIX_VMEM),
        cost_estimate=pl.CostEstimate(flops=2 * batch * width * (depth + 3 * hidden), bytes_accessed=2 * width * (depth + 3 * hidden), transcendentals=batch * hidden),
        name=f"mix{layer}",
    )(*in_vmem(attn), *(in_hbm if layer == 0 else in_vmem)(x_own), g_mlp, g_attn, *in_hbm(w_o, w_gate, w_up, w_down, k_cache, v_cache))


def solution(mesh):
    weight_col = P(None, None, "tp")
    weight_row = P(None, "tp", None)
    bias_col = P(None, "tp")
    cache_spec = P(None, "dp", None, "tp", None)
    in_specs = (P("dp", None), P("dp"), P(None, None), P(None, None), weight_col, bias_col, weight_col, bias_col, weight_col, bias_col, weight_row, weight_col, weight_col, weight_row, cache_spec, cache_spec)
    out_specs = (P("dp", None), cache_spec, cache_spec)

    def local_step(x_in, seq_lens, g_attn, g_mlp, w_q, b_q, w_k, b_k, w_v, b_v, w_o, w_gate, w_up, w_down, k_cache, v_cache):
        layers, batch, slots, _, head = k_cache.shape
        inv_freq = ROPE_THETA ** (-2.0 * np.arange(head // 2) / head)
        freq = jnp.asarray(np.concatenate([inv_freq, inv_freq])[None, :].astype(np.float32))
        k_flat = k_cache.reshape(layers, batch, slots, head)
        v_flat = v_cache.reshape(layers, batch, slots, head)
        normed, x_own, prev = x_in, x_in, None
        caches = (k_flat, v_flat)
        for layer in range(layers):
            last = layer == layers - 1
            attn, k_out, v_out = attn_call(layer, layer == 0, seq_lens, freq, normed, g_attn, b_q, b_k, b_v, w_q, w_k, w_v, caches, prev)
            prev = (k_out, v_out)
            outs = mix_call(layer, last, attn, x_own, g_mlp, g_attn, w_o, w_gate, w_up, w_down, k_flat, v_flat)
            if last:
                x_out = outs[0]
            else:
                normed, x_own, caches = outs[0], outs[1], outs[2:]
        return x_out, prev[0].reshape(k_cache.shape), prev[1].reshape(v_cache.shape)

    return jax.shard_map(local_step, mesh=mesh, in_specs=in_specs, out_specs=out_specs, check_vma=False)
```

```python
import functools
import math

import jax
import jax.numpy as jnp
import numpy as np
from jax import lax
from jax.experimental import pallas as pl
from jax.experimental.pallas import tpu as pltpu
from jax.sharding import PartitionSpec as P

ROPE_THETA = 1000000.0
EPS = 1e-6
F32 = jnp.float32
BF16 = jnp.bfloat16
NT = (((1,), (1,)), ((), ()))
SEQ_CHUNK = 16
ROW_CHUNKS = 4
MLP_CHUNKS = 2
ATTN_VMEM = 24 * 1024 * 1024
MIX_VMEM = 22 * 1024 * 1024


def norm_rows(vec_f32, gain_row):
    mean_sq = jnp.mean(vec_f32 * vec_f32, axis=-1, keepdims=True)
    return (vec_f32 * lax.rsqrt(mean_sq + EPS) * gain_row).astype(BF16)


def attn_kernel(layer, do_norm, aliased, *refs):
    (lens_smem, lens_row, freq, x_hbm, g_ref, bq_ref, bk_ref, bv_ref, wq_hbm, wk_hbm, wv_hbm) = refs[:11]
    kc_hbm, vc_hbm = (None, None) if aliased else refs[11:13]
    refs = refs[14 if aliased else 13:]
    attn_ref, ko_hbm, vo_hbm = refs[:3]
    refs = refs[3:]
    kv_buf = refs[0] if aliased else refs[-1]
    k_buf, v_buf = kv_buf.at[0], kv_buf.at[1]
    refs = refs[1:] if aliased else refs[:-1]
    (x_buf, w_buf, q_f32, k_f32, v_f32, lens_col, out_f32, s_buf, x_sem, w_sem, k_sem, v_sem, ko_sem, vo_sem) = refs
    batch, slots, head = k_buf.shape
    q_width = wq_hbm.shape[2]
    n_chunks = batch // SEQ_CHUNK

    if do_norm:
        x_copy = pltpu.make_async_copy(x_hbm, x_buf, x_sem)
        x_copy.start()
    w_copies = [
        pltpu.make_async_copy(wq_hbm.at[layer], w_buf.at[:, :q_width], w_sem.at[0]),
        pltpu.make_async_copy(wk_hbm.at[layer], w_buf.at[:, q_width:q_width + head], w_sem.at[1]),
        pltpu.make_async_copy(wv_hbm.at[layer], w_buf.at[:, q_width + head:], w_sem.at[2]),
    ]
    for copy in w_copies:
        copy.start()

    def chunk_copies(idx):
        rows = pl.ds(pl.multiple_of(idx * SEQ_CHUNK, SEQ_CHUNK), SEQ_CHUNK)
        return (
            None if aliased else pltpu.make_async_copy(kc_hbm.at[layer, rows], k_buf.at[rows], k_sem.at[idx]),
            None if aliased else pltpu.make_async_copy(vc_hbm.at[layer, rows], v_buf.at[rows], v_sem.at[idx]),
            pltpu.make_async_copy(k_buf.at[rows], ko_hbm.at[layer, rows], ko_sem.at[idx]),
            pltpu.make_async_copy(v_buf.at[rows], vo_hbm.at[layer, rows], vo_sem.at[idx]),
        )

    if not aliased:
        @pl.loop(0, n_chunks)
        def _(idx):
            k_in, v_in, _, _ = chunk_copies(idx)
            k_in.start()
            v_in.start()

    lens_f = lens_row[...].astype(F32)
    same = lax.broadcasted_iota(jnp.int32, (batch, batch), 0) == lax.broadcasted_iota(jnp.int32, (batch, batch), 1)
    pos_col = jnp.sum(jnp.where(same, jnp.broadcast_to(lens_f, (batch, batch)), 0.0), axis=1, keepdims=True)
    lens_col[...] = jnp.broadcast_to(pos_col, (batch, head)).astype(jnp.int32)
    angles = pos_col * freq[...]
    cos_tab = jnp.cos(angles)
    lane = lax.broadcasted_iota(jnp.int32, (1, head), 1)
    sin_tab = jnp.sin(angles) * jnp.where(lane < head // 2, -1.0, 1.0)

    def rope(vec):
        return vec * cos_tab + pltpu.roll(vec, head // 2, 1) * sin_tab

    for copy in w_copies:
        copy.wait()
    if do_norm:
        x_copy.wait()
        normed = norm_rows(x_buf[...].astype(F32), g_ref[layer:layer + 1, :].astype(F32))
    else:
        normed = x_hbm[...]
    for col in range(q_width // head):
        cols = slice(col * head, (col + 1) * head)
        part = jnp.dot(normed, w_buf[:, cols], preferred_element_type=F32) + bq_ref[layer:layer + 1, cols].astype(F32)
        q_f32[:, cols] = rope(part).astype(BF16).astype(F32)
    part = jnp.dot(normed, w_buf[:, q_width:], preferred_element_type=F32)
    k_f32[...] = rope(part[:, :head] + bk_ref[layer:layer + 1, :].astype(F32)).astype(BF16).astype(F32)
    v_f32[...] = (part[:, head:] + bv_ref[layer:layer + 1, :].astype(F32)).astype(BF16).astype(F32)

    half = 8
    scale = head ** -0.5
    row_in_group = lax.broadcasted_iota(jnp.int32, (2 * half, head), 0) % half
    slot_id = lax.broadcasted_iota(jnp.int32, (2 * half, slots), 1)
    tile_row = lax.broadcasted_iota(jnp.int32, (16, head), 0)

    def patch(idx):
        for sub in range(SEQ_CHUNK):
            seq = idx * SEQ_CHUNK + sub
            pos = lens_smem[seq]
            base = pl.multiple_of((pos >> 4) << 4, 16)
            hit = tile_row == pos - base
            for buf, new in ((k_buf, k_f32), (v_buf, v_f32)):
                row = jnp.broadcast_to(new[pl.ds(seq, 1), :], (16, head))
                old = buf[seq, pl.ds(base, 16), :]
                buf[seq, pl.ds(base, 16), :] = jnp.where(hit, row, old.astype(F32)).astype(BF16)

    groups = SEQ_CHUNK // half

    def first_row(idx, group):
        return pl.multiple_of(idx * SEQ_CHUNK + group * half, half)

    def scores_of(idx, group):
        first = first_row(idx, group)
        q_rows = q_f32[pl.ds(first, half), :]
        q_all = jnp.concatenate([q_rows[:, :head], q_rows[:, head:]], axis=0)
        scores = jnp.zeros((2 * half, slots), F32)
        for pair in range(half // 2):
            lhs = jnp.concatenate([jnp.where(row_in_group == 2 * pair + e, q_all, 0.0) for e in range(2)], axis=1).astype(BF16)
            rhs = jnp.concatenate([k_buf[first + 2 * pair + e] for e in range(2)], axis=1)
            scores += lax.dot_general(lhs, rhs, NT, preferred_element_type=F32)
        return scores

    def probs_of(idx, group):
        pos_rows = lens_col[pl.ds(first_row(idx, group), half), 0:1]
        pos_all = jnp.concatenate([pos_rows, pos_rows], axis=0)
        scores = jnp.where(slot_id <= pos_all, s_buf[group] * scale, -1e30)
        expo = jnp.exp(scores - jnp.max(scores, axis=-1, keepdims=True))
        return (expo / jnp.sum(expo, axis=-1, keepdims=True)).astype(BF16)

    def values_of(idx, group, probs):
        first = first_row(idx, group)
        out = jnp.zeros((2 * half, head), F32)
        for pair in range(half // 2):
            rhs = jnp.concatenate([v_buf[first + 2 * pair + e] for e in range(2)], axis=1)
            both = jnp.dot(probs, rhs, preferred_element_type=F32)
            for e in range(2):
                out = jnp.where(row_in_group == 2 * pair + e, both[:, e * head:(e + 1) * head], out)
        return jnp.concatenate([out[:half], out[half:]], axis=1)

    s_buf[...] = jnp.zeros_like(s_buf)

    @pl.loop(0, n_chunks + 1)
    def _(idx):
        @pl.when(idx < n_chunks)
        def _():
            k_in, v_in, k_out, v_out = chunk_copies(idx)
            if not aliased:
                k_in.wait()
                v_in.wait()
            patch(idx)
            k_out.start()
            v_out.start()

        now = jnp.maximum(idx - 1, 0)
        later = jnp.minimum(idx, n_chunks - 1)
        new_scores = [scores_of(later, group) for group in range(groups)]
        probs = [probs_of(now, group) for group in range(groups)]
        outs = [values_of(now, group, probs[group]) for group in range(groups)]
        for group in range(groups):
            s_buf[group] = new_scores[group]
            out_f32[pl.ds(first_row(now, group), half), :] = outs[group]

    attn_ref[...] = out_f32[...].astype(BF16)

    @pl.loop(0, n_chunks)
    def _(idx):
        _, _, k_out, v_out = chunk_copies(idx)
        k_out.wait()
        v_out.wait()


def in_hbm(*arrays):
    return [pltpu.with_memory_space_constraint(a, pltpu.HBM) for a in arrays]


def in_vmem(*arrays):
    return [pltpu.with_memory_space_constraint(a, pltpu.VMEM) for a in arrays]


def attn_call(layer, do_norm, lens, freq, x_in, gain, b_q, b_k, b_v, w_q, w_k, w_v, caches, prev):
    batch, slots, head = caches[0].shape[-3:]
    width = x_in.shape[1]
    q_width = w_q.shape[2]
    any_spec = pl.BlockSpec(memory_space=pltpu.HBM)
    vmem = pl.BlockSpec(memory_space=pltpu.VMEM)
    aliased = prev is not None
    place = in_hbm if do_norm else in_vmem
    args = [lens, lens.reshape(1, batch), freq, *place(x_in), gain, b_q, b_k, b_v, *in_hbm(w_q, w_k, w_v), *place(*caches)]
    in_specs = [pl.BlockSpec(memory_space=pltpu.SMEM), vmem, vmem, any_spec if do_norm else vmem, vmem, vmem, vmem, vmem] + [any_spec] * 5
    aliases = {}
    if aliased:
        aliases = {len(args): 1, len(args) + 1: 2, len(args) - 1: 3}
        args += in_hbm(*prev)
        in_specs = in_specs[:-2] + [vmem] + [any_spec] * 2
    cache_buf = pltpu.VMEM((2, batch, slots, head), BF16)
    out_cache = jax.ShapeDtypeStruct((w_q.shape[0], batch, slots, head), BF16)
    n_chunks = batch // SEQ_CHUNK
    macs = batch * width * (q_width + 2 * head) + 2 * batch * slots * q_width
    return pl.pallas_call(
        functools.partial(attn_kernel, layer, do_norm, aliased),
        out_shape=(
            pltpu.VMEM((batch, q_width), BF16),
            out_cache,
            out_cache,
        ) + ((cache_buf,) if aliased else ()),
        in_specs=in_specs,
        out_specs=(vmem, any_spec, any_spec) + ((vmem,) if aliased else ()),
        scratch_shapes=[
            pltpu.VMEM((batch, width), BF16),
            pltpu.VMEM((width, q_width + 2 * head), BF16),
            pltpu.VMEM((batch, q_width), F32),
            pltpu.VMEM((batch, head), F32),
            pltpu.VMEM((batch, head), F32),
            pltpu.VMEM((batch, head), jnp.int32),
            pltpu.VMEM((batch, q_width), F32),
            pltpu.VMEM((SEQ_CHUNK // 8, 16, slots), F32),
            pltpu.SemaphoreType.DMA,
            pltpu.SemaphoreType.DMA((3,)),
            pltpu.SemaphoreType.DMA((n_chunks,)),
            pltpu.SemaphoreType.DMA((n_chunks,)),
            pltpu.SemaphoreType.DMA((n_chunks,)),
            pltpu.SemaphoreType.DMA((n_chunks,)),
        ] + ([] if aliased else [cache_buf]),
        input_output_aliases=aliases,
        compiler_params=pltpu.CompilerParams(vmem_limit_bytes=ATTN_VMEM + (0 if aliased else 4 * batch * slots * head)),
        cost_estimate=pl.CostEstimate(flops=2 * macs, bytes_accessed=4 * batch * slots * head * 2, transcendentals=batch * slots * 2),
        name=f"attn{layer}",
    )(*args)[:3]


def mix_kernel(layer, last, attn_ref, x_hbm, gm_ref, gn_ref, wo_hbm, wg_hbm, wu_hbm, wd_hbm, kc_hbm, vc_hbm, *refs):
    if last:
        out_hbm = refs[0]
        refs = refs[1:]
    else:
        out_hbm, xs_ref, kv_next = refs[:3]
        refs = refs[3:]
    (wo, wg, wu, wd, x_own, act, d_send, d_recv, own, r_send, r_recv, gathered,
     w_sem, x_sem, ds_sem, dr_sem, rs_sem, rr_sem, as_sem, ar_sem, fs_sem, fr_sem, o_sem, c_sem) = refs
    width = wo.shape[1]
    hidden = wg.shape[1]
    rows = attn_ref.shape[0] // ROW_CHUNKS
    core_rows = rows // 2
    blk = core_rows // 4
    me = lax.axis_index("tp")
    core = me % 2
    chip = me // 2
    partner = me + 1 - 2 * core
    peer_y = (chip + 2) % 4
    peer_x = chip + 1 - 2 * (chip % 2)
    peers = [chip, peer_x * (1 - core) + peer_y * core, peer_y * (1 - core) + peer_x * core, 3 - chip]

    def dev(idx):
        return {"tp": idx}

    w_copies = [pltpu.make_async_copy(src.at[layer], dst, w_sem.at[i])
                for i, (src, dst) in enumerate(((wo_hbm, wo), (wg_hbm, wg), (wu_hbm, wu), (wd_hbm, wd)))]
    w_copies[0].start()

    def own_rows(j):
        return pl.ds(pl.multiple_of(j * rows + core * core_rows + chip * blk, blk), blk)

    x_copies = []
    for j in range(ROW_CHUNKS):
        if layer:
            x_own[j] = x_hbm[j]
        else:
            x_copies.append(pltpu.make_async_copy(x_hbm.at[own_rows(j)], x_own.at[j], x_sem.at[j]))
            x_copies[-1].start()

    c_copies = []
    if not last:
        parts = c_sem.shape[1]
        size = kv_next.shape[1] // parts
        for i, src in enumerate((kc_hbm, vc_hbm)):
            for n in range(parts):
                part = pl.ds(n * size, size)
                c_copies.append(pltpu.make_async_copy(src.at[layer + 1, part], kv_next.at[i, part], c_sem.at[i, n]))

    def prefetch(count):
        for _ in range(min(count, len(waiting))):
            waiting.pop(0).start()

    waiting = list(c_copies)
    prefetch(2)
    barrier = pltpu.get_barrier_semaphore()
    others = [partner] + [2 * peers[r] + core for r in range(1, 4)]
    for other in others:
        pl.semaphore_signal(barrier, inc=1, device_id=dev(other), device_id_type=pl.DeviceIdType.MESH)

    def remote(src, dst, send, recv, target):
        return pltpu.make_async_remote_copy(src_ref=src, dst_ref=dst, send_sem=send, recv_sem=recv,
                                            device_id=dev(target), device_id_type=pl.DeviceIdType.MESH)

    def share(s, first, count, lhs, weight):
        step = 512
        here = pl.ds(first * rows, count * rows)

        @pl.loop(0, width // step)
        def _(n):
            cols = pl.ds(pl.multiple_of(n * step, step), step)
            own[s, here, cols] = jnp.dot(lhs, weight[:, cols], preferred_element_type=F32)

        for j in range(first, first + count):
            d_send[s, j] = own[s, pl.ds(pl.multiple_of(j * rows + (1 - core) * core_rows, core_rows), core_rows), :].astype(BF16)

    def d_copy(s, j):
        return remote(d_send.at[s, j], d_recv.at[s, j], ds_sem.at[s, j], dr_sem.at[s, j], partner)

    def r_copy(s, j, r):
        return remote(r_send.at[s, j, r], r_recv.at[s, j, r], rs_sem.at[s, j, r], rr_sem.at[s, j, r], 2 * peers[r] + core)

    def scatter(s, j):
        d_copy(s, j).wait()
        for r in (3, 1, 2):
            off = pl.multiple_of(peers[r] * blk, blk)
            mine = own[s, pl.ds(pl.multiple_of(j * rows + core * core_rows + off, blk), blk), :]
            r_send[s, j, r] = (mine + d_recv[s, j, pl.ds(off, blk), :].astype(F32)).astype(BF16)
            r_copy(s, j, r).start()

    def reduce(s, j):
        off = pl.multiple_of(chip * blk, blk)
        total = own[s, own_rows(j), :] + d_recv[s, j, pl.ds(off, blk), :].astype(F32)
        for r in (1, 2, 3):
            r_copy(s, j, r).wait()
            total += r_recv[s, j, r].astype(F32)
        new = (x_own[j].astype(F32) + total).astype(BF16)
        x_own[j] = new
        return new

    def block_row(j, cc, k):
        return pl.ds(pl.multiple_of(j * rows + cc * core_rows + k * blk, blk), blk)

    def a_copy(s, j, r):
        here = block_row(j, core, chip)
        target = partner if r == 0 else 2 * peers[r] + core
        return remote(gathered.at[s, here], gathered.at[s, here], as_sem.at[s, j, r], ar_sem.at[s, j, r], target)

    def f_copy(s, j, r):
        here = block_row(j, core, peers[r])
        return remote(gathered.at[s, here], gathered.at[s, here], fs_sem.at[s, j, r], fr_sem.at[s, j, r], partner)

    def gather_start(s, j, value):
        gathered[s, block_row(j, core, chip), :] = value
        for r in (3, 1, 2, 0):
            a_copy(s, j, r).start()

    def gather_forward(s, j):
        for r in (1, 2, 3):
            a_copy(s, j, r).wait_recv()
            f_copy(s, j, r).start()

    def gather_finish(s, j):
        a_copy(s, j, 0).wait_recv()
        for r in (1, 2, 3):
            f_copy(s, j, r).wait_recv()

    chunks = range(ROW_CHUNKS)
    per = MLP_CHUNKS
    w_copies[0].wait()
    for first in range(0, ROW_CHUNKS, per):
        share(0, first, per, attn_ref[first * rows:(first + per) * rows, :], wo)
        if first == 0:
            pl.semaphore_wait(barrier, len(others))
        for j in range(first, first + per):
            d_copy(0, j).start()
    for copy in x_copies:
        copy.wait()
    for j in chunks:
        scatter(0, j)
    for copy in w_copies[1:]:
        copy.start()
    for j in chunks:
        new = reduce(0, j)
        gather_start(0, j, norm_rows(new.astype(F32), gm_ref[layer:layer + 1, :].astype(F32)))
    prefetch(3)

    def mlp(first):
        here = slice(first * rows, (first + per) * rows)
        step = 256

        @pl.loop(0, hidden // step)
        def _(n):
            cols = pl.ds(pl.multiple_of(n * step, step), step)
            lhs = gathered[0, here, :]
            gate = jnp.dot(lhs, wg[:, cols], preferred_element_type=F32)
            up = jnp.dot(lhs, wu[:, cols], preferred_element_type=F32)
            act[here, cols] = (gate * jax.nn.sigmoid(gate) * up).astype(BF16)
        share(1, first, per, act[here, :], wd)
        for j in range(first, first + per):
            d_copy(1, j).start()

    for j in range(per):
        gather_forward(0, j)
    for copy in w_copies[1:]:
        copy.wait()
    for first in range(0, ROW_CHUNKS, per):
        for j in range(first, first + per):
            gather_finish(0, j)
        prefetch(3)
        mlp(first)
        for j in range(first + per, min(first + 2 * per, ROW_CHUNKS)):
            gather_forward(0, j)
        for j in range(first, first + per):
            scatter(1, j)

    def second(j):
        new = reduce(1, j)
        if last:
            gather_start(1, j, new)
        else:
            xs_ref[j] = new
            gather_start(1, j, norm_rows(new.astype(F32), gn_ref[layer + 1:layer + 2, :].astype(F32)))

    prefetch(1)
    for j in chunks:
        second(j)
    prefetch(4)
    for j in chunks:
        gather_forward(1, j)
    prefetch(len(waiting))
    outs = []
    for j in chunks:
        gather_finish(1, j)
        here = pl.ds(j * rows, rows)
        if last:
            outs.append(pltpu.make_async_copy(gathered.at[1, here], out_hbm.at[here], o_sem.at[j]))
            outs[-1].start()
        else:
            out_hbm[here, :] = gathered[1, here, :]
    for s in range(2):
        for j in range(ROW_CHUNKS):
            for r in range(4):
                a_copy(s, j, r).wait_send()
            for r in range(1, 4):
                f_copy(s, j, r).wait_send()
    for copy in outs + c_copies:
        copy.wait()


def mix_call(layer, last, attn, x_own, g_mlp, g_attn, w_o, w_gate, w_up, w_down, k_cache, v_cache):
    batch = attn.shape[0]
    depth, width = w_o.shape[1:]
    hidden = w_gate.shape[2]
    rows = batch // ROW_CHUNKS
    blk = rows // 8
    any_spec = pl.BlockSpec(memory_space=pltpu.HBM)
    vmem = pl.BlockSpec(memory_space=pltpu.VMEM)
    if last:
        out_shape = [jax.ShapeDtypeStruct((batch, width), BF16)]
        out_specs = [any_spec]
    else:
        out_shape = [pltpu.VMEM((batch, width), BF16), pltpu.VMEM((ROW_CHUNKS, blk, width), BF16)]
        out_shape.append(pltpu.VMEM((2,) + k_cache.shape[1:], BF16))
        out_specs = [vmem] * 3
    sem = pltpu.SemaphoreType.DMA
    nc = ROW_CHUNKS
    return pl.pallas_call(
        functools.partial(mix_kernel, layer, last),
        out_shape=out_shape,
        in_specs=[vmem, any_spec if layer == 0 else vmem, vmem, vmem] + [any_spec] * 6,
        out_specs=out_specs,
        scratch_shapes=[
            pltpu.VMEM((depth, width), BF16),
            pltpu.VMEM((width, hidden), BF16),
            pltpu.VMEM((width, hidden), BF16),
            pltpu.VMEM((hidden, width), BF16),
            pltpu.VMEM((nc, blk, width), BF16),
            pltpu.VMEM((batch, hidden), BF16),
            pltpu.VMEM((2, nc, rows // 2, width), BF16),
            pltpu.VMEM((2, nc, rows // 2, width), BF16),
            pltpu.VMEM((2, batch, width), F32),
            pltpu.VMEM((2, nc, 4, blk, width), BF16),
            pltpu.VMEM((2, nc, 4, blk, width), BF16),
            pltpu.VMEM((2, batch, width), BF16),
            sem((4,)), sem((nc,)),
            sem((2, nc)), sem((2, nc)),
            sem((2, nc, 4)), sem((2, nc, 4)),
            sem((2, nc, 4)), sem((2, nc, 4)),
            sem((2, nc, 4)), sem((2, nc, 4)),
            sem((nc,)), sem((2, 8)),
        ],
        compiler_params=pltpu.CompilerParams(collective_id=layer, has_side_effects=True, vmem_limit_bytes=MIX_VMEM),
        cost_estimate=pl.CostEstimate(flops=2 * batch * width * (depth + 3 * hidden), bytes_accessed=2 * width * (depth + 3 * hidden), transcendentals=batch * hidden),
        name=f"mix{layer}",
    )(*in_vmem(attn), *(in_hbm if layer == 0 else in_vmem)(x_own), g_mlp, g_attn, *in_hbm(w_o, w_gate, w_up, w_down, k_cache, v_cache))


def solution(mesh):
    weight_col = P(None, None, "tp")
    weight_row = P(None, "tp", None)
    bias_col = P(None, "tp")
    cache_spec = P(None, "dp", None, "tp", None)
    in_specs = (P("dp", None), P("dp"), P(None, None), P(None, None), weight_col, bias_col, weight_col, bias_col, weight_col, bias_col, weight_row, weight_col, weight_col, weight_row, cache_spec, cache_spec)
    out_specs = (P("dp", None), cache_spec, cache_spec)

    def local_step(x_in, seq_lens, g_attn, g_mlp, w_q, b_q, w_k, b_k, w_v, b_v, w_o, w_gate, w_up, w_down, k_cache, v_cache):
        layers, batch, slots, _, head = k_cache.shape
        inv_freq = ROPE_THETA ** (-2.0 * np.arange(head // 2) / head)
        freq = jnp.asarray(np.concatenate([inv_freq, inv_freq])[None, :].astype(np.float32))
        k_flat = k_cache.reshape(layers, batch, slots, head)
        v_flat = v_cache.reshape(layers, batch, slots, head)
        normed, x_own, prev = x_in, x_in, None
        caches = (k_flat, v_flat)
        for layer in range(layers):
            last = layer == layers - 1
            attn, k_out, v_out = attn_call(layer, layer == 0, seq_lens, freq, normed, g_attn, b_q, b_k, b_v, w_q, w_k, w_v, caches, prev)
            prev = (k_out, v_out)
            outs = mix_call(layer, last, attn, x_own, g_mlp, g_attn, w_o, w_gate, w_up, w_down, k_flat, v_flat)
            if last:
                x_out = outs[0]
            else:
                normed, x_own, caches = outs[0], outs[1], outs[2:]
        return x_out, prev[0].reshape(k_cache.shape), prev[1].reshape(v_cache.shape)

    return jax.shard_map(local_step, mesh=mesh, in_specs=in_specs, out_specs=out_specs, check_vma=False)
```

```python
import functools
import math

import jax
import jax.numpy as jnp
import numpy as np
from jax import lax
from jax.experimental import pallas as pl
from jax.experimental.pallas import tpu as pltpu
from jax.sharding import PartitionSpec as P

ROPE_THETA = 1000000.0
EPS = 1e-6
F32 = jnp.float32
BF16 = jnp.bfloat16
NT = (((1,), (1,)), ((), ()))
SEQ_CHUNK = 16
ROW_CHUNKS = 4
MLP_CHUNKS = 2
PARTS = 8
PREFETCHED = 6
ATTN_VMEM = 24 * 1024 * 1024
MIX_VMEM = 22 * 1024 * 1024


def norm_rows(vec_f32, gain_row):
    mean_sq = jnp.mean(vec_f32 * vec_f32, axis=-1, keepdims=True)
    return (vec_f32 * lax.rsqrt(mean_sq + EPS) * gain_row).astype(BF16)


def attn_kernel(layer, do_norm, aliased, *refs):
    (lens_smem, lens_row, freq, x_hbm, g_ref, bq_ref, bk_ref, bv_ref, wq_hbm, wk_hbm, wv_hbm, wo_hbm, kc_hbm, vc_hbm) = refs[:14]
    refs = refs[17 if aliased else 14:]
    part_ref, ko_hbm, vo_hbm = refs[:3]
    refs = refs[3:]
    kv_buf = refs[0] if aliased else refs[-1]
    k_buf, v_buf = kv_buf.at[0], kv_buf.at[1]
    refs = refs[1:] if aliased else refs[:-1]
    (x_buf, w_buf, wo, q_f32, k_f32, v_f32, lens_col, out_f32, s_buf, x_sem, w_sem, k_sem, v_sem, ko_sem, vo_sem) = refs
    batch, slots, head = k_buf.shape
    q_width = wq_hbm.shape[2]
    n_chunks = batch // SEQ_CHUNK

    if do_norm:
        x_copy = pltpu.make_async_copy(x_hbm, x_buf, x_sem)
        x_copy.start()
    w_copies = [
        pltpu.make_async_copy(wq_hbm.at[layer], w_buf.at[:, :q_width], w_sem.at[0]),
        pltpu.make_async_copy(wk_hbm.at[layer], w_buf.at[:, q_width:q_width + head], w_sem.at[1]),
        pltpu.make_async_copy(wv_hbm.at[layer], w_buf.at[:, q_width + head:], w_sem.at[2]),
    ]
    for copy in w_copies:
        copy.start()
    first_read = n_chunks * PREFETCHED // PARTS if aliased else 0
    wo_copy = pltpu.make_async_copy(wo_hbm.at[layer], wo, w_sem.at[3])

    def chunk_copies(idx):
        rows = pl.ds(pl.multiple_of(idx * SEQ_CHUNK, SEQ_CHUNK), SEQ_CHUNK)
        return (
            pltpu.make_async_copy(kc_hbm.at[layer, rows], k_buf.at[rows], k_sem.at[idx]),
            pltpu.make_async_copy(vc_hbm.at[layer, rows], v_buf.at[rows], v_sem.at[idx]),
            pltpu.make_async_copy(k_buf.at[rows], ko_hbm.at[layer, rows], ko_sem.at[idx]),
            pltpu.make_async_copy(v_buf.at[rows], vo_hbm.at[layer, rows], vo_sem.at[idx]),
        )

    @pl.loop(first_read, n_chunks)
    def _(idx):
        k_in, v_in, _, _ = chunk_copies(idx)
        k_in.start()
        v_in.start()

    wo_copy.start()

    lens_f = lens_row[...].astype(F32)
    same = lax.broadcasted_iota(jnp.int32, (batch, batch), 0) == lax.broadcasted_iota(jnp.int32, (batch, batch), 1)
    pos_col = jnp.sum(jnp.where(same, jnp.broadcast_to(lens_f, (batch, batch)), 0.0), axis=1, keepdims=True)
    lens_col[...] = jnp.broadcast_to(pos_col, (batch, head)).astype(jnp.int32)
    angles = pos_col * freq[...]
    cos_tab = jnp.cos(angles)
    lane = lax.broadcasted_iota(jnp.int32, (1, head), 1)
    sin_tab = jnp.sin(angles) * jnp.where(lane < head // 2, -1.0, 1.0)

    def rope(vec):
        return vec * cos_tab + pltpu.roll(vec, head // 2, 1) * sin_tab

    for copy in w_copies:
        copy.wait()
    if do_norm:
        x_copy.wait()
        normed = norm_rows(x_buf[...].astype(F32), g_ref[layer:layer + 1, :].astype(F32))
    else:
        normed = x_hbm[...]
    for col in range(q_width // head):
        cols = slice(col * head, (col + 1) * head)
        part = jnp.dot(normed, w_buf[:, cols], preferred_element_type=F32) + bq_ref[layer:layer + 1, cols].astype(F32)
        q_f32[:, cols] = rope(part).astype(BF16).astype(F32)
    part = jnp.dot(normed, w_buf[:, q_width:], preferred_element_type=F32)
    k_f32[...] = rope(part[:, :head] + bk_ref[layer:layer + 1, :].astype(F32)).astype(BF16).astype(F32)
    v_f32[...] = (part[:, head:] + bv_ref[layer:layer + 1, :].astype(F32)).astype(BF16).astype(F32)

    half = 8
    scale = head ** -0.5
    row_in_group = lax.broadcasted_iota(jnp.int32, (2 * half, head), 0) % half
    slot_id = lax.broadcasted_iota(jnp.int32, (2 * half, slots), 1)
    tile_row = lax.broadcasted_iota(jnp.int32, (16, head), 0)

    def patch(idx):
        for sub in range(SEQ_CHUNK):
            seq = idx * SEQ_CHUNK + sub
            pos = lens_smem[seq]
            base = pl.multiple_of((pos >> 4) << 4, 16)
            hit = tile_row == pos - base
            for buf, new in ((k_buf, k_f32), (v_buf, v_f32)):
                row = jnp.broadcast_to(new[pl.ds(seq, 1), :], (16, head))
                old = buf[seq, pl.ds(base, 16), :]
                buf[seq, pl.ds(base, 16), :] = jnp.where(hit, row, old.astype(F32)).astype(BF16)

    groups = SEQ_CHUNK // half

    def first_row(idx, group):
        return pl.multiple_of(idx * SEQ_CHUNK + group * half, half)

    def scores_of(idx, group):
        first = first_row(idx, group)
        q_rows = q_f32[pl.ds(first, half), :]
        q_all = jnp.concatenate([q_rows[:, :head], q_rows[:, head:]], axis=0)
        scores = jnp.zeros((2 * half, slots), F32)
        for pair in range(half // 2):
            lhs = jnp.concatenate([jnp.where(row_in_group == 2 * pair + e, q_all, 0.0) for e in range(2)], axis=1).astype(BF16)
            rhs = jnp.concatenate([k_buf[first + 2 * pair + e] for e in range(2)], axis=1)
            scores += lax.dot_general(lhs, rhs, NT, preferred_element_type=F32)
        return scores

    def probs_of(idx, group):
        pos_rows = lens_col[pl.ds(first_row(idx, group), half), 0:1]
        pos_all = jnp.concatenate([pos_rows, pos_rows], axis=0)
        scores = jnp.where(slot_id <= pos_all, s_buf[group] * scale, -1e30)
        expo = jnp.exp(scores - jnp.max(scores, axis=-1, keepdims=True))
        return (expo / jnp.sum(expo, axis=-1, keepdims=True)).astype(BF16)

    def values_of(idx, group, probs):
        first = first_row(idx, group)
        out = jnp.zeros((2 * half, head), F32)
        for pair in range(half // 2):
            rhs = jnp.concatenate([v_buf[first + 2 * pair + e] for e in range(2)], axis=1)
            both = jnp.dot(probs, rhs, preferred_element_type=F32)
            for e in range(2):
                out = jnp.where(row_in_group == 2 * pair + e, both[:, e * head:(e + 1) * head], out)
        return jnp.concatenate([out[:half], out[half:]], axis=1)

    s_buf[...] = jnp.zeros_like(s_buf)

    @pl.loop(0, n_chunks + 1)
    def _(idx):
        @pl.when(idx < n_chunks)
        def _():
            k_in, v_in, k_out, v_out = chunk_copies(idx)
            @pl.when(idx >= first_read)
            def _():
                k_in.wait()
                v_in.wait()

            patch(idx)
            k_out.start()
            v_out.start()

        now = jnp.maximum(idx - 1, 0)
        later = jnp.minimum(idx, n_chunks - 1)
        new_scores = [scores_of(later, group) for group in range(groups)]
        probs = [probs_of(now, group) for group in range(groups)]
        outs = [values_of(now, group, probs[group]) for group in range(groups)]
        for group in range(groups):
            s_buf[group] = new_scores[group]
            out_f32[pl.ds(first_row(now, group), half), :] = outs[group]

    wo_copy.wait()
    attn = out_f32[...].astype(BF16)
    step = 512
    for col in range(0, wo.shape[1], step):
        part_ref[:, col:col + step] = jnp.dot(attn, wo[:, col:col + step], preferred_element_type=F32).astype(BF16)

    @pl.loop(0, n_chunks)
    def _(idx):
        _, _, k_out, v_out = chunk_copies(idx)
        k_out.wait()
        v_out.wait()


def in_hbm(*arrays):
    return [pltpu.with_memory_space_constraint(a, pltpu.HBM) for a in arrays]


def in_vmem(*arrays):
    return [pltpu.with_memory_space_constraint(a, pltpu.VMEM) for a in arrays]


def attn_call(layer, do_norm, lens, freq, x_in, gain, b_q, b_k, b_v, w_q, w_k, w_v, w_o, k_cache, v_cache, prev):
    batch, slots, head = k_cache.shape[-3:]
    width = x_in.shape[1]
    q_width = w_q.shape[2]
    any_spec = pl.BlockSpec(memory_space=pltpu.HBM)
    vmem = pl.BlockSpec(memory_space=pltpu.VMEM)
    aliased = prev is not None
    place = in_hbm if do_norm else in_vmem
    args = [lens, lens.reshape(1, batch), freq, *place(x_in), gain, b_q, b_k, b_v, *in_hbm(w_q, w_k, w_v, w_o, k_cache, v_cache)]
    in_specs = [pl.BlockSpec(memory_space=pltpu.SMEM), vmem, vmem, any_spec if do_norm else vmem, vmem, vmem, vmem, vmem] + [any_spec] * 6
    aliases = {}
    if aliased:
        aliases = {len(args): 3, len(args) + 1: 1, len(args) + 2: 2}
        args += [*in_vmem(prev[0]), *in_hbm(*prev[1:])]
        in_specs += [vmem] + [any_spec] * 2
    cache_buf = pltpu.VMEM((2, batch, slots, head), BF16)
    out_cache = jax.ShapeDtypeStruct((w_q.shape[0], batch, slots, head), BF16)
    n_chunks = batch // SEQ_CHUNK
    macs = batch * width * (q_width + 2 * head) + 2 * batch * slots * q_width
    return pl.pallas_call(
        functools.partial(attn_kernel, layer, do_norm, aliased),
        out_shape=(
            pltpu.VMEM((batch, width), BF16),
            out_cache,
            out_cache,
        ) + ((cache_buf,) if aliased else ()),
        in_specs=in_specs,
        out_specs=(vmem, any_spec, any_spec) + ((vmem,) if aliased else ()),
        scratch_shapes=[
            pltpu.VMEM((batch, width), BF16),
            pltpu.VMEM((width, q_width + 2 * head), BF16),
            pltpu.VMEM((q_width, width), BF16),
            pltpu.VMEM((batch, q_width), F32),
            pltpu.VMEM((batch, head), F32),
            pltpu.VMEM((batch, head), F32),
            pltpu.VMEM((batch, head), jnp.int32),
            pltpu.VMEM((batch, q_width), F32),
            pltpu.VMEM((SEQ_CHUNK // 8, 16, slots), F32),
            pltpu.SemaphoreType.DMA,
            pltpu.SemaphoreType.DMA((4,)),
            pltpu.SemaphoreType.DMA((n_chunks,)),
            pltpu.SemaphoreType.DMA((n_chunks,)),
            pltpu.SemaphoreType.DMA((n_chunks,)),
            pltpu.SemaphoreType.DMA((n_chunks,)),
        ] + ([] if aliased else [cache_buf]),
        input_output_aliases=aliases,
        compiler_params=pltpu.CompilerParams(vmem_limit_bytes=ATTN_VMEM + (0 if aliased else 4 * batch * slots * head)),
        cost_estimate=pl.CostEstimate(flops=2 * macs, bytes_accessed=4 * batch * slots * head * 2, transcendentals=batch * slots * 2),
        name=f"attn{layer}",
    )(*args)[:3]


def mix_kernel(layer, last, part_ref, x_hbm, gm_ref, gn_ref, wg_hbm, wu_hbm, wd_hbm, kc_hbm, vc_hbm, *refs):
    if last:
        out_hbm = refs[0]
        refs = refs[1:]
    else:
        out_hbm, xs_ref, kv_next = refs[:3]
        refs = refs[3:]
    (wg, wu, wd, x_own, act, part2, d_recv, r_send, r_recv, gathered,
     w_sem, x_sem, ds_sem, dr_sem, rs_sem, rr_sem, as_sem, ar_sem, fs_sem, fr_sem, o_sem, c_sem) = refs
    width = wg.shape[0]
    parts = (part_ref, part2)
    hidden = wg.shape[1]
    rows = part_ref.shape[0] // ROW_CHUNKS
    core_rows = rows // 2
    blk = core_rows // 4
    me = lax.axis_index("tp")
    core = me % 2
    chip = me // 2
    partner = me + 1 - 2 * core
    peer_y = (chip + 2) % 4
    peer_x = chip + 1 - 2 * (chip % 2)
    peers = [chip, peer_x * (1 - core) + peer_y * core, peer_y * (1 - core) + peer_x * core, 3 - chip]

    def dev(idx):
        return {"tp": idx}

    w_copies = [pltpu.make_async_copy(src.at[layer], dst, w_sem.at[i])
                for i, (src, dst) in enumerate(((wg_hbm, wg), (wu_hbm, wu), (wd_hbm, wd)))]

    def own_rows(j):
        return pl.ds(pl.multiple_of(j * rows + core * core_rows + chip * blk, blk), blk)

    x_copies = []
    for j in range(ROW_CHUNKS):
        if layer:
            x_own[j] = x_hbm[j]
        else:
            x_copies.append(pltpu.make_async_copy(x_hbm.at[own_rows(j)], x_own.at[j], x_sem.at[j]))
            x_copies[-1].start()

    c_copies = []
    if not last:
        size = kv_next.shape[1] // PARTS
        for n in range(PREFETCHED):
            for i, src in enumerate((kc_hbm, vc_hbm)):
                part = pl.ds(n * size, size)
                c_copies.append(pltpu.make_async_copy(src.at[layer + 1, part], kv_next.at[i, part], c_sem.at[i, n]))

    def prefetch(count):
        for _ in range(min(count, len(waiting))):
            waiting.pop(0).start()

    waiting = list(c_copies)
    prefetch(2)
    barrier = pltpu.get_barrier_semaphore()
    others = [partner] + [2 * peers[r] + core for r in range(1, 4)]
    for other in others:
        pl.semaphore_signal(barrier, inc=1, device_id=dev(other), device_id_type=pl.DeviceIdType.MESH)

    def remote(src, dst, send, recv, target):
        return pltpu.make_async_remote_copy(src_ref=src, dst_ref=dst, send_sem=send, recv_sem=recv,
                                            device_id=dev(target), device_id_type=pl.DeviceIdType.MESH)

    def d_copy(s, j):
        here = pl.ds(pl.multiple_of(j * rows + (1 - core) * core_rows, core_rows), core_rows)
        return remote(parts[s].at[here], d_recv.at[s, j], ds_sem.at[s, j], dr_sem.at[s, j], partner)

    def r_copy(s, j, r):
        return remote(r_send.at[s, j, r], r_recv.at[s, j, r], rs_sem.at[s, j, r], rr_sem.at[s, j, r], 2 * peers[r] + core)

    def scatter(s, j):
        d_copy(s, j).wait()
        for r in (3, 1, 2):
            off = pl.multiple_of(peers[r] * blk, blk)
            mine = parts[s][pl.ds(pl.multiple_of(j * rows + core * core_rows + off, blk), blk), :].astype(F32)
            r_send[s, j, r] = (mine + d_recv[s, j, pl.ds(off, blk), :].astype(F32)).astype(BF16)
            r_copy(s, j, r).start()

    def reduce(s, j):
        off = pl.multiple_of(chip * blk, blk)
        total = parts[s][own_rows(j), :].astype(F32) + d_recv[s, j, pl.ds(off, blk), :].astype(F32)
        for r in (1, 2, 3):
            r_copy(s, j, r).wait()
            total += r_recv[s, j, r].astype(F32)
        new = (x_own[j].astype(F32) + total).astype(BF16)
        x_own[j] = new
        return new

    def block_row(j, cc, k):
        return pl.ds(pl.multiple_of(j * rows + cc * core_rows + k * blk, blk), blk)

    def a_copy(s, j, r):
        here = block_row(j, core, chip)
        target = partner if r == 0 else 2 * peers[r] + core
        return remote(gathered.at[s, here], gathered.at[s, here], as_sem.at[s, j, r], ar_sem.at[s, j, r], target)

    def f_copy(s, j, r):
        here = block_row(j, core, peers[r])
        return remote(gathered.at[s, here], gathered.at[s, here], fs_sem.at[s, j, r], fr_sem.at[s, j, r], partner)

    def gather_start(s, j, value):
        gathered[s, block_row(j, core, chip), :] = value
        for r in (3, 1, 2, 0):
            a_copy(s, j, r).start()

    def gather_forward(s, j):
        for r in (1, 2, 3):
            a_copy(s, j, r).wait_recv()
            f_copy(s, j, r).start()

    def gather_finish(s, j):
        a_copy(s, j, 0).wait_recv()
        for r in (1, 2, 3):
            f_copy(s, j, r).wait_recv()

    chunks = range(ROW_CHUNKS)
    per = MLP_CHUNKS
    pl.semaphore_wait(barrier, len(others))
    for j in chunks:
        d_copy(0, j).start()
    for copy in x_copies:
        copy.wait()
    for j in chunks:
        scatter(0, j)
    for copy in w_copies:
        copy.start()
    for j in chunks:
        new = reduce(0, j)
        gather_start(0, j, norm_rows(new.astype(F32), gm_ref[layer:layer + 1, :].astype(F32)))
    prefetch(3)

    def mlp(first):
        here = slice(first * rows, (first + per) * rows)
        step = 256
        lhs = gathered[0, here, :]
        for col in range(0, hidden, step):
            cols = slice(col, col + step)
            gate = jnp.dot(lhs, wg[:, cols], preferred_element_type=F32)
            up = jnp.dot(lhs, wu[:, cols], preferred_element_type=F32)
            act[here, cols] = (gate * jax.nn.sigmoid(gate) * up).astype(BF16)
        lhs = act[here, :]
        for col in range(0, width, 2 * step):
            cols = slice(col, col + 2 * step)
            part2[here, cols] = jnp.dot(lhs, wd[:, cols], preferred_element_type=F32).astype(BF16)
        for j in range(first, first + per):
            d_copy(1, j).start()

    for j in range(per):
        gather_forward(0, j)
    for copy in w_copies:
        copy.wait()
    for first in range(0, ROW_CHUNKS, per):
        for j in range(first, first + per):
            gather_finish(0, j)
        prefetch(3)
        mlp(first)
        for j in range(first + per, min(first + 2 * per, ROW_CHUNKS)):
            gather_forward(0, j)
        for j in range(first, first + per):
            scatter(1, j)

    def second(j):
        new = reduce(1, j)
        if last:
            gather_start(1, j, new)
        else:
            xs_ref[j] = new
            gather_start(1, j, norm_rows(new.astype(F32), gn_ref[layer + 1:layer + 2, :].astype(F32)))

    for j in chunks:
        second(j)
    prefetch(1)
    for j in chunks:
        gather_forward(1, j)
    prefetch(len(waiting))
    outs = []
    for j in chunks:
        gather_finish(1, j)
        here = pl.ds(j * rows, rows)
        if last:
            outs.append(pltpu.make_async_copy(gathered.at[1, here], out_hbm.at[here], o_sem.at[j]))
            outs[-1].start()
        else:
            out_hbm[here, :] = gathered[1, here, :]
    for s in range(2):
        for j in range(ROW_CHUNKS):
            for r in range(4):
                a_copy(s, j, r).wait_send()
            for r in range(1, 4):
                f_copy(s, j, r).wait_send()
    for copy in outs + c_copies:
        copy.wait()


def mix_call(layer, last, part, x_own, g_mlp, g_attn, w_gate, w_up, w_down, k_cache, v_cache):
    batch, width = part.shape
    hidden = w_gate.shape[2]
    rows = batch // ROW_CHUNKS
    blk = rows // 8
    any_spec = pl.BlockSpec(memory_space=pltpu.HBM)
    vmem = pl.BlockSpec(memory_space=pltpu.VMEM)
    if last:
        out_shape = [jax.ShapeDtypeStruct((batch, width), BF16)]
        out_specs = [any_spec]
    else:
        out_shape = [pltpu.VMEM((batch, width), BF16), pltpu.VMEM((ROW_CHUNKS, blk, width), BF16)]
        out_shape.append(pltpu.VMEM((2,) + k_cache.shape[1:], BF16))
        out_specs = [vmem] * 3
    sem = pltpu.SemaphoreType.DMA
    nc = ROW_CHUNKS
    return pl.pallas_call(
        functools.partial(mix_kernel, layer, last),
        out_shape=out_shape,
        in_specs=[vmem, any_spec if layer == 0 else vmem, vmem, vmem] + [any_spec] * 5,
        out_specs=out_specs,
        scratch_shapes=[
            pltpu.VMEM((width, hidden), BF16),
            pltpu.VMEM((width, hidden), BF16),
            pltpu.VMEM((hidden, width), BF16),
            pltpu.VMEM((nc, blk, width), BF16),
            pltpu.VMEM((batch, hidden), BF16),
            pltpu.VMEM((batch, width), BF16),
            pltpu.VMEM((2, nc, rows // 2, width), BF16),
            pltpu.VMEM((2, nc, 4, blk, width), BF16),
            pltpu.VMEM((2, nc, 4, blk, width), BF16),
            pltpu.VMEM((2, batch, width), BF16),
            sem((3,)), sem((nc,)),
            sem((2, nc)), sem((2, nc)),
            sem((2, nc, 4)), sem((2, nc, 4)),
            sem((2, nc, 4)), sem((2, nc, 4)),
            sem((2, nc, 4)), sem((2, nc, 4)),
            sem((nc,)), sem((2, PREFETCHED)),
        ],
        compiler_params=pltpu.CompilerParams(collective_id=layer, has_side_effects=True, vmem_limit_bytes=MIX_VMEM),
        cost_estimate=pl.CostEstimate(flops=6 * batch * width * hidden, bytes_accessed=6 * width * hidden, transcendentals=batch * hidden),
        name=f"mix{layer}",
    )(*in_vmem(part), *(in_hbm if layer == 0 else in_vmem)(x_own), g_mlp, g_attn, *in_hbm(w_gate, w_up, w_down, k_cache, v_cache))


def solution(mesh):
    weight_col = P(None, None, "tp")
    weight_row = P(None, "tp", None)
    bias_col = P(None, "tp")
    cache_spec = P(None, "dp", None, "tp", None)
    in_specs = (P("dp", None), P("dp"), P(None, None), P(None, None), weight_col, bias_col, weight_col, bias_col, weight_col, bias_col, weight_row, weight_col, weight_col, weight_row, cache_spec, cache_spec)
    out_specs = (P("dp", None), cache_spec, cache_spec)

    def local_step(x_in, seq_lens, g_attn, g_mlp, w_q, b_q, w_k, b_k, w_v, b_v, w_o, w_gate, w_up, w_down, k_cache, v_cache):
        layers, batch, slots, _, head = k_cache.shape
        inv_freq = ROPE_THETA ** (-2.0 * np.arange(head // 2) / head)
        freq = jnp.asarray(np.concatenate([inv_freq, inv_freq])[None, :].astype(np.float32))
        k_flat = k_cache.reshape(layers, batch, slots, head)
        v_flat = v_cache.reshape(layers, batch, slots, head)
        normed, x_own, prev = x_in, x_in, None
        for layer in range(layers):
            last = layer == layers - 1
            part, k_out, v_out = attn_call(layer, layer == 0, seq_lens, freq, normed, g_attn, b_q, b_k, b_v, w_q, w_k, w_v, w_o, k_flat, v_flat, prev)
            outs = mix_call(layer, last, part, x_own, g_mlp, g_attn, w_gate, w_up, w_down, k_flat, v_flat)
            if last:
                x_out = outs[0]
            else:
                normed, x_own, prev = outs[0], outs[1], (outs[2], k_out, v_out)
        return x_out, k_out.reshape(k_cache.shape), v_out.reshape(v_cache.shape)

    return jax.shard_map(local_step, mesh=mesh, in_specs=in_specs, out_specs=out_specs, check_vma=False)
```

```python
import functools
import math

import jax
import jax.numpy as jnp
import numpy as np
from jax import lax
from jax.experimental import pallas as pl
from jax.experimental.pallas import tpu as pltpu
from jax.sharding import PartitionSpec as P

ROPE_THETA = 1000000.0
EPS = 1e-6
F32 = jnp.float32
BF16 = jnp.bfloat16
NT = (((1,), (1,)), ((), ()))
SEQ_CHUNK = 16
ROW_CHUNKS = 4
MLP_CHUNKS = 2
PARTS = 8
PREFETCHED = 6
ATTN_VMEM = 24 * 1024 * 1024
MIX_VMEM = 22 * 1024 * 1024


def norm_rows(vec_f32, gain_row):
    mean_sq = jnp.mean(vec_f32 * vec_f32, axis=-1, keepdims=True)
    return (vec_f32 * lax.rsqrt(mean_sq + EPS) * gain_row).astype(BF16)


def attn_kernel(layer, do_norm, aliased, *refs):
    (lens_smem, lens_row, freq, x_hbm, g_ref, bq_ref, bk_ref, bv_ref, wq_hbm, wk_hbm, wv_hbm, wo_hbm, kc_hbm, vc_hbm) = refs[:14]
    refs = refs[17 if aliased else 14:]
    part_ref, ko_hbm, vo_hbm = refs[:3]
    refs = refs[3:]
    kv_buf = refs[0] if aliased else refs[-1]
    k_buf, v_buf = kv_buf.at[0], kv_buf.at[1]
    refs = refs[1:] if aliased else refs[:-1]
    (x_buf, w_buf, wo, q_f32, k_f32, v_f32, lens_col, out_f32, s_buf, x_sem, w_sem, k_sem, v_sem, ko_sem, vo_sem) = refs
    batch, slots, head = k_buf.shape
    q_width = wq_hbm.shape[2]
    n_chunks = batch // SEQ_CHUNK

    if do_norm:
        x_copy = pltpu.make_async_copy(x_hbm, x_buf, x_sem)
        x_copy.start()
    w_copies = [
        pltpu.make_async_copy(wq_hbm.at[layer], w_buf.at[:, :q_width], w_sem.at[0]),
        pltpu.make_async_copy(wk_hbm.at[layer], w_buf.at[:, q_width:q_width + head], w_sem.at[1]),
        pltpu.make_async_copy(wv_hbm.at[layer], w_buf.at[:, q_width + head:], w_sem.at[2]),
    ]
    for copy in w_copies:
        copy.start()
    first_read = n_chunks * PREFETCHED // PARTS if aliased else 0
    wo_copy = pltpu.make_async_copy(wo_hbm.at[layer], wo, w_sem.at[3])

    def chunk_copies(idx):
        rows = pl.ds(pl.multiple_of(idx * SEQ_CHUNK, SEQ_CHUNK), SEQ_CHUNK)
        return (
            pltpu.make_async_copy(kc_hbm.at[layer, rows], k_buf.at[rows], k_sem.at[idx]),
            pltpu.make_async_copy(vc_hbm.at[layer, rows], v_buf.at[rows], v_sem.at[idx]),
            pltpu.make_async_copy(k_buf.at[rows], ko_hbm.at[layer, rows], ko_sem.at[idx]),
            pltpu.make_async_copy(v_buf.at[rows], vo_hbm.at[layer, rows], vo_sem.at[idx]),
        )

    @pl.loop(first_read, n_chunks)
    def _(idx):
        k_in, v_in, _, _ = chunk_copies(idx)
        k_in.start()
        v_in.start()

    wo_copy.start()

    lens_f = lens_row[...].astype(F32)
    same = lax.broadcasted_iota(jnp.int32, (batch, batch), 0) == lax.broadcasted_iota(jnp.int32, (batch, batch), 1)
    pos_col = jnp.sum(jnp.where(same, jnp.broadcast_to(lens_f, (batch, batch)), 0.0), axis=1, keepdims=True)
    lens_col[...] = jnp.broadcast_to(pos_col, (batch, head)).astype(jnp.int32)
    angles = pos_col * freq[...]
    cos_tab = jnp.cos(angles)
    lane = lax.broadcasted_iota(jnp.int32, (1, head), 1)
    sin_tab = jnp.sin(angles) * jnp.where(lane < head // 2, -1.0, 1.0)

    def rope(vec):
        return vec * cos_tab + pltpu.roll(vec, head // 2, 1) * sin_tab

    for copy in w_copies:
        copy.wait()
    if do_norm:
        x_copy.wait()
        normed = norm_rows(x_buf[...].astype(F32), g_ref[layer:layer + 1, :].astype(F32))
    else:
        normed = x_hbm[...]
    part = jnp.dot(normed, w_buf[:, :q_width], preferred_element_type=F32) + bq_ref[layer:layer + 1, :].astype(F32)
    for col in range(q_width // head):
        cols = slice(col * head, (col + 1) * head)
        q_f32[:, cols] = rope(part[:, cols]).astype(BF16).astype(F32)
    part = jnp.dot(normed, w_buf[:, q_width:], preferred_element_type=F32)
    k_f32[...] = rope(part[:, :head] + bk_ref[layer:layer + 1, :].astype(F32)).astype(BF16).astype(F32)
    v_f32[...] = (part[:, head:] + bv_ref[layer:layer + 1, :].astype(F32)).astype(BF16).astype(F32)

    half = 8
    scale = head ** -0.5
    row_in_group = lax.broadcasted_iota(jnp.int32, (2 * half, head), 0) % half
    slot_id = lax.broadcasted_iota(jnp.int32, (2 * half, slots), 1)
    tile_row = lax.broadcasted_iota(jnp.int32, (16, head), 0)

    def patch(idx):
        for sub in range(SEQ_CHUNK):
            seq = idx * SEQ_CHUNK + sub
            pos = lens_smem[seq]
            base = pl.multiple_of((pos >> 4) << 4, 16)
            hit = tile_row == pos - base
            for buf, new in ((k_buf, k_f32), (v_buf, v_f32)):
                row = jnp.broadcast_to(new[pl.ds(seq, 1), :], (16, head))
                old = buf[seq, pl.ds(base, 16), :]
                buf[seq, pl.ds(base, 16), :] = jnp.where(hit, row, old.astype(F32)).astype(BF16)

    groups = SEQ_CHUNK // half

    def first_row(idx, group):
        return pl.multiple_of(idx * SEQ_CHUNK + group * half, half)

    def scores_of(idx, group):
        first = first_row(idx, group)
        q_rows = q_f32[pl.ds(first, half), :]
        q_all = jnp.concatenate([q_rows[:, :head], q_rows[:, head:]], axis=0)
        scores = jnp.zeros((2 * half, slots), F32)
        for pair in range(half // 2):
            lhs = jnp.concatenate([jnp.where(row_in_group == 2 * pair + e, q_all, 0.0) for e in range(2)], axis=1).astype(BF16)
            rhs = jnp.concatenate([k_buf[first + 2 * pair + e] for e in range(2)], axis=1)
            scores += lax.dot_general(lhs, rhs, NT, preferred_element_type=F32)
        return scores

    def probs_of(idx, group):
        pos_rows = lens_col[pl.ds(first_row(idx, group), half), 0:1]
        pos_all = jnp.concatenate([pos_rows, pos_rows], axis=0)
        scores = jnp.where(slot_id <= pos_all, s_buf[group] * scale, -1e30)
        expo = jnp.exp(scores - jnp.max(scores, axis=-1, keepdims=True))
        return (expo / jnp.sum(expo, axis=-1, keepdims=True)).astype(BF16)

    def values_of(idx, group, probs):
        first = first_row(idx, group)
        out = jnp.zeros((2 * half, head), F32)
        for pair in range(half // 2):
            rhs = jnp.concatenate([v_buf[first + 2 * pair + e] for e in range(2)], axis=1)
            both = jnp.dot(probs, rhs, preferred_element_type=F32)
            for e in range(2):
                out = jnp.where(row_in_group == 2 * pair + e, both[:, e * head:(e + 1) * head], out)
        return jnp.concatenate([out[:half], out[half:]], axis=1)

    def values_step(idx):
        probs = [probs_of(idx, group) for group in range(groups)]
        for group in range(groups):
            out_f32[pl.ds(first_row(idx, group), half), :] = values_of(idx, group, probs[group])

    s_buf[...] = jnp.zeros_like(s_buf)

    @pl.loop(0, n_chunks)
    def _(idx):
        k_in, v_in, k_out, v_out = chunk_copies(idx)
        if aliased:
            @pl.when(idx >= first_read)
            def _():
                k_in.wait()
                v_in.wait()
        else:
            k_in.wait()
            v_in.wait()

        values_step(jnp.maximum(idx - 1, 0))
        patch(idx)
        k_out.start()
        v_out.start()
        new_scores = [scores_of(idx, group) for group in range(groups)]
        for group in range(groups):
            s_buf[group] = new_scores[group]

    values_step(n_chunks - 1)

    wo_copy.wait()
    attn = out_f32[...].astype(BF16)
    step = 512
    for col in range(0, wo.shape[1], step):
        part_ref[:, col:col + step] = jnp.dot(attn, wo[:, col:col + step], preferred_element_type=F32).astype(BF16)

    @pl.loop(0, n_chunks)
    def _(idx):
        _, _, k_out, v_out = chunk_copies(idx)
        k_out.wait()
        v_out.wait()


def in_hbm(*arrays):
    return [pltpu.with_memory_space_constraint(a, pltpu.HBM) for a in arrays]


def in_vmem(*arrays):
    return [pltpu.with_memory_space_constraint(a, pltpu.VMEM) for a in arrays]


def attn_call(layer, do_norm, lens, freq, x_in, gain, b_q, b_k, b_v, w_q, w_k, w_v, w_o, k_cache, v_cache, prev):
    batch, slots, head = k_cache.shape[-3:]
    width = x_in.shape[1]
    q_width = w_q.shape[2]
    any_spec = pl.BlockSpec(memory_space=pltpu.HBM)
    vmem = pl.BlockSpec(memory_space=pltpu.VMEM)
    aliased = prev is not None
    place = in_hbm if do_norm else in_vmem
    args = [lens, lens.reshape(1, batch), freq, *place(x_in), gain, b_q, b_k, b_v, *in_hbm(w_q, w_k, w_v, w_o, k_cache, v_cache)]
    in_specs = [pl.BlockSpec(memory_space=pltpu.SMEM), vmem, vmem, any_spec if do_norm else vmem, vmem, vmem, vmem, vmem] + [any_spec] * 6
    aliases = {}
    if aliased:
        aliases = {len(args): 3, len(args) + 1: 1, len(args) + 2: 2}
        args += [*in_vmem(prev[0]), *in_hbm(*prev[1:])]
        in_specs += [vmem] + [any_spec] * 2
    cache_buf = pltpu.VMEM((2, batch, slots, head), BF16)
    out_cache = jax.ShapeDtypeStruct((w_q.shape[0], batch, slots, head), BF16)
    n_chunks = batch // SEQ_CHUNK
    macs = batch * width * (q_width + 2 * head) + 2 * batch * slots * q_width
    return pl.pallas_call(
        functools.partial(attn_kernel, layer, do_norm, aliased),
        out_shape=(
            pltpu.VMEM((batch, width), BF16),
            out_cache,
            out_cache,
        ) + ((cache_buf,) if aliased else ()),
        in_specs=in_specs,
        out_specs=(vmem, any_spec, any_spec) + ((vmem,) if aliased else ()),
        scratch_shapes=[
            pltpu.VMEM((batch, width), BF16),
            pltpu.VMEM((width, q_width + 2 * head), BF16),
            pltpu.VMEM((q_width, width), BF16),
            pltpu.VMEM((batch, q_width), F32),
            pltpu.VMEM((batch, head), F32),
            pltpu.VMEM((batch, head), F32),
            pltpu.VMEM((batch, head), jnp.int32),
            pltpu.VMEM((batch, q_width), F32),
            pltpu.VMEM((SEQ_CHUNK // 8, 16, slots), F32),
            pltpu.SemaphoreType.DMA,
            pltpu.SemaphoreType.DMA((4,)),
            pltpu.SemaphoreType.DMA((n_chunks,)),
            pltpu.SemaphoreType.DMA((n_chunks,)),
            pltpu.SemaphoreType.DMA((n_chunks,)),
            pltpu.SemaphoreType.DMA((n_chunks,)),
        ] + ([] if aliased else [cache_buf]),
        input_output_aliases=aliases,
        compiler_params=pltpu.CompilerParams(vmem_limit_bytes=ATTN_VMEM + (0 if aliased else 4 * batch * slots * head)),
        cost_estimate=pl.CostEstimate(flops=2 * macs, bytes_accessed=4 * batch * slots * head * 2, transcendentals=batch * slots * 2),
        name=f"attn{layer}",
    )(*args)[:3]


def mix_kernel(layer, last, part_ref, x_hbm, gm_ref, gn_ref, wg_hbm, wu_hbm, wd_hbm, kc_hbm, vc_hbm, *refs):
    if last:
        out_hbm = refs[0]
        refs = refs[1:]
    else:
        out_hbm, xs_ref, kv_next = refs[:3]
        refs = refs[3:]
    (wg, wu, wd, x_own, act, part2, d_recv, r_send, r_recv, gathered,
     w_sem, x_sem, ds_sem, dr_sem, rs_sem, rr_sem, as_sem, ar_sem, fs_sem, fr_sem, o_sem, c_sem) = refs
    width = wg.shape[0]
    parts = (part_ref, part2)
    hidden = wg.shape[1]
    rows = part_ref.shape[0] // ROW_CHUNKS
    core_rows = rows // 2
    blk = core_rows // 4
    me = lax.axis_index("tp")
    core = me % 2
    chip = me // 2
    partner = me + 1 - 2 * core
    peer_y = (chip + 2) % 4
    peer_x = chip + 1 - 2 * (chip % 2)
    peers = [chip, peer_x * (1 - core) + peer_y * core, peer_y * (1 - core) + peer_x * core, 3 - chip]

    def dev(idx):
        return {"tp": idx}

    w_copies = [pltpu.make_async_copy(src.at[layer], dst, w_sem.at[i])
                for i, (src, dst) in enumerate(((wg_hbm, wg), (wu_hbm, wu), (wd_hbm, wd)))]

    def own_rows(j):
        return pl.ds(pl.multiple_of(j * rows + core * core_rows + chip * blk, blk), blk)

    x_copies = []
    for j in range(ROW_CHUNKS):
        if layer:
            x_own[j] = x_hbm[j]
        else:
            x_copies.append(pltpu.make_async_copy(x_hbm.at[own_rows(j)], x_own.at[j], x_sem.at[j]))
            x_copies[-1].start()

    c_copies = []
    if not last:
        size = kv_next.shape[1] // PARTS
        for n in range(PREFETCHED):
            for i, src in enumerate((kc_hbm, vc_hbm)):
                part = pl.ds(n * size, size)
                c_copies.append(pltpu.make_async_copy(src.at[layer + 1, part], kv_next.at[i, part], c_sem.at[i, n]))

    def prefetch(count):
        for _ in range(min(count, len(waiting))):
            waiting.pop(0).start()

    waiting = list(c_copies)
    prefetch(2)
    barrier = pltpu.get_barrier_semaphore()
    others = [partner] + [2 * peers[r] + core for r in range(1, 4)]
    for other in others:
        pl.semaphore_signal(barrier, inc=1, device_id=dev(other), device_id_type=pl.DeviceIdType.MESH)

    def remote(src, dst, send, recv, target):
        return pltpu.make_async_remote_copy(src_ref=src, dst_ref=dst, send_sem=send, recv_sem=recv,
                                            device_id=dev(target), device_id_type=pl.DeviceIdType.MESH)

    def d_copy(s, j):
        here = pl.ds(pl.multiple_of(j * rows + (1 - core) * core_rows, core_rows), core_rows)
        return remote(parts[s].at[here], d_recv.at[s, j], ds_sem.at[s, j], dr_sem.at[s, j], partner)

    def r_copy(s, j, r):
        return remote(r_send.at[s, j, r], r_recv.at[s, j, r], rs_sem.at[s, j, r], rr_sem.at[s, j, r], 2 * peers[r] + core)

    def scatter(s, j):
        d_copy(s, j).wait()
        for r in (3, 1, 2):
            off = pl.multiple_of(peers[r] * blk, blk)
            mine = parts[s][pl.ds(pl.multiple_of(j * rows + core * core_rows + off, blk), blk), :].astype(F32)
            r_send[s, j, r] = (mine + d_recv[s, j, pl.ds(off, blk), :].astype(F32)).astype(BF16)
            r_copy(s, j, r).start()

    def reduce(s, j):
        off = pl.multiple_of(chip * blk, blk)
        total = parts[s][own_rows(j), :].astype(F32) + d_recv[s, j, pl.ds(off, blk), :].astype(F32)
        for r in (1, 2, 3):
            r_copy(s, j, r).wait()
            total += r_recv[s, j, r].astype(F32)
        new = (x_own[j].astype(F32) + total).astype(BF16)
        x_own[j] = new
        return new

    def block_row(j, cc, k):
        return pl.ds(pl.multiple_of(j * rows + cc * core_rows + k * blk, blk), blk)

    def a_copy(s, j, r):
        here = block_row(j, core, chip)
        target = partner if r == 0 else 2 * peers[r] + core
        return remote(gathered.at[s, here], gathered.at[s, here], as_sem.at[s, j, r], ar_sem.at[s, j, r], target)

    def f_copy(s, j, r):
        here = block_row(j, core, peers[r])
        return remote(gathered.at[s, here], gathered.at[s, here], fs_sem.at[s, j, r], fr_sem.at[s, j, r], partner)

    def gather_start(s, j, value):
        gathered[s, block_row(j, core, chip), :] = value
        for r in (3, 1, 2, 0):
            a_copy(s, j, r).start()

    def gather_forward(s, j):
        for r in (1, 2, 3):
            a_copy(s, j, r).wait_recv()
            f_copy(s, j, r).start()

    def gather_finish(s, j):
        a_copy(s, j, 0).wait_recv()
        for r in (1, 2, 3):
            f_copy(s, j, r).wait_recv()

    chunks = range(ROW_CHUNKS)
    per = MLP_CHUNKS
    pl.semaphore_wait(barrier, len(others))
    for j in chunks:
        d_copy(0, j).start()
    for copy in x_copies:
        copy.wait()
    for j in chunks:
        scatter(0, j)
    for copy in w_copies:
        copy.start()
    for j in chunks:
        new = reduce(0, j)
        gather_start(0, j, norm_rows(new.astype(F32), gm_ref[layer:layer + 1, :].astype(F32)))
    prefetch(3)

    def mlp(first):
        here = slice(first * rows, (first + per) * rows)
        step = 256
        lhs = gathered[0, here, :]
        for col in range(0, hidden, step):
            cols = slice(col, col + step)
            gate = jnp.dot(lhs, wg[:, cols], preferred_element_type=F32)
            up = jnp.dot(lhs, wu[:, cols], preferred_element_type=F32)
            act[here, cols] = (gate * jax.nn.sigmoid(gate) * up).astype(BF16)
        lhs = act[here, :]
        for col in range(0, width, 2 * step):
            cols = slice(col, col + 2 * step)
            part2[here, cols] = jnp.dot(lhs, wd[:, cols], preferred_element_type=F32).astype(BF16)
        for j in range(first, first + per):
            d_copy(1, j).start()

    for j in range(per):
        gather_forward(0, j)
    for copy in w_copies:
        copy.wait()
    for first in range(0, ROW_CHUNKS, per):
        for j in range(first, first + per):
            gather_finish(0, j)
        prefetch(3)
        mlp(first)
        for j in range(first + per, min(first + 2 * per, ROW_CHUNKS)):
            gather_forward(0, j)
        for j in range(first, first + per):
            scatter(1, j)

    def second(j):
        new = reduce(1, j)
        if last:
            gather_start(1, j, new)
        else:
            xs_ref[j] = new
            gather_start(1, j, norm_rows(new.astype(F32), gn_ref[layer + 1:layer + 2, :].astype(F32)))

    for j in chunks:
        second(j)
    prefetch(1)
    for j in chunks:
        gather_forward(1, j)
    prefetch(len(waiting))
    outs = []
    for j in chunks:
        gather_finish(1, j)
        here = pl.ds(j * rows, rows)
        if last:
            outs.append(pltpu.make_async_copy(gathered.at[1, here], out_hbm.at[here], o_sem.at[j]))
            outs[-1].start()
        else:
            out_hbm[here, :] = gathered[1, here, :]
    for s in range(2):
        for j in range(ROW_CHUNKS):
            for r in range(4):
                a_copy(s, j, r).wait_send()
            for r in range(1, 4):
                f_copy(s, j, r).wait_send()
    for copy in outs + c_copies:
        copy.wait()


def mix_call(layer, last, part, x_own, g_mlp, g_attn, w_gate, w_up, w_down, k_cache, v_cache):
    batch, width = part.shape
    hidden = w_gate.shape[2]
    rows = batch // ROW_CHUNKS
    blk = rows // 8
    any_spec = pl.BlockSpec(memory_space=pltpu.HBM)
    vmem = pl.BlockSpec(memory_space=pltpu.VMEM)
    if last:
        out_shape = [jax.ShapeDtypeStruct((batch, width), BF16)]
        out_specs = [any_spec]
    else:
        out_shape = [pltpu.VMEM((batch, width), BF16), pltpu.VMEM((ROW_CHUNKS, blk, width), BF16)]
        out_shape.append(pltpu.VMEM((2,) + k_cache.shape[1:], BF16))
        out_specs = [vmem] * 3
    sem = pltpu.SemaphoreType.DMA
    nc = ROW_CHUNKS
    return pl.pallas_call(
        functools.partial(mix_kernel, layer, last),
        out_shape=out_shape,
        in_specs=[vmem, any_spec if layer == 0 else vmem, vmem, vmem] + [any_spec] * 5,
        out_specs=out_specs,
        scratch_shapes=[
            pltpu.VMEM((width, hidden), BF16),
            pltpu.VMEM((width, hidden), BF16),
            pltpu.VMEM((hidden, width), BF16),
            pltpu.VMEM((nc, blk, width), BF16),
            pltpu.VMEM((batch, hidden), BF16),
            pltpu.VMEM((batch, width), BF16),
            pltpu.VMEM((2, nc, rows // 2, width), BF16),
            pltpu.VMEM((2, nc, 4, blk, width), BF16),
            pltpu.VMEM((2, nc, 4, blk, width), BF16),
            pltpu.VMEM((2, batch, width), BF16),
            sem((3,)), sem((nc,)),
            sem((2, nc)), sem((2, nc)),
            sem((2, nc, 4)), sem((2, nc, 4)),
            sem((2, nc, 4)), sem((2, nc, 4)),
            sem((2, nc, 4)), sem((2, nc, 4)),
            sem((nc,)), sem((2, PREFETCHED)),
        ],
        compiler_params=pltpu.CompilerParams(collective_id=layer, has_side_effects=True, vmem_limit_bytes=MIX_VMEM),
        cost_estimate=pl.CostEstimate(flops=6 * batch * width * hidden, bytes_accessed=6 * width * hidden, transcendentals=batch * hidden),
        name=f"mix{layer}",
    )(*in_vmem(part), *(in_hbm if layer == 0 else in_vmem)(x_own), g_mlp, g_attn, *in_hbm(w_gate, w_up, w_down, k_cache, v_cache))


def solution(mesh):
    weight_col = P(None, None, "tp")
    weight_row = P(None, "tp", None)
    bias_col = P(None, "tp")
    cache_spec = P(None, "dp", None, "tp", None)
    in_specs = (P("dp", None), P("dp"), P(None, None), P(None, None), weight_col, bias_col, weight_col, bias_col, weight_col, bias_col, weight_row, weight_col, weight_col, weight_row, cache_spec, cache_spec)
    out_specs = (P("dp", None), cache_spec, cache_spec)

    def local_step(x_in, seq_lens, g_attn, g_mlp, w_q, b_q, w_k, b_k, w_v, b_v, w_o, w_gate, w_up, w_down, k_cache, v_cache):
        layers, batch, slots, _, head = k_cache.shape
        inv_freq = ROPE_THETA ** (-2.0 * np.arange(head // 2) / head)
        freq = jnp.asarray(np.concatenate([inv_freq, inv_freq])[None, :].astype(np.float32))
        k_flat = k_cache.reshape(layers, batch, slots, head)
        v_flat = v_cache.reshape(layers, batch, slots, head)
        normed, x_own, prev = x_in, x_in, None
        for layer in range(layers):
            last = layer == layers - 1
            part, k_out, v_out = attn_call(layer, layer == 0, seq_lens, freq, normed, g_attn, b_q, b_k, b_v, w_q, w_k, w_v, w_o, k_flat, v_flat, prev)
            outs = mix_call(layer, last, part, x_own, g_mlp, g_attn, w_gate, w_up, w_down, k_flat, v_flat)
            if last:
                x_out = outs[0]
            else:
                normed, x_own, prev = outs[0], outs[1], (outs[2], k_out, v_out)
        return x_out, k_out.reshape(k_cache.shape), v_out.reshape(v_cache.shape)

    return jax.shard_map(local_step, mesh=mesh, in_specs=in_specs, out_specs=out_specs, check_vma=False)
```

```python
import functools
import math

import jax
import jax.numpy as jnp
import numpy as np
from jax import lax
from jax.experimental import pallas as pl
from jax.experimental.pallas import tpu as pltpu
from jax.sharding import PartitionSpec as P

ROPE_THETA = 1000000.0
EPS = 1e-6
F32 = jnp.float32
BF16 = jnp.bfloat16
NT = (((1,), (1,)), ((), ()))
SEQ_CHUNK = 16
ROW_CHUNKS = 4
MLP_CHUNKS = 2
PARTS = 8
PREFETCHED = 6
ATTN_VMEM = 24 * 1024 * 1024
MIX_VMEM = 22 * 1024 * 1024


def norm_rows(vec_f32, gain_row):
    mean_sq = jnp.mean(vec_f32 * vec_f32, axis=-1, keepdims=True)
    return (vec_f32 * lax.rsqrt(mean_sq + EPS) * gain_row).astype(BF16)


def attn_kernel(layer, do_norm, aliased, *refs):
    (lens_smem, lens_row, freq, x_hbm, g_ref, bq_ref, bk_ref, bv_ref, wq_hbm, wk_hbm, wv_hbm, wo_hbm, kc_hbm, vc_hbm) = refs[:14]
    refs = refs[17 if aliased else 14:]
    part_ref, ko_hbm, vo_hbm = refs[:3]
    refs = refs[3:]
    kv_buf = refs[0] if aliased else refs[-1]
    k_buf, v_buf = kv_buf.at[0], kv_buf.at[1]
    refs = refs[1:] if aliased else refs[:-1]
    (x_buf, w_buf, wo, q_f32, k_f32, v_f32, lens_col, out_f32, s_buf, x_sem, w_sem, k_sem, v_sem, ko_sem, vo_sem) = refs
    batch, slots, head = k_buf.shape
    q_width = wq_hbm.shape[2]
    n_chunks = batch // SEQ_CHUNK

    if do_norm:
        x_copy = pltpu.make_async_copy(x_hbm, x_buf, x_sem)
        x_copy.start()
    w_copies = [
        pltpu.make_async_copy(wq_hbm.at[layer], w_buf.at[:, :q_width], w_sem.at[0]),
        pltpu.make_async_copy(wk_hbm.at[layer], w_buf.at[:, q_width:q_width + head], w_sem.at[1]),
        pltpu.make_async_copy(wv_hbm.at[layer], w_buf.at[:, q_width + head:], w_sem.at[2]),
    ]
    for copy in w_copies:
        copy.start()
    first_read = n_chunks * PREFETCHED // PARTS if aliased else 0
    wo_copy = pltpu.make_async_copy(wo_hbm.at[layer], wo, w_sem.at[3])

    def chunk_copies(idx):
        rows = pl.ds(pl.multiple_of(idx * SEQ_CHUNK, SEQ_CHUNK), SEQ_CHUNK)
        return (
            pltpu.make_async_copy(kc_hbm.at[layer, rows], k_buf.at[rows], k_sem.at[idx]),
            pltpu.make_async_copy(vc_hbm.at[layer, rows], v_buf.at[rows], v_sem.at[idx]),
            pltpu.make_async_copy(k_buf.at[rows], ko_hbm.at[layer, rows], ko_sem.at[idx]),
            pltpu.make_async_copy(v_buf.at[rows], vo_hbm.at[layer, rows], vo_sem.at[idx]),
        )

    @pl.loop(first_read, n_chunks)
    def _(idx):
        k_in, v_in, _, _ = chunk_copies(idx)
        k_in.start()
        v_in.start()

    wo_copy.start()

    lens_f = lens_row[...].astype(F32)
    same = lax.broadcasted_iota(jnp.int32, (batch, batch), 0) == lax.broadcasted_iota(jnp.int32, (batch, batch), 1)
    pos_col = jnp.sum(jnp.where(same, jnp.broadcast_to(lens_f, (batch, batch)), 0.0), axis=1, keepdims=True)
    lens_col[...] = jnp.broadcast_to(pos_col, (batch, head)).astype(jnp.int32)
    angles = pos_col * freq[...]
    cos_tab = jnp.cos(angles)
    lane = lax.broadcasted_iota(jnp.int32, (1, head), 1)
    sin_tab = jnp.sin(angles) * jnp.where(lane < head // 2, -1.0, 1.0)

    def rope(vec):
        return vec * cos_tab + pltpu.roll(vec, head // 2, 1) * sin_tab

    for copy in w_copies:
        copy.wait()
    if do_norm:
        x_copy.wait()
        normed = norm_rows(x_buf[...].astype(F32), g_ref[layer:layer + 1, :].astype(F32))
    else:
        normed = x_hbm[...]
    part = jnp.dot(normed, w_buf[:, :q_width], preferred_element_type=F32) + bq_ref[layer:layer + 1, :].astype(F32)
    for col in range(q_width // head):
        cols = slice(col * head, (col + 1) * head)
        q_f32[:, cols] = rope(part[:, cols]).astype(BF16).astype(F32)
    part = jnp.dot(normed, w_buf[:, q_width:], preferred_element_type=F32)
    k_f32[...] = rope(part[:, :head] + bk_ref[layer:layer + 1, :].astype(F32)).astype(BF16).astype(F32)
    v_f32[...] = (part[:, head:] + bv_ref[layer:layer + 1, :].astype(F32)).astype(BF16).astype(F32)

    half = 8
    scale = head ** -0.5
    row_in_group = lax.broadcasted_iota(jnp.int32, (2 * half, head), 0) % half
    slot_id = lax.broadcasted_iota(jnp.int32, (2 * half, slots), 1)
    tile_row = lax.broadcasted_iota(jnp.int32, (16, head), 0)

    def patch(idx):
        for sub in range(SEQ_CHUNK):
            seq = idx * SEQ_CHUNK + sub
            pos = lens_smem[seq]
            base = pl.multiple_of((pos >> 4) << 4, 16)
            hit = tile_row == pos - base
            for buf, new in ((k_buf, k_f32), (v_buf, v_f32)):
                row = jnp.broadcast_to(new[pl.ds(seq, 1), :], (16, head))
                old = buf[seq, pl.ds(base, 16), :]
                buf[seq, pl.ds(base, 16), :] = jnp.where(hit, row, old.astype(F32)).astype(BF16)

    groups = SEQ_CHUNK // half

    def first_row(idx, group):
        return pl.multiple_of(idx * SEQ_CHUNK + group * half, half)

    def scores_of(idx, group):
        first = first_row(idx, group)
        q_rows = q_f32[pl.ds(first, half), :]
        q_all = jnp.concatenate([q_rows[:, :head], q_rows[:, head:]], axis=0)
        scores = jnp.zeros((2 * half, slots), F32)
        for pair in range(half // 2):
            lhs = jnp.concatenate([jnp.where(row_in_group == 2 * pair + e, q_all, 0.0) for e in range(2)], axis=1).astype(BF16)
            rhs = jnp.concatenate([k_buf[first + 2 * pair + e] for e in range(2)], axis=1)
            scores += lax.dot_general(lhs, rhs, NT, preferred_element_type=F32)
        return scores

    def probs_of(idx, group):
        pos_rows = lens_col[pl.ds(first_row(idx, group), half), 0:1]
        pos_all = jnp.concatenate([pos_rows, pos_rows], axis=0)
        scores = jnp.where(slot_id <= pos_all, s_buf[group] * scale, -1e30)
        expo = jnp.exp(scores - jnp.max(scores, axis=-1, keepdims=True))
        return (expo / jnp.sum(expo, axis=-1, keepdims=True)).astype(BF16)

    def values_of(idx, group, probs):
        first = first_row(idx, group)
        out = jnp.zeros((2 * half, head), F32)
        for pair in range(half // 2):
            rhs = jnp.concatenate([v_buf[first + 2 * pair + e] for e in range(2)], axis=1)
            both = jnp.dot(probs, rhs, preferred_element_type=F32)
            for e in range(2):
                out = jnp.where(row_in_group == 2 * pair + e, both[:, e * head:(e + 1) * head], out)
        return jnp.concatenate([out[:half], out[half:]], axis=1)

    def values_step(idx, probs):
        for group in range(groups):
            out_f32[pl.ds(first_row(idx, group), half), :] = values_of(idx, group, probs[group])

    def step(idx, now):
        new_scores = [scores_of(idx, group) for group in range(groups)]
        values_step(now, [probs_of(now, group) for group in range(groups)])
        for group in range(groups):
            s_buf[group] = new_scores[group]

    def arrive(idx):
        k_in, v_in, _, _ = chunk_copies(idx)
        k_in.wait()
        v_in.wait()

    def leave(idx):
        _, _, k_out, v_out = chunk_copies(idx)
        k_out.start()
        v_out.start()

    s_buf[...] = jnp.zeros_like(s_buf)
    if not aliased:
        arrive(0)
    patch(0)
    leave(0)

    @pl.loop(0, n_chunks - 1)
    def _(idx):
        if aliased:
            pl.when(idx + 1 >= first_read)(lambda: arrive(idx + 1))
        else:
            arrive(idx + 1)
        step(idx, jnp.maximum(idx - 1, 0))
        patch(idx + 1)
        leave(idx + 1)

    step(n_chunks - 1, n_chunks - 2)
    values_step(n_chunks - 1, [probs_of(n_chunks - 1, group) for group in range(groups)])

    wo_copy.wait()
    attn = out_f32[...].astype(BF16)
    block = 512
    for col in range(0, wo.shape[1], block):
        part_ref[:, col:col + block] = jnp.dot(attn, wo[:, col:col + block], preferred_element_type=F32).astype(BF16)

    @pl.loop(0, n_chunks)
    def _(idx):
        _, _, k_out, v_out = chunk_copies(idx)
        k_out.wait()
        v_out.wait()


def in_hbm(*arrays):
    return [pltpu.with_memory_space_constraint(a, pltpu.HBM) for a in arrays]


def in_vmem(*arrays):
    return [pltpu.with_memory_space_constraint(a, pltpu.VMEM) for a in arrays]


def attn_call(layer, do_norm, lens, freq, x_in, gain, b_q, b_k, b_v, w_q, w_k, w_v, w_o, k_cache, v_cache, prev):
    batch, slots, head = k_cache.shape[-3:]
    width = x_in.shape[1]
    q_width = w_q.shape[2]
    any_spec = pl.BlockSpec(memory_space=pltpu.HBM)
    vmem = pl.BlockSpec(memory_space=pltpu.VMEM)
    aliased = prev is not None
    place = in_hbm if do_norm else in_vmem
    args = [lens, lens.reshape(1, batch), freq, *place(x_in), gain, b_q, b_k, b_v, *in_hbm(w_q, w_k, w_v, w_o, k_cache, v_cache)]
    in_specs = [pl.BlockSpec(memory_space=pltpu.SMEM), vmem, vmem, any_spec if do_norm else vmem, vmem, vmem, vmem, vmem] + [any_spec] * 6
    aliases = {}
    if aliased:
        aliases = {len(args): 3, len(args) + 1: 1, len(args) + 2: 2}
        args += [*in_vmem(prev[0]), *in_hbm(*prev[1:])]
        in_specs += [vmem] + [any_spec] * 2
    cache_buf = pltpu.VMEM((2, batch, slots, head), BF16)
    out_cache = jax.ShapeDtypeStruct((w_q.shape[0], batch, slots, head), BF16)
    n_chunks = batch // SEQ_CHUNK
    macs = batch * width * (q_width + 2 * head) + 2 * batch * slots * q_width
    return pl.pallas_call(
        functools.partial(attn_kernel, layer, do_norm, aliased),
        out_shape=(
            pltpu.VMEM((batch, width), BF16),
            out_cache,
            out_cache,
        ) + ((cache_buf,) if aliased else ()),
        in_specs=in_specs,
        out_specs=(vmem, any_spec, any_spec) + ((vmem,) if aliased else ()),
        scratch_shapes=[
            pltpu.VMEM((batch, width), BF16),
            pltpu.VMEM((width, q_width + 2 * head), BF16),
            pltpu.VMEM((q_width, width), BF16),
            pltpu.VMEM((batch, q_width), F32),
            pltpu.VMEM((batch, head), F32),
            pltpu.VMEM((batch, head), F32),
            pltpu.VMEM((batch, head), jnp.int32),
            pltpu.VMEM((batch, q_width), F32),
            pltpu.VMEM((SEQ_CHUNK // 8, 16, slots), F32),
            pltpu.SemaphoreType.DMA,
            pltpu.SemaphoreType.DMA((4,)),
            pltpu.SemaphoreType.DMA((n_chunks,)),
            pltpu.SemaphoreType.DMA((n_chunks,)),
            pltpu.SemaphoreType.DMA((n_chunks,)),
            pltpu.SemaphoreType.DMA((n_chunks,)),
        ] + ([] if aliased else [cache_buf]),
        input_output_aliases=aliases,
        compiler_params=pltpu.CompilerParams(vmem_limit_bytes=ATTN_VMEM + (0 if aliased else 4 * batch * slots * head)),
        cost_estimate=pl.CostEstimate(flops=2 * macs, bytes_accessed=4 * batch * slots * head * 2, transcendentals=batch * slots * 2),
        name=f"attn{layer}",
    )(*args)[:3]


def mix_kernel(layer, last, part_ref, x_hbm, gm_ref, gn_ref, wg_hbm, wu_hbm, wd_hbm, kc_hbm, vc_hbm, *refs):
    if last:
        out_hbm = refs[0]
        refs = refs[1:]
    else:
        out_hbm, xs_ref, kv_next = refs[:3]
        refs = refs[3:]
    (wg, wu, wd, x_own, act, part2, d_recv, r_send, r_recv, gathered,
     w_sem, x_sem, ds_sem, dr_sem, rs_sem, rr_sem, as_sem, ar_sem, fs_sem, fr_sem, o_sem, c_sem) = refs
    width = wg.shape[0]
    parts = (part_ref, part2)
    hidden = wg.shape[1]
    rows = part_ref.shape[0] // ROW_CHUNKS
    core_rows = rows // 2
    blk = core_rows // 4
    me = lax.axis_index("tp")
    core = me % 2
    chip = me // 2
    partner = me + 1 - 2 * core
    peer_y = (chip + 2) % 4
    peer_x = chip + 1 - 2 * (chip % 2)
    peers = [chip, peer_x * (1 - core) + peer_y * core, peer_y * (1 - core) + peer_x * core, 3 - chip]

    def dev(idx):
        return {"tp": idx}

    w_copies = [pltpu.make_async_copy(src.at[layer], dst, w_sem.at[i])
                for i, (src, dst) in enumerate(((wg_hbm, wg), (wu_hbm, wu), (wd_hbm, wd)))]

    def own_rows(j):
        return pl.ds(pl.multiple_of(j * rows + core * core_rows + chip * blk, blk), blk)

    x_copies = []
    for j in range(ROW_CHUNKS):
        if layer:
            x_own[j] = x_hbm[j]
        else:
            x_copies.append(pltpu.make_async_copy(x_hbm.at[own_rows(j)], x_own.at[j], x_sem.at[j]))
            x_copies[-1].start()

    c_copies = []
    if not last:
        size = kv_next.shape[1] // PARTS
        for n in range(PREFETCHED):
            for i, src in enumerate((kc_hbm, vc_hbm)):
                part = pl.ds(n * size, size)
                c_copies.append(pltpu.make_async_copy(src.at[layer + 1, part], kv_next.at[i, part], c_sem.at[i, n]))

    def prefetch(count):
        for _ in range(min(count, len(waiting))):
            waiting.pop(0).start()

    waiting = list(c_copies)
    prefetch(2)
    barrier = pltpu.get_barrier_semaphore()
    others = [partner] + [2 * peers[r] + core for r in range(1, 4)]
    for other in others:
        pl.semaphore_signal(barrier, inc=1, device_id=dev(other), device_id_type=pl.DeviceIdType.MESH)

    def remote(src, dst, send, recv, target):
        return pltpu.make_async_remote_copy(src_ref=src, dst_ref=dst, send_sem=send, recv_sem=recv,
                                            device_id=dev(target), device_id_type=pl.DeviceIdType.MESH)

    def d_copy(s, j):
        here = pl.ds(pl.multiple_of(j * rows + (1 - core) * core_rows, core_rows), core_rows)
        return remote(parts[s].at[here], d_recv.at[s, j], ds_sem.at[s, j], dr_sem.at[s, j], partner)

    def r_copy(s, j, r):
        return remote(r_send.at[s, j, r], r_recv.at[s, j, r], rs_sem.at[s, j, r], rr_sem.at[s, j, r], 2 * peers[r] + core)

    def scatter(s, j):
        d_copy(s, j).wait()
        for r in (3, 1, 2):
            off = pl.multiple_of(peers[r] * blk, blk)
            mine = parts[s][pl.ds(pl.multiple_of(j * rows + core * core_rows + off, blk), blk), :].astype(F32)
            r_send[s, j, r] = (mine + d_recv[s, j, pl.ds(off, blk), :].astype(F32)).astype(BF16)
            r_copy(s, j, r).start()

    def reduce(s, j):
        off = pl.multiple_of(chip * blk, blk)
        total = parts[s][own_rows(j), :].astype(F32) + d_recv[s, j, pl.ds(off, blk), :].astype(F32)
        for r in (1, 2, 3):
            r_copy(s, j, r).wait()
            total += r_recv[s, j, r].astype(F32)
        new = (x_own[j].astype(F32) + total).astype(BF16)
        x_own[j] = new
        return new

    def block_row(j, cc, k):
        return pl.ds(pl.multiple_of(j * rows + cc * core_rows + k * blk, blk), blk)

    def a_copy(s, j, r):
        here = block_row(j, core, chip)
        target = partner if r == 0 else 2 * peers[r] + core
        return remote(gathered.at[s, here], gathered.at[s, here], as_sem.at[s, j, r], ar_sem.at[s, j, r], target)

    def f_copy(s, j, r):
        here = block_row(j, core, peers[r])
        return remote(gathered.at[s, here], gathered.at[s, here], fs_sem.at[s, j, r], fr_sem.at[s, j, r], partner)

    def gather_start(s, j, value):
        gathered[s, block_row(j, core, chip), :] = value
        for r in (3, 1, 2, 0):
            a_copy(s, j, r).start()

    def gather_forward(s, j):
        for r in (1, 2, 3):
            a_copy(s, j, r).wait_recv()
            f_copy(s, j, r).start()

    def gather_finish(s, j):
        a_copy(s, j, 0).wait_recv()
        for r in (1, 2, 3):
            f_copy(s, j, r).wait_recv()

    chunks = range(ROW_CHUNKS)
    per = MLP_CHUNKS
    pl.semaphore_wait(barrier, len(others))
    for j in chunks:
        d_copy(0, j).start()
    for copy in x_copies:
        copy.wait()
    for j in chunks:
        scatter(0, j)
    for copy in w_copies:
        copy.start()
    for j in chunks:
        new = reduce(0, j)
        gather_start(0, j, norm_rows(new.astype(F32), gm_ref[layer:layer + 1, :].astype(F32)))
    prefetch(3)

    def mlp(first):
        here = slice(first * rows, (first + per) * rows)
        step = 256
        lhs = gathered[0, here, :]
        for col in range(0, hidden, step):
            cols = slice(col, col + step)
            gate = jnp.dot(lhs, wg[:, cols], preferred_element_type=F32)
            up = jnp.dot(lhs, wu[:, cols], preferred_element_type=F32)
            act[here, cols] = (gate * jax.nn.sigmoid(gate) * up).astype(BF16)
        lhs = act[here, :]
        for col in range(0, width, 2 * step):
            cols = slice(col, col + 2 * step)
            part2[here, cols] = jnp.dot(lhs, wd[:, cols], preferred_element_type=F32).astype(BF16)
        for j in range(first, first + per):
            d_copy(1, j).start()

    for j in range(per):
        gather_forward(0, j)
    for copy in w_copies:
        copy.wait()
    for first in range(0, ROW_CHUNKS, per):
        for j in range(first, first + per):
            gather_finish(0, j)
        prefetch(3)
        mlp(first)
        for j in range(first + per, min(first + 2 * per, ROW_CHUNKS)):
            gather_forward(0, j)
        for j in range(first, first + per):
            scatter(1, j)

    def second(j):
        new = reduce(1, j)
        if last:
            gather_start(1, j, new)
        else:
            xs_ref[j] = new
            gather_start(1, j, norm_rows(new.astype(F32), gn_ref[layer + 1:layer + 2, :].astype(F32)))

    for j in chunks:
        second(j)
    prefetch(1)
    for j in chunks:
        gather_forward(1, j)
    prefetch(len(waiting))
    outs = []
    for j in chunks:
        gather_finish(1, j)
        here = pl.ds(j * rows, rows)
        if last:
            outs.append(pltpu.make_async_copy(gathered.at[1, here], out_hbm.at[here], o_sem.at[j]))
            outs[-1].start()
        else:
            out_hbm[here, :] = gathered[1, here, :]
    for s in range(2):
        for j in range(ROW_CHUNKS):
            for r in range(4):
                a_copy(s, j, r).wait_send()
            for r in range(1, 4):
                f_copy(s, j, r).wait_send()
    for copy in outs + c_copies:
        copy.wait()


def mix_call(layer, last, part, x_own, g_mlp, g_attn, w_gate, w_up, w_down, k_cache, v_cache):
    batch, width = part.shape
    hidden = w_gate.shape[2]
    rows = batch // ROW_CHUNKS
    blk = rows // 8
    any_spec = pl.BlockSpec(memory_space=pltpu.HBM)
    vmem = pl.BlockSpec(memory_space=pltpu.VMEM)
    if last:
        out_shape = [jax.ShapeDtypeStruct((batch, width), BF16)]
        out_specs = [any_spec]
    else:
        out_shape = [pltpu.VMEM((batch, width), BF16), pltpu.VMEM((ROW_CHUNKS, blk, width), BF16)]
        out_shape.append(pltpu.VMEM((2,) + k_cache.shape[1:], BF16))
        out_specs = [vmem] * 3
    sem = pltpu.SemaphoreType.DMA
    nc = ROW_CHUNKS
    return pl.pallas_call(
        functools.partial(mix_kernel, layer, last),
        out_shape=out_shape,
        in_specs=[vmem, any_spec if layer == 0 else vmem, vmem, vmem] + [any_spec] * 5,
        out_specs=out_specs,
        scratch_shapes=[
            pltpu.VMEM((width, hidden), BF16),
            pltpu.VMEM((width, hidden), BF16),
            pltpu.VMEM((hidden, width), BF16),
            pltpu.VMEM((nc, blk, width), BF16),
            pltpu.VMEM((batch, hidden), BF16),
            pltpu.VMEM((batch, width), BF16),
            pltpu.VMEM((2, nc, rows // 2, width), BF16),
            pltpu.VMEM((2, nc, 4, blk, width), BF16),
            pltpu.VMEM((2, nc, 4, blk, width), BF16),
            pltpu.VMEM((2, batch, width), BF16),
            sem((3,)), sem((nc,)),
            sem((2, nc)), sem((2, nc)),
            sem((2, nc, 4)), sem((2, nc, 4)),
            sem((2, nc, 4)), sem((2, nc, 4)),
            sem((2, nc, 4)), sem((2, nc, 4)),
            sem((nc,)), sem((2, PREFETCHED)),
        ],
        compiler_params=pltpu.CompilerParams(collective_id=layer, has_side_effects=True, vmem_limit_bytes=MIX_VMEM),
        cost_estimate=pl.CostEstimate(flops=6 * batch * width * hidden, bytes_accessed=6 * width * hidden, transcendentals=batch * hidden),
        name=f"mix{layer}",
    )(*in_vmem(part), *(in_hbm if layer == 0 else in_vmem)(x_own), g_mlp, g_attn, *in_hbm(w_gate, w_up, w_down, k_cache, v_cache))


def solution(mesh):
    weight_col = P(None, None, "tp")
    weight_row = P(None, "tp", None)
    bias_col = P(None, "tp")
    cache_spec = P(None, "dp", None, "tp", None)
    in_specs = (P("dp", None), P("dp"), P(None, None), P(None, None), weight_col, bias_col, weight_col, bias_col, weight_col, bias_col, weight_row, weight_col, weight_col, weight_row, cache_spec, cache_spec)
    out_specs = (P("dp", None), cache_spec, cache_spec)

    def local_step(x_in, seq_lens, g_attn, g_mlp, w_q, b_q, w_k, b_k, w_v, b_v, w_o, w_gate, w_up, w_down, k_cache, v_cache):
        layers, batch, slots, _, head = k_cache.shape
        inv_freq = ROPE_THETA ** (-2.0 * np.arange(head // 2) / head)
        freq = jnp.asarray(np.concatenate([inv_freq, inv_freq])[None, :].astype(np.float32))
        k_flat = k_cache.reshape(layers, batch, slots, head)
        v_flat = v_cache.reshape(layers, batch, slots, head)
        normed, x_own, prev = x_in, x_in, None
        for layer in range(layers):
            last = layer == layers - 1
            part, k_out, v_out = attn_call(layer, layer == 0, seq_lens, freq, normed, g_attn, b_q, b_k, b_v, w_q, w_k, w_v, w_o, k_flat, v_flat, prev)
            outs = mix_call(layer, last, part, x_own, g_mlp, g_attn, w_gate, w_up, w_down, k_flat, v_flat)
            if last:
                x_out = outs[0]
            else:
                normed, x_own, prev = outs[0], outs[1], (outs[2], k_out, v_out)
        return x_out, k_out.reshape(k_cache.shape), v_out.reshape(v_cache.shape)

    return jax.shard_map(local_step, mesh=mesh, in_specs=in_specs, out_specs=out_specs, check_vma=False)
```

```python
import functools
import math

import jax
import jax.numpy as jnp
import numpy as np
from jax import lax
from jax.experimental import pallas as pl
from jax.experimental.pallas import tpu as pltpu
from jax.sharding import PartitionSpec as P

ROPE_THETA = 1000000.0
EPS = 1e-6
F32 = jnp.float32
BF16 = jnp.bfloat16
NT = (((1,), (1,)), ((), ()))
SEQ_CHUNK = 16
ROW_CHUNKS = 4
MLP_CHUNKS = 2
PARTS = 8
PREFETCHED = 6
ATTN_VMEM = 24 * 1024 * 1024
MIX_VMEM = 22 * 1024 * 1024


def norm_rows(vec_f32, gain_row):
    mean_sq = jnp.mean(vec_f32 * vec_f32, axis=-1, keepdims=True)
    return (vec_f32 * lax.rsqrt(mean_sq + EPS) * gain_row).astype(BF16)


def attn_kernel(layer, do_norm, aliased, *refs):
    (lens_smem, lens_row, freq, x_hbm, g_ref, bq_ref, bk_ref, bv_ref, wq_hbm, wk_hbm, wv_hbm, wo_hbm, kc_hbm, vc_hbm) = refs[:14]
    refs = refs[17 if aliased else 14:]
    part_ref, ko_hbm, vo_hbm = refs[:3]
    refs = refs[3:]
    kv_buf = refs[0] if aliased else refs[-1]
    k_buf, v_buf = kv_buf.at[0], kv_buf.at[1]
    refs = refs[1:] if aliased else refs[:-1]
    (x_buf, w_buf, wo, q_f32, k_f32, v_f32, lens_col, out_f32, s_buf, x_sem, w_sem, k_sem, v_sem, ko_sem, vo_sem) = refs
    batch, slots, head = k_buf.shape
    q_width = wq_hbm.shape[2]
    n_chunks = batch // SEQ_CHUNK

    if do_norm:
        x_copy = pltpu.make_async_copy(x_hbm, x_buf, x_sem)
        x_copy.start()
    w_copies = [
        pltpu.make_async_copy(wq_hbm.at[layer], w_buf.at[:, :q_width], w_sem.at[0]),
        pltpu.make_async_copy(wk_hbm.at[layer], w_buf.at[:, q_width:q_width + head], w_sem.at[1]),
        pltpu.make_async_copy(wv_hbm.at[layer], w_buf.at[:, q_width + head:], w_sem.at[2]),
    ]
    for copy in w_copies:
        copy.start()
    first_read = n_chunks * PREFETCHED // PARTS if aliased else 0
    wo_copy = pltpu.make_async_copy(wo_hbm.at[layer], wo, w_sem.at[3])

    def chunk_copies(idx):
        rows = pl.ds(pl.multiple_of(idx * SEQ_CHUNK, SEQ_CHUNK), SEQ_CHUNK)
        return (
            pltpu.make_async_copy(kc_hbm.at[layer, rows], k_buf.at[rows], k_sem.at[idx]),
            pltpu.make_async_copy(vc_hbm.at[layer, rows], v_buf.at[rows], v_sem.at[idx]),
            pltpu.make_async_copy(k_buf.at[rows], ko_hbm.at[layer, rows], ko_sem.at[idx]),
            pltpu.make_async_copy(v_buf.at[rows], vo_hbm.at[layer, rows], vo_sem.at[idx]),
        )

    @pl.loop(first_read, n_chunks)
    def _(idx):
        k_in, v_in, _, _ = chunk_copies(idx)
        k_in.start()
        v_in.start()

    wo_copy.start()

    lens_f = lens_row[...].astype(F32)
    same = lax.broadcasted_iota(jnp.int32, (batch, batch), 0) == lax.broadcasted_iota(jnp.int32, (batch, batch), 1)
    pos_col = jnp.sum(jnp.where(same, jnp.broadcast_to(lens_f, (batch, batch)), 0.0), axis=1, keepdims=True)
    lens_col[...] = jnp.broadcast_to(pos_col, (batch, head)).astype(jnp.int32)
    angles = pos_col * freq[...]
    cos_tab = jnp.cos(angles)
    lane = lax.broadcasted_iota(jnp.int32, (1, head), 1)
    sin_tab = jnp.sin(angles) * jnp.where(lane < head // 2, -1.0, 1.0)

    def rope(vec):
        return vec * cos_tab + pltpu.roll(vec, head // 2, 1) * sin_tab

    for copy in w_copies:
        copy.wait()
    if do_norm:
        x_copy.wait()
        normed = norm_rows(x_buf[...].astype(F32), g_ref[layer:layer + 1, :].astype(F32))
    else:
        normed = x_hbm[...]
    part = jnp.dot(normed, w_buf[:, :q_width], preferred_element_type=F32) + bq_ref[layer:layer + 1, :].astype(F32)
    for col in range(q_width // head):
        cols = slice(col * head, (col + 1) * head)
        q_f32[:, cols] = rope(part[:, cols]).astype(BF16).astype(F32)
    part = jnp.dot(normed, w_buf[:, q_width:], preferred_element_type=F32)
    k_f32[...] = rope(part[:, :head] + bk_ref[layer:layer + 1, :].astype(F32)).astype(BF16).astype(F32)
    v_f32[...] = (part[:, head:] + bv_ref[layer:layer + 1, :].astype(F32)).astype(BF16).astype(F32)

    half = 8
    scale = head ** -0.5
    row_in_group = lax.broadcasted_iota(jnp.int32, (2 * half, head), 0) % half
    slot_id = lax.broadcasted_iota(jnp.int32, (2 * half, slots), 1)
    tile_row = lax.broadcasted_iota(jnp.int32, (16, head), 0)

    def patch(idx):
        for sub in range(SEQ_CHUNK):
            seq = idx * SEQ_CHUNK + sub
            pos = lens_smem[seq]
            base = pl.multiple_of((pos >> 4) << 4, 16)
            hit = tile_row == pos - base
            for buf, new in ((k_buf, k_f32), (v_buf, v_f32)):
                row = jnp.broadcast_to(new[pl.ds(seq, 1), :], (16, head))
                old = buf[seq, pl.ds(base, 16), :]
                buf[seq, pl.ds(base, 16), :] = jnp.where(hit, row, old.astype(F32)).astype(BF16)

    groups = SEQ_CHUNK // half

    def first_row(idx, group):
        return pl.multiple_of(idx * SEQ_CHUNK + group * half, half)

    def scores_of(idx, group):
        first = first_row(idx, group)
        q_rows = q_f32[pl.ds(first, half), :]
        q_all = jnp.concatenate([q_rows[:, :head], q_rows[:, head:]], axis=0)
        scores = jnp.zeros((2 * half, slots), F32)
        for pair in range(half // 2):
            lhs = jnp.concatenate([jnp.where(row_in_group == 2 * pair + e, q_all, 0.0) for e in range(2)], axis=1).astype(BF16)
            rhs = jnp.concatenate([k_buf[first + 2 * pair + e] for e in range(2)], axis=1)
            scores += lax.dot_general(lhs, rhs, NT, preferred_element_type=F32)
        return scores

    def probs_of(idx, group):
        pos_rows = lens_col[pl.ds(first_row(idx, group), half), 0:1]
        pos_all = jnp.concatenate([pos_rows, pos_rows], axis=0)
        scores = jnp.where(slot_id <= pos_all, s_buf[group] * scale, -1e30)
        expo = jnp.exp(scores - jnp.max(scores, axis=-1, keepdims=True))
        return (expo / jnp.sum(expo, axis=-1, keepdims=True)).astype(BF16)

    def values_of(idx, group, probs):
        first = first_row(idx, group)
        out = jnp.zeros((2 * half, head), F32)
        for pair in range(half // 2):
            rhs = jnp.concatenate([v_buf[first + 2 * pair + e] for e in range(2)], axis=1)
            both = jnp.dot(probs, rhs, preferred_element_type=F32)
            for e in range(2):
                out = jnp.where(row_in_group == 2 * pair + e, both[:, e * head:(e + 1) * head], out)
        return jnp.concatenate([out[:half], out[half:]], axis=1)

    s_buf[...] = jnp.zeros_like(s_buf)

    @pl.loop(0, n_chunks + 1)
    def _(idx):
        @pl.when(idx < n_chunks)
        def _():
            k_in, v_in, k_out, v_out = chunk_copies(idx)
            @pl.when(idx >= first_read)
            def _():
                k_in.wait()
                v_in.wait()

            patch(idx)
            k_out.start()
            v_out.start()

        now = jnp.maximum(idx - 1, 0)
        later = jnp.minimum(idx, n_chunks - 1)
        new_scores = [scores_of(later, group) for group in range(groups)]
        probs = [probs_of(now, group) for group in range(groups)]
        outs = [values_of(now, group, probs[group]) for group in range(groups)]
        for group in range(groups):
            s_buf[group] = new_scores[group]
            out_f32[pl.ds(first_row(now, group), half), :] = outs[group]

    wo_copy.wait()
    attn = out_f32[...].astype(BF16)
    block = 512
    for col in range(0, wo.shape[1], block):
        part_ref[:, col:col + block] = jnp.dot(attn, wo[:, col:col + block], preferred_element_type=F32).astype(BF16)

    @pl.loop(0, n_chunks)
    def _(idx):
        _, _, k_out, v_out = chunk_copies(idx)
        k_out.wait()
        v_out.wait()


def in_hbm(*arrays):
    return [pltpu.with_memory_space_constraint(a, pltpu.HBM) for a in arrays]


def in_vmem(*arrays):
    return [pltpu.with_memory_space_constraint(a, pltpu.VMEM) for a in arrays]


def attn_call(layer, do_norm, lens, freq, x_in, gain, b_q, b_k, b_v, w_q, w_k, w_v, w_o, k_cache, v_cache, prev):
    batch, slots, head = k_cache.shape[-3:]
    width = x_in.shape[1]
    q_width = w_q.shape[2]
    any_spec = pl.BlockSpec(memory_space=pltpu.HBM)
    vmem = pl.BlockSpec(memory_space=pltpu.VMEM)
    aliased = prev is not None
    place = in_hbm if do_norm else in_vmem
    args = [lens, lens.reshape(1, batch), freq, *place(x_in), gain, b_q, b_k, b_v, *in_hbm(w_q, w_k, w_v, w_o, k_cache, v_cache)]
    in_specs = [pl.BlockSpec(memory_space=pltpu.SMEM), vmem, vmem, any_spec if do_norm else vmem, vmem, vmem, vmem, vmem] + [any_spec] * 6
    aliases = {}
    if aliased:
        aliases = {len(args): 3, len(args) + 1: 1, len(args) + 2: 2}
        args += [*in_vmem(prev[0]), *in_hbm(*prev[1:])]
        in_specs += [vmem] + [any_spec] * 2
    cache_buf = pltpu.VMEM((2, batch, slots, head), BF16)
    out_cache = jax.ShapeDtypeStruct((w_q.shape[0], batch, slots, head), BF16)
    n_chunks = batch // SEQ_CHUNK
    macs = batch * width * (q_width + 2 * head) + 2 * batch * slots * q_width
    return pl.pallas_call(
        functools.partial(attn_kernel, layer, do_norm, aliased),
        out_shape=(
            pltpu.VMEM((batch, width), BF16),
            out_cache,
            out_cache,
        ) + ((cache_buf,) if aliased else ()),
        in_specs=in_specs,
        out_specs=(vmem, any_spec, any_spec) + ((vmem,) if aliased else ()),
        scratch_shapes=[
            pltpu.VMEM((batch, width), BF16),
            pltpu.VMEM((width, q_width + 2 * head), BF16),
            pltpu.VMEM((q_width, width), BF16),
            pltpu.VMEM((batch, q_width), F32),
            pltpu.VMEM((batch, head), F32),
            pltpu.VMEM((batch, head), F32),
            pltpu.VMEM((batch, head), jnp.int32),
            pltpu.VMEM((batch, q_width), F32),
            pltpu.VMEM((SEQ_CHUNK // 8, 16, slots), F32),
            pltpu.SemaphoreType.DMA,
            pltpu.SemaphoreType.DMA((4,)),
            pltpu.SemaphoreType.DMA((n_chunks,)),
            pltpu.SemaphoreType.DMA((n_chunks,)),
            pltpu.SemaphoreType.DMA((n_chunks,)),
            pltpu.SemaphoreType.DMA((n_chunks,)),
        ] + ([] if aliased else [cache_buf]),
        input_output_aliases=aliases,
        compiler_params=pltpu.CompilerParams(vmem_limit_bytes=ATTN_VMEM + (0 if aliased else 4 * batch * slots * head)),
        cost_estimate=pl.CostEstimate(flops=2 * macs, bytes_accessed=4 * batch * slots * head * 2, transcendentals=batch * slots * 2),
        name=f"attn{layer}",
    )(*args)[:3]


def mix_kernel(layer, last, part_ref, x_hbm, gm_ref, gn_ref, wg_hbm, wu_hbm, wd_hbm, kc_hbm, vc_hbm, *refs):
    if last:
        out_hbm = refs[0]
        refs = refs[1:]
    else:
        out_hbm, xs_ref, kv_next = refs[:3]
        refs = refs[3:]
    (wg, wu, wd, x_own, act, part2, d_recv, r_send, r_recv, gathered,
     w_sem, x_sem, ds_sem, dr_sem, rs_sem, rr_sem, as_sem, ar_sem, fs_sem, fr_sem, o_sem, c_sem) = refs
    width = wg.shape[0]
    parts = (part_ref, part2)
    hidden = wg.shape[1]
    rows = part_ref.shape[0] // ROW_CHUNKS
    core_rows = rows // 2
    blk = core_rows // 4
    me = lax.axis_index("tp")
    core = me % 2
    chip = me // 2
    partner = me + 1 - 2 * core
    peer_y = (chip + 2) % 4
    peer_x = chip + 1 - 2 * (chip % 2)
    peers = [chip, peer_x * (1 - core) + peer_y * core, peer_y * (1 - core) + peer_x * core, 3 - chip]

    def dev(idx):
        return {"tp": idx}

    w_copies = [pltpu.make_async_copy(src.at[layer], dst, w_sem.at[i])
                for i, (src, dst) in enumerate(((wg_hbm, wg), (wu_hbm, wu), (wd_hbm, wd)))]

    def own_rows(j):
        return pl.ds(pl.multiple_of(j * rows + core * core_rows + chip * blk, blk), blk)

    x_copies = []
    for j in range(ROW_CHUNKS):
        if layer:
            x_own[j] = x_hbm[j]
        else:
            x_copies.append(pltpu.make_async_copy(x_hbm.at[own_rows(j)], x_own.at[j], x_sem.at[j]))
            x_copies[-1].start()

    c_copies = []
    if not last:
        size = kv_next.shape[1] // PARTS
        for n in range(PREFETCHED):
            for i, src in enumerate((kc_hbm, vc_hbm)):
                part = pl.ds(n * size, size)
                c_copies.append(pltpu.make_async_copy(src.at[layer + 1, part], kv_next.at[i, part], c_sem.at[i, n]))

    def prefetch(count):
        for _ in range(min(count, len(waiting))):
            waiting.pop(0).start()

    waiting = list(c_copies)
    prefetch(3)
    barrier = pltpu.get_barrier_semaphore()
    others = [partner] + [2 * peers[r] + core for r in range(1, 4)]
    for other in others:
        pl.semaphore_signal(barrier, inc=1, device_id=dev(other), device_id_type=pl.DeviceIdType.MESH)

    def remote(src, dst, send, recv, target):
        return pltpu.make_async_remote_copy(src_ref=src, dst_ref=dst, send_sem=send, recv_sem=recv,
                                            device_id=dev(target), device_id_type=pl.DeviceIdType.MESH)

    def d_copy(s, j):
        here = pl.ds(pl.multiple_of(j * rows + (1 - core) * core_rows, core_rows), core_rows)
        return remote(parts[s].at[here], d_recv.at[s, j], ds_sem.at[s, j], dr_sem.at[s, j], partner)

    def r_copy(s, j, r):
        return remote(r_send.at[s, j, r], r_recv.at[s, j, r], rs_sem.at[s, j, r], rr_sem.at[s, j, r], 2 * peers[r] + core)

    def scatter(s, j):
        d_copy(s, j).wait()
        for r in (3, 1, 2):
            off = pl.multiple_of(peers[r] * blk, blk)
            mine = parts[s][pl.ds(pl.multiple_of(j * rows + core * core_rows + off, blk), blk), :].astype(F32)
            r_send[s, j, r] = (mine + d_recv[s, j, pl.ds(off, blk), :].astype(F32)).astype(BF16)
            r_copy(s, j, r).start()

    def reduce(s, j):
        off = pl.multiple_of(chip * blk, blk)
        total = parts[s][own_rows(j), :].astype(F32) + d_recv[s, j, pl.ds(off, blk), :].astype(F32)
        for r in (1, 2, 3):
            r_copy(s, j, r).wait()
            total += r_recv[s, j, r].astype(F32)
        new = (x_own[j].astype(F32) + total).astype(BF16)
        x_own[j] = new
        return new

    def block_row(j, cc, k):
        return pl.ds(pl.multiple_of(j * rows + cc * core_rows + k * blk, blk), blk)

    def a_copy(s, j, r):
        here = block_row(j, core, chip)
        target = partner if r == 0 else 2 * peers[r] + core
        return remote(gathered.at[s, here], gathered.at[s, here], as_sem.at[s, j, r], ar_sem.at[s, j, r], target)

    def f_copy(s, j, r):
        here = block_row(j, core, peers[r])
        return remote(gathered.at[s, here], gathered.at[s, here], fs_sem.at[s, j, r], fr_sem.at[s, j, r], partner)

    def gather_start(s, j, value):
        gathered[s, block_row(j, core, chip), :] = value
        for r in (3, 1, 2, 0):
            a_copy(s, j, r).start()

    def gather_forward(s, j):
        for r in (1, 2, 3):
            a_copy(s, j, r).wait_recv()
            f_copy(s, j, r).start()

    def gather_finish(s, j):
        a_copy(s, j, 0).wait_recv()
        for r in (1, 2, 3):
            f_copy(s, j, r).wait_recv()

    chunks = range(ROW_CHUNKS)
    per = MLP_CHUNKS
    pl.semaphore_wait(barrier, len(others))
    for j in chunks:
        d_copy(0, j).start()
    for copy in x_copies:
        copy.wait()
    for j in chunks:
        scatter(0, j)
    for copy in w_copies:
        copy.start()
    for j in chunks:
        new = reduce(0, j)
        gather_start(0, j, norm_rows(new.astype(F32), gm_ref[layer:layer + 1, :].astype(F32)))
    prefetch(3)

    def mlp_up(first):
        here = slice(first * rows, (first + per) * rows)
        step = 256
        lhs = gathered[0, here, :]
        for col in range(0, hidden, step):
            cols = slice(col, col + step)
            gate = jnp.dot(lhs, wg[:, cols], preferred_element_type=F32)
            up = jnp.dot(lhs, wu[:, cols], preferred_element_type=F32)
            act[here, cols] = (gate * jax.nn.sigmoid(gate) * up).astype(BF16)

    def mlp_down(first):
        here = slice(first * rows, (first + per) * rows)
        step = 512
        lhs = act[here, :]
        for col in range(0, width, step):
            cols = slice(col, col + step)
            part2[here, cols] = jnp.dot(lhs, wd[:, cols], preferred_element_type=F32).astype(BF16)
        for j in range(first, first + per):
            d_copy(1, j).start()

    def group(first):
        return range(max(first, 0), min(first + per, ROW_CHUNKS))

    for j in group(0):
        gather_forward(0, j)
    for copy in w_copies:
        copy.wait()
    for first in range(0, ROW_CHUNKS, per):
        for j in group(first):
            gather_finish(0, j)
        prefetch(2)
        mlp_up(first)
        if first + per < ROW_CHUNKS:
            for j in group(first + per):
                gather_forward(0, j)
        if first:
            for j in group(first - per):
                scatter(1, j)
        mlp_down(first)
    for j in group(ROW_CHUNKS - per):
        scatter(1, j)

    def second(j):
        new = reduce(1, j)
        if last:
            gather_start(1, j, new)
        else:
            xs_ref[j] = new
            gather_start(1, j, norm_rows(new.astype(F32), gn_ref[layer + 1:layer + 2, :].astype(F32)))

    for j in chunks:
        second(j)
    prefetch(2)
    for j in chunks:
        gather_forward(1, j)
    prefetch(len(waiting))
    outs = []
    for j in chunks:
        gather_finish(1, j)
        here = pl.ds(j * rows, rows)
        if last:
            outs.append(pltpu.make_async_copy(gathered.at[1, here], out_hbm.at[here], o_sem.at[j]))
            outs[-1].start()
        else:
            out_hbm[here, :] = gathered[1, here, :]
    for s in range(2):
        for j in range(ROW_CHUNKS):
            for r in range(4):
                a_copy(s, j, r).wait_send()
            for r in range(1, 4):
                f_copy(s, j, r).wait_send()
    for copy in outs + c_copies:
        copy.wait()


def mix_call(layer, last, part, x_own, g_mlp, g_attn, w_gate, w_up, w_down, k_cache, v_cache):
    batch, width = part.shape
    hidden = w_gate.shape[2]
    rows = batch // ROW_CHUNKS
    blk = rows // 8
    any_spec = pl.BlockSpec(memory_space=pltpu.HBM)
    vmem = pl.BlockSpec(memory_space=pltpu.VMEM)
    if last:
        out_shape = [jax.ShapeDtypeStruct((batch, width), BF16)]
        out_specs = [any_spec]
    else:
        out_shape = [pltpu.VMEM((batch, width), BF16), pltpu.VMEM((ROW_CHUNKS, blk, width), BF16)]
        out_shape.append(pltpu.VMEM((2,) + k_cache.shape[1:], BF16))
        out_specs = [vmem] * 3
    sem = pltpu.SemaphoreType.DMA
    nc = ROW_CHUNKS
    return pl.pallas_call(
        functools.partial(mix_kernel, layer, last),
        out_shape=out_shape,
        in_specs=[vmem, any_spec if layer == 0 else vmem, vmem, vmem] + [any_spec] * 5,
        out_specs=out_specs,
        scratch_shapes=[
            pltpu.VMEM((width, hidden), BF16),
            pltpu.VMEM((width, hidden), BF16),
            pltpu.VMEM((hidden, width), BF16),
            pltpu.VMEM((nc, blk, width), BF16),
            pltpu.VMEM((batch, hidden), BF16),
            pltpu.VMEM((batch, width), BF16),
            pltpu.VMEM((2, nc, rows // 2, width), BF16),
            pltpu.VMEM((2, nc, 4, blk, width), BF16),
            pltpu.VMEM((2, nc, 4, blk, width), BF16),
            pltpu.VMEM((2, batch, width), BF16),
            sem((3,)), sem((nc,)),
            sem((2, nc)), sem((2, nc)),
            sem((2, nc, 4)), sem((2, nc, 4)),
            sem((2, nc, 4)), sem((2, nc, 4)),
            sem((2, nc, 4)), sem((2, nc, 4)),
            sem((nc,)), sem((2, PREFETCHED)),
        ],
        compiler_params=pltpu.CompilerParams(collective_id=layer, has_side_effects=True, vmem_limit_bytes=MIX_VMEM),
        cost_estimate=pl.CostEstimate(flops=6 * batch * width * hidden, bytes_accessed=6 * width * hidden, transcendentals=batch * hidden),
        name=f"mix{layer}",
    )(*in_vmem(part), *(in_hbm if layer == 0 else in_vmem)(x_own), g_mlp, g_attn, *in_hbm(w_gate, w_up, w_down, k_cache, v_cache))


def solution(mesh):
    weight_col = P(None, None, "tp")
    weight_row = P(None, "tp", None)
    bias_col = P(None, "tp")
    cache_spec = P(None, "dp", None, "tp", None)
    in_specs = (P("dp", None), P("dp"), P(None, None), P(None, None), weight_col, bias_col, weight_col, bias_col, weight_col, bias_col, weight_row, weight_col, weight_col, weight_row, cache_spec, cache_spec)
    out_specs = (P("dp", None), cache_spec, cache_spec)

    def local_step(x_in, seq_lens, g_attn, g_mlp, w_q, b_q, w_k, b_k, w_v, b_v, w_o, w_gate, w_up, w_down, k_cache, v_cache):
        layers, batch, slots, _, head = k_cache.shape
        inv_freq = ROPE_THETA ** (-2.0 * np.arange(head // 2) / head)
        freq = jnp.asarray(np.concatenate([inv_freq, inv_freq])[None, :].astype(np.float32))
        k_flat = k_cache.reshape(layers, batch, slots, head)
        v_flat = v_cache.reshape(layers, batch, slots, head)
        normed, x_own, prev = x_in, x_in, None
        for layer in range(layers):
            last = layer == layers - 1
            part, k_out, v_out = attn_call(layer, layer == 0, seq_lens, freq, normed, g_attn, b_q, b_k, b_v, w_q, w_k, w_v, w_o, k_flat, v_flat, prev)
            outs = mix_call(layer, last, part, x_own, g_mlp, g_attn, w_gate, w_up, w_down, k_flat, v_flat)
            if last:
                x_out = outs[0]
            else:
                normed, x_own, prev = outs[0], outs[1], (outs[2], k_out, v_out)
        return x_out, k_out.reshape(k_cache.shape), v_out.reshape(v_cache.shape)

    return jax.shard_map(local_step, mesh=mesh, in_specs=in_specs, out_specs=out_specs, check_vma=False)
```

```python
import functools
import math

import jax
import jax.numpy as jnp
import numpy as np
from jax import lax
from jax.experimental import pallas as pl
from jax.experimental.pallas import tpu as pltpu
from jax.sharding import PartitionSpec as P

ROPE_THETA = 1000000.0
EPS = 1e-6
F32 = jnp.float32
BF16 = jnp.bfloat16
NT = (((1,), (1,)), ((), ()))
SEQ_CHUNK = 16
ROW_CHUNKS = 4
MLP_CHUNKS = 2
PARTS = 8
PREFETCHED = 7
ATTN_VMEM = 24 * 1024 * 1024
MIX_VMEM = 22 * 1024 * 1024


def norm_rows(vec_f32, gain_row):
    mean_sq = jnp.mean(vec_f32 * vec_f32, axis=-1, keepdims=True)
    return (vec_f32 * lax.rsqrt(mean_sq + EPS) * gain_row).astype(BF16)


def attn_kernel(layer, do_norm, aliased, *refs):
    (lens_smem, lens_row, freq, x_hbm, g_ref, bq_ref, bk_ref, bv_ref, wq_hbm, wk_hbm, wv_hbm, wo_hbm, kc_hbm, vc_hbm) = refs[:14]
    refs = refs[17 if aliased else 14:]
    part_ref, ko_hbm, vo_hbm = refs[:3]
    refs = refs[3:]
    kv_buf = refs[0] if aliased else refs[-1]
    k_buf, v_buf = kv_buf.at[0], kv_buf.at[1]
    refs = refs[1:] if aliased else refs[:-1]
    (x_buf, w_buf, wo, q_f32, k_f32, v_f32, lens_col, out_f32, s_buf, x_sem, w_sem, k_sem, v_sem, ko_sem, vo_sem) = refs
    batch, slots, head = k_buf.shape
    q_width = wq_hbm.shape[2]
    n_chunks = batch // SEQ_CHUNK

    if do_norm:
        x_copy = pltpu.make_async_copy(x_hbm, x_buf, x_sem)
        x_copy.start()
    w_copies = [
        pltpu.make_async_copy(wq_hbm.at[layer], w_buf.at[:, :q_width], w_sem.at[0]),
        pltpu.make_async_copy(wk_hbm.at[layer], w_buf.at[:, q_width:q_width + head], w_sem.at[1]),
        pltpu.make_async_copy(wv_hbm.at[layer], w_buf.at[:, q_width + head:], w_sem.at[2]),
    ]
    for copy in w_copies:
        copy.start()
    first_read = n_chunks * PREFETCHED // PARTS if aliased else 0
    wo_copy = pltpu.make_async_copy(wo_hbm.at[layer], wo, w_sem.at[3])

    def chunk_copies(idx):
        rows = pl.ds(pl.multiple_of(idx * SEQ_CHUNK, SEQ_CHUNK), SEQ_CHUNK)
        return (
            pltpu.make_async_copy(kc_hbm.at[layer, rows], k_buf.at[rows], k_sem.at[idx]),
            pltpu.make_async_copy(vc_hbm.at[layer, rows], v_buf.at[rows], v_sem.at[idx]),
            pltpu.make_async_copy(k_buf.at[rows], ko_hbm.at[layer, rows], ko_sem.at[idx]),
            pltpu.make_async_copy(v_buf.at[rows], vo_hbm.at[layer, rows], vo_sem.at[idx]),
        )

    @pl.loop(first_read, n_chunks)
    def _(idx):
        k_in, v_in, _, _ = chunk_copies(idx)
        k_in.start()
        v_in.start()

    wo_copy.start()

    lens_f = lens_row[...].astype(F32)
    same = lax.broadcasted_iota(jnp.int32, (batch, batch), 0) == lax.broadcasted_iota(jnp.int32, (batch, batch), 1)
    pos_col = jnp.sum(jnp.where(same, jnp.broadcast_to(lens_f, (batch, batch)), 0.0), axis=1, keepdims=True)
    lens_col[...] = jnp.broadcast_to(pos_col, (batch, head)).astype(jnp.int32)
    angles = pos_col * freq[...]
    cos_tab = jnp.cos(angles)
    lane = lax.broadcasted_iota(jnp.int32, (1, head), 1)
    sin_tab = jnp.sin(angles) * jnp.where(lane < head // 2, -1.0, 1.0)

    def rope(vec):
        return vec * cos_tab + pltpu.roll(vec, head // 2, 1) * sin_tab

    for copy in w_copies:
        copy.wait()
    if do_norm:
        x_copy.wait()
        normed = norm_rows(x_buf[...].astype(F32), g_ref[layer:layer + 1, :].astype(F32))
    else:
        normed = x_hbm[...]
    part = jnp.dot(normed, w_buf[:, :q_width], preferred_element_type=F32) + bq_ref[layer:layer + 1, :].astype(F32)
    for col in range(q_width // head):
        cols = slice(col * head, (col + 1) * head)
        q_f32[:, cols] = rope(part[:, cols]).astype(BF16).astype(F32)
    part = jnp.dot(normed, w_buf[:, q_width:], preferred_element_type=F32)
    k_f32[...] = rope(part[:, :head] + bk_ref[layer:layer + 1, :].astype(F32)).astype(BF16).astype(F32)
    v_f32[...] = (part[:, head:] + bv_ref[layer:layer + 1, :].astype(F32)).astype(BF16).astype(F32)

    half = 8
    scale = head ** -0.5
    row_in_group = lax.broadcasted_iota(jnp.int32, (2 * half, head), 0) % half
    slot_id = lax.broadcasted_iota(jnp.int32, (2 * half, slots), 1)
    tile_row = lax.broadcasted_iota(jnp.int32, (16, head), 0)

    def patch(idx):
        for sub in range(SEQ_CHUNK):
            seq = idx * SEQ_CHUNK + sub
            pos = lens_smem[seq]
            base = pl.multiple_of((pos >> 4) << 4, 16)
            hit = tile_row == pos - base
            for buf, new in ((k_buf, k_f32), (v_buf, v_f32)):
                row = jnp.broadcast_to(new[pl.ds(seq, 1), :], (16, head))
                old = buf[seq, pl.ds(base, 16), :]
                buf[seq, pl.ds(base, 16), :] = jnp.where(hit, row, old.astype(F32)).astype(BF16)

    groups = SEQ_CHUNK // half

    def first_row(idx, group):
        return pl.multiple_of(idx * SEQ_CHUNK + group * half, half)

    def scores_of(idx, group):
        first = first_row(idx, group)
        q_rows = q_f32[pl.ds(first, half), :]
        q_all = jnp.concatenate([q_rows[:, :head], q_rows[:, head:]], axis=0)
        scores = jnp.zeros((2 * half, slots), F32)
        for pair in range(half // 2):
            lhs = jnp.concatenate([jnp.where(row_in_group == 2 * pair + e, q_all, 0.0) for e in range(2)], axis=1).astype(BF16)
            rhs = jnp.concatenate([k_buf[first + 2 * pair + e] for e in range(2)], axis=1)
            scores += lax.dot_general(lhs, rhs, NT, preferred_element_type=F32)
        return scores

    def probs_of(idx, group):
        pos_rows = lens_col[pl.ds(first_row(idx, group), half), 0:1]
        pos_all = jnp.concatenate([pos_rows, pos_rows], axis=0)
        scores = jnp.where(slot_id <= pos_all, s_buf[group] * scale, -1e30)
        expo = jnp.exp(scores - jnp.max(scores, axis=-1, keepdims=True))
        return (expo / jnp.sum(expo, axis=-1, keepdims=True)).astype(BF16)

    def values_of(idx, group, probs):
        first = first_row(idx, group)
        out = jnp.zeros((2 * half, head), F32)
        for pair in range(half // 2):
            rhs = jnp.concatenate([v_buf[first + 2 * pair + e] for e in range(2)], axis=1)
            both = jnp.dot(probs, rhs, preferred_element_type=F32)
            for e in range(2):
                out = jnp.where(row_in_group == 2 * pair + e, both[:, e * head:(e + 1) * head], out)
        return jnp.concatenate([out[:half], out[half:]], axis=1)

    def values_step(idx, probs):
        for group in range(groups):
            out_f32[pl.ds(first_row(idx, group), half), :] = values_of(idx, group, probs[group])

    def step(idx, now):
        new_scores = [scores_of(idx, group) for group in range(groups)]
        values_step(now, [probs_of(now, group) for group in range(groups)])
        for group in range(groups):
            s_buf[group] = new_scores[group]

    def arrive(idx):
        k_in, v_in, _, _ = chunk_copies(idx)
        k_in.wait()
        v_in.wait()

    def leave(idx):
        _, _, k_out, v_out = chunk_copies(idx)
        k_out.start()
        v_out.start()

    s_buf[...] = jnp.zeros_like(s_buf)
    if not aliased:
        arrive(0)
    patch(0)
    leave(0)

    @pl.loop(0, n_chunks - 1)
    def _(idx):
        if aliased:
            pl.when(idx + 1 >= first_read)(lambda: arrive(idx + 1))
        else:
            arrive(idx + 1)
        step(idx, jnp.maximum(idx - 1, 0))
        patch(idx + 1)
        leave(idx + 1)

    step(n_chunks - 1, n_chunks - 2)
    values_step(n_chunks - 1, [probs_of(n_chunks - 1, group) for group in range(groups)])

    wo_copy.wait()
    attn = out_f32[...].astype(BF16)
    block = 512
    for col in range(0, wo.shape[1], block):
        part_ref[:, col:col + block] = jnp.dot(attn, wo[:, col:col + block], preferred_element_type=F32).astype(BF16)

    @pl.loop(0, n_chunks)
    def _(idx):
        _, _, k_out, v_out = chunk_copies(idx)
        k_out.wait()
        v_out.wait()


def in_hbm(*arrays):
    return [pltpu.with_memory_space_constraint(a, pltpu.HBM) for a in arrays]


def in_vmem(*arrays):
    return [pltpu.with_memory_space_constraint(a, pltpu.VMEM) for a in arrays]


def attn_call(layer, do_norm, lens, freq, x_in, gain, b_q, b_k, b_v, w_q, w_k, w_v, w_o, k_cache, v_cache, prev):
    batch, slots, head = k_cache.shape[-3:]
    width = x_in.shape[1]
    q_width = w_q.shape[2]
    any_spec = pl.BlockSpec(memory_space=pltpu.HBM)
    vmem = pl.BlockSpec(memory_space=pltpu.VMEM)
    aliased = prev is not None
    place = in_hbm if do_norm else in_vmem
    args = [lens, lens.reshape(1, batch), freq, *place(x_in), gain, b_q, b_k, b_v, *in_hbm(w_q, w_k, w_v, w_o, k_cache, v_cache)]
    in_specs = [pl.BlockSpec(memory_space=pltpu.SMEM), vmem, vmem, any_spec if do_norm else vmem, vmem, vmem, vmem, vmem] + [any_spec] * 6
    aliases = {}
    if aliased:
        aliases = {len(args): 3, len(args) + 1: 1, len(args) + 2: 2}
        args += [*in_vmem(prev[0]), *in_hbm(*prev[1:])]
        in_specs += [vmem] + [any_spec] * 2
    cache_buf = pltpu.VMEM((2, batch, slots, head), BF16)
    out_cache = jax.ShapeDtypeStruct((w_q.shape[0], batch, slots, head), BF16)
    n_chunks = batch // SEQ_CHUNK
    macs = batch * width * (q_width + 2 * head) + 2 * batch * slots * q_width
    return pl.pallas_call(
        functools.partial(attn_kernel, layer, do_norm, aliased),
        out_shape=(
            pltpu.VMEM((batch, width), BF16),
            out_cache,
            out_cache,
        ) + ((cache_buf,) if aliased else ()),
        in_specs=in_specs,
        out_specs=(vmem, any_spec, any_spec) + ((vmem,) if aliased else ()),
        scratch_shapes=[
            pltpu.VMEM((batch, width), BF16),
            pltpu.VMEM((width, q_width + 2 * head), BF16),
            pltpu.VMEM((q_width, width), BF16),
            pltpu.VMEM((batch, q_width), F32),
            pltpu.VMEM((batch, head), F32),
            pltpu.VMEM((batch, head), F32),
            pltpu.VMEM((batch, head), jnp.int32),
            pltpu.VMEM((batch, q_width), F32),
            pltpu.VMEM((SEQ_CHUNK // 8, 16, slots), F32),
            pltpu.SemaphoreType.DMA,
            pltpu.SemaphoreType.DMA((4,)),
            pltpu.SemaphoreType.DMA((n_chunks,)),
            pltpu.SemaphoreType.DMA((n_chunks,)),
            pltpu.SemaphoreType.DMA((n_chunks,)),
            pltpu.SemaphoreType.DMA((n_chunks,)),
        ] + ([] if aliased else [cache_buf]),
        input_output_aliases=aliases,
        compiler_params=pltpu.CompilerParams(vmem_limit_bytes=ATTN_VMEM + (0 if aliased else 4 * batch * slots * head)),
        cost_estimate=pl.CostEstimate(flops=2 * macs, bytes_accessed=4 * batch * slots * head * 2, transcendentals=batch * slots * 2),
        name=f"attn{layer}",
    )(*args)[:3]


def mix_kernel(layer, last, part_ref, x_hbm, gm_ref, gn_ref, wg_hbm, wu_hbm, wd_hbm, kc_hbm, vc_hbm, *refs):
    if last:
        out_hbm = refs[0]
        refs = refs[1:]
    else:
        out_hbm, xs_ref, kv_next = refs[:3]
        refs = refs[3:]
    (wg, wu, wd, x_own, act, part2, d_recv, r_send, r_recv, gathered,
     w_sem, x_sem, ds_sem, dr_sem, rs_sem, rr_sem, as_sem, ar_sem, fs_sem, fr_sem, o_sem, c_sem) = refs
    width = wg.shape[0]
    parts = (part_ref, part2)
    hidden = wg.shape[1]
    rows = part_ref.shape[0] // ROW_CHUNKS
    core_rows = rows // 2
    blk = core_rows // 4
    me = lax.axis_index("tp")
    core = me % 2
    chip = me // 2
    partner = me + 1 - 2 * core
    peer_y = (chip + 2) % 4
    peer_x = chip + 1 - 2 * (chip % 2)
    peers = [chip, peer_x * (1 - core) + peer_y * core, peer_y * (1 - core) + peer_x * core, 3 - chip]

    def dev(idx):
        return {"tp": idx}

    w_copies = [pltpu.make_async_copy(src.at[layer], dst, w_sem.at[i])
                for i, (src, dst) in enumerate(((wg_hbm, wg), (wu_hbm, wu), (wd_hbm, wd)))]

    def own_rows(j):
        return pl.ds(pl.multiple_of(j * rows + core * core_rows + chip * blk, blk), blk)

    x_copies = []
    for j in range(ROW_CHUNKS):
        if layer:
            x_own[j] = x_hbm[j]
        else:
            x_copies.append(pltpu.make_async_copy(x_hbm.at[own_rows(j)], x_own.at[j], x_sem.at[j]))
            x_copies[-1].start()

    c_copies = []
    if not last:
        size = kv_next.shape[1] // PARTS
        for n in range(PREFETCHED):
            for i, src in enumerate((kc_hbm, vc_hbm)):
                part = pl.ds(n * size, size)
                c_copies.append(pltpu.make_async_copy(src.at[layer + 1, part], kv_next.at[i, part], c_sem.at[i, n]))

    def prefetch(count):
        for _ in range(min(count, len(waiting))):
            waiting.pop(0).start()

    waiting = list(c_copies)
    prefetch(2)
    barrier = pltpu.get_barrier_semaphore()
    others = [partner] + [2 * peers[r] + core for r in range(1, 4)]
    for other in others:
        pl.semaphore_signal(barrier, inc=1, device_id=dev(other), device_id_type=pl.DeviceIdType.MESH)

    def remote(src, dst, send, recv, target):
        return pltpu.make_async_remote_copy(src_ref=src, dst_ref=dst, send_sem=send, recv_sem=recv,
                                            device_id=dev(target), device_id_type=pl.DeviceIdType.MESH)

    def d_copy(s, j):
        here = pl.ds(pl.multiple_of(j * rows + (1 - core) * core_rows, core_rows), core_rows)
        return remote(parts[s].at[here], d_recv.at[s, j], ds_sem.at[s, j], dr_sem.at[s, j], partner)

    def r_copy(s, j, r):
        return remote(r_send.at[s, j, r], r_recv.at[s, j, r], rs_sem.at[s, j, r], rr_sem.at[s, j, r], 2 * peers[r] + core)

    def scatter(s, j):
        d_copy(s, j).wait()
        for r in (3, 1, 2):
            off = pl.multiple_of(peers[r] * blk, blk)
            mine = parts[s][pl.ds(pl.multiple_of(j * rows + core * core_rows + off, blk), blk), :].astype(F32)
            r_send[s, j, r] = (mine + d_recv[s, j, pl.ds(off, blk), :].astype(F32)).astype(BF16)
            r_copy(s, j, r).start()

    def reduce(s, j):
        off = pl.multiple_of(chip * blk, blk)
        total = parts[s][own_rows(j), :].astype(F32) + d_recv[s, j, pl.ds(off, blk), :].astype(F32)
        for r in (1, 2, 3):
            r_copy(s, j, r).wait()
            total += r_recv[s, j, r].astype(F32)
        new = (x_own[j].astype(F32) + total).astype(BF16)
        x_own[j] = new
        return new

    def block_row(j, cc, k):
        return pl.ds(pl.multiple_of(j * rows + cc * core_rows + k * blk, blk), blk)

    def a_copy(s, j, r):
        here = block_row(j, core, chip)
        target = partner if r == 0 else 2 * peers[r] + core
        return remote(gathered.at[s, here], gathered.at[s, here], as_sem.at[s, j, r], ar_sem.at[s, j, r], target)

    def f_copy(s, j, r):
        here = block_row(j, core, peers[r])
        return remote(gathered.at[s, here], gathered.at[s, here], fs_sem.at[s, j, r], fr_sem.at[s, j, r], partner)

    def gather_start(s, j, value):
        gathered[s, block_row(j, core, chip), :] = value
        for r in (3, 1, 2, 0):
            a_copy(s, j, r).start()

    def gather_forward(s, j):
        for r in (1, 2, 3):
            a_copy(s, j, r).wait_recv()
            f_copy(s, j, r).start()

    def gather_finish(s, j):
        a_copy(s, j, 0).wait_recv()
        for r in (1, 2, 3):
            f_copy(s, j, r).wait_recv()

    chunks = range(ROW_CHUNKS)
    per = MLP_CHUNKS
    pl.semaphore_wait(barrier, len(others))
    for j in chunks:
        d_copy(0, j).start()
    for copy in x_copies:
        copy.wait()
    for j in chunks:
        scatter(0, j)
    for copy in w_copies:
        copy.start()
    for j in chunks:
        new = reduce(0, j)
        gather_start(0, j, norm_rows(new.astype(F32), gm_ref[layer:layer + 1, :].astype(F32)))
    prefetch(3)

    def mlp(first):
        here = slice(first * rows, (first + per) * rows)
        step = 256
        lhs = gathered[0, here, :]
        for col in range(0, hidden, step):
            cols = slice(col, col + step)
            gate = jnp.dot(lhs, wg[:, cols], preferred_element_type=F32)
            up = jnp.dot(lhs, wu[:, cols], preferred_element_type=F32)
            act[here, cols] = (gate * jax.nn.sigmoid(gate) * up).astype(BF16)
        lhs = act[here, :]
        for col in range(0, width, 2 * step):
            cols = slice(col, col + 2 * step)
            part2[here, cols] = jnp.dot(lhs, wd[:, cols], preferred_element_type=F32).astype(BF16)
        for j in range(first, first + per):
            d_copy(1, j).start()

    for j in range(per):
        gather_forward(0, j)
    for copy in w_copies:
        copy.wait()
    for first in range(0, ROW_CHUNKS, per):
        for j in range(first, first + per):
            gather_finish(0, j)
        prefetch(4)
        mlp(first)
        for j in range(first + per, min(first + 2 * per, ROW_CHUNKS)):
            gather_forward(0, j)
        for j in range(first, first + per):
            scatter(1, j)

    def second(j):
        new = reduce(1, j)
        if last:
            gather_start(1, j, new)
        else:
            xs_ref[j] = new
            gather_start(1, j, norm_rows(new.astype(F32), gn_ref[layer + 1:layer + 2, :].astype(F32)))

    for j in chunks:
        second(j)
    prefetch(1)
    for j in chunks:
        gather_forward(1, j)
    prefetch(len(waiting))
    outs = []
    for j in chunks:
        gather_finish(1, j)
        here = pl.ds(j * rows, rows)
        if last:
            outs.append(pltpu.make_async_copy(gathered.at[1, here], out_hbm.at[here], o_sem.at[j]))
            outs[-1].start()
        else:
            out_hbm[here, :] = gathered[1, here, :]
    for s in range(2):
        for j in range(ROW_CHUNKS):
            for r in range(4):
                a_copy(s, j, r).wait_send()
            for r in range(1, 4):
                f_copy(s, j, r).wait_send()
    for copy in outs + c_copies:
        copy.wait()


def mix_call(layer, last, part, x_own, g_mlp, g_attn, w_gate, w_up, w_down, k_cache, v_cache):
    batch, width = part.shape
    hidden = w_gate.shape[2]
    rows = batch // ROW_CHUNKS
    blk = rows // 8
    any_spec = pl.BlockSpec(memory_space=pltpu.HBM)
    vmem = pl.BlockSpec(memory_space=pltpu.VMEM)
    if last:
        out_shape = [jax.ShapeDtypeStruct((batch, width), BF16)]
        out_specs = [any_spec]
    else:
        out_shape = [pltpu.VMEM((batch, width), BF16), pltpu.VMEM((ROW_CHUNKS, blk, width), BF16)]
        out_shape.append(pltpu.VMEM((2,) + k_cache.shape[1:], BF16))
        out_specs = [vmem] * 3
    sem = pltpu.SemaphoreType.DMA
    nc = ROW_CHUNKS
    return pl.pallas_call(
        functools.partial(mix_kernel, layer, last),
        out_shape=out_shape,
        in_specs=[vmem, any_spec if layer == 0 else vmem, vmem, vmem] + [any_spec] * 5,
        out_specs=out_specs,
        scratch_shapes=[
            pltpu.VMEM((width, hidden), BF16),
            pltpu.VMEM((width, hidden), BF16),
            pltpu.VMEM((hidden, width), BF16),
            pltpu.VMEM((nc, blk, width), BF16),
            pltpu.VMEM((batch, hidden), BF16),
            pltpu.VMEM((batch, width), BF16),
            pltpu.VMEM((2, nc, rows // 2, width), BF16),
            pltpu.VMEM((2, nc, 4, blk, width), BF16),
            pltpu.VMEM((2, nc, 4, blk, width), BF16),
            pltpu.VMEM((2, batch, width), BF16),
            sem((3,)), sem((nc,)),
            sem((2, nc)), sem((2, nc)),
            sem((2, nc, 4)), sem((2, nc, 4)),
            sem((2, nc, 4)), sem((2, nc, 4)),
            sem((2, nc, 4)), sem((2, nc, 4)),
            sem((nc,)), sem((2, PREFETCHED)),
        ],
        compiler_params=pltpu.CompilerParams(collective_id=layer, has_side_effects=True, vmem_limit_bytes=MIX_VMEM),
        cost_estimate=pl.CostEstimate(flops=6 * batch * width * hidden, bytes_accessed=6 * width * hidden, transcendentals=batch * hidden),
        name=f"mix{layer}",
    )(*in_vmem(part), *(in_hbm if layer == 0 else in_vmem)(x_own), g_mlp, g_attn, *in_hbm(w_gate, w_up, w_down, k_cache, v_cache))


def solution(mesh):
    weight_col = P(None, None, "tp")
    weight_row = P(None, "tp", None)
    bias_col = P(None, "tp")
    cache_spec = P(None, "dp", None, "tp", None)
    in_specs = (P("dp", None), P("dp"), P(None, None), P(None, None), weight_col, bias_col, weight_col, bias_col, weight_col, bias_col, weight_row, weight_col, weight_col, weight_row, cache_spec, cache_spec)
    out_specs = (P("dp", None), cache_spec, cache_spec)

    def local_step(x_in, seq_lens, g_attn, g_mlp, w_q, b_q, w_k, b_k, w_v, b_v, w_o, w_gate, w_up, w_down, k_cache, v_cache):
        layers, batch, slots, _, head = k_cache.shape
        inv_freq = ROPE_THETA ** (-2.0 * np.arange(head // 2) / head)
        freq = jnp.asarray(np.concatenate([inv_freq, inv_freq])[None, :].astype(np.float32))
        k_flat = k_cache.reshape(layers, batch, slots, head)
        v_flat = v_cache.reshape(layers, batch, slots, head)
        normed, x_own, prev = x_in, x_in, None
        for layer in range(layers):
            last = layer == layers - 1
            part, k_out, v_out = attn_call(layer, layer == 0, seq_lens, freq, normed, g_attn, b_q, b_k, b_v, w_q, w_k, w_v, w_o, k_flat, v_flat, prev)
            outs = mix_call(layer, last, part, x_own, g_mlp, g_attn, w_gate, w_up, w_down, k_flat, v_flat)
            if last:
                x_out = outs[0]
            else:
                normed, x_own, prev = outs[0], outs[1], (outs[2], k_out, v_out)
        return x_out, k_out.reshape(k_cache.shape), v_out.reshape(v_cache.shape)

    return jax.shard_map(local_step, mesh=mesh, in_specs=in_specs, out_specs=out_specs, check_vma=False)
```
